32 devices in a mesh: section: 2 (over x), fsdp: 16 (over z, y, core).
Axes of the slice: x: 2, y: 2, z: 4, core: 2. Of those that a mesh axis runs over, the one named last changes fastest.
Arguments:
- hidden_in: bfloat16 [8, 16, 64, 1536], P(None, 'fsdp'), may hold values from -6 to 6
- norm_gain: float32 [2, 2, 1536], P(None, 'section'), may hold values from 0.25 to 1.75
- qkv_weight: bfloat16 [2, 2, 1536, 2048], P(None, 'section', 'fsdp'), may hold values from -0.15625 to 0.15625
- qkv_bias: float32 [2, 2, 2048], P(None, 'section'), may hold values from -30 to 30, as said below
- out_weight: bfloat16 [2, 2, 1536, 1536], P(None, 'section', 'fsdp'), may hold values from -0.15625 to 0.15625
Outputs:
- hidden_out: bfloat16 [8, 16, 64, 1536], P('section', 'fsdp')
The draws below stay inside these ranges and needn't reach their ends.
Inputs may be any that keep to these rules, and one draw needn't show every extreme that they name: `qkv_bias`: entries of the query, key and value biases.
All inputs are finite; a program needn't handle non-finite values.
Results may differ from the reference program's by a relative error of at most 0.035.
Values may be sent and summed in bfloat16 or wider, within the bound.
A program may use at most 128 MiB of HBM per device.

```python
import math
import jax
import jax.numpy as jnp
from jax import lax

D = 1536
HEADS = 12
KV_HEADS = 2
HEAD_DIM = 128
LEN = 64
MICRO = 8
SPANS = 2
SEQS = 16
QKV = 2048
N_SECTION = 2


def draw_qkv_bias(key, part):
    bias_shape = (SPANS, N_SECTION, QKV)
    return jnp.clip(0.5 * jax.random.normal(key, bias_shape, jnp.float32), -3.0, 3.0)


def block_levels(key, extent, shards, least, top_value):
    def one(position, shards_of):
        heights = jax.random.uniform(jax.random.fold_in(jax.random.fold_in(key, 6), position), (shards_of,), jnp.float32, least / len(shards), top_value / len(shards))
        return jnp.repeat(jnp.exp(heights), extent[position] // shards_of).reshape((-1,) + (1,) * (len(extent) - position - 1))

    loudness = one(*shards[0])
    for cut in shards[1:]:
        loudness = loudness * one(*cut)
    return loudness


def scatter_about(stream_key, dims, deviation, most, split=(), kind=jnp.bfloat16):
    values = jax.random.normal(stream_key, dims, jnp.float32) * deviation
    if len(split) > 0:
        values = block_levels(stream_key, dims, split, -0.22, 0.18) * values
    return jnp.clip(values, min=-most, max=most).astype(kind)


def setup_inputs(seed: int = 0) -> dict:
    arg_keys = jax.random.split(jax.random.key(seed), 6)
    return {
        "hidden_in": scatter_about(arg_keys[0], (MICRO, SEQS, LEN, D), 1.0, 6.0, ((1, 16),)),
        "norm_gain": jnp.clip(1.0 + 0.15 * jax.random.normal(arg_keys[1], (SPANS, N_SECTION, D), jnp.float32), 0.25, 1.75),
        "qkv_weight": scatter_about(arg_keys[2], (SPANS, N_SECTION, D, QKV), D ** -0.5, 0.15625, ((1, 2), (2, 16))),
        "qkv_bias": draw_qkv_bias(jax.random.fold_in(arg_keys[5], 71), 0),
        "out_weight": scatter_about(arg_keys[4], (SPANS, N_SECTION, D, D), D ** -0.5, 0.15625, ((1, 2), (2, 16))),
    }


THETA = 1000000.0
EPS = 1.0

def rotate(tensor, cosine, sine_part):
    half_dim = tensor.shape[-1] // 2
    leading = tensor[..., :half_dim]
    second = tensor[..., half_dim:]
    return jnp.concatenate([leading * cosine - second * sine_part, second * cosine + leading * sine_part], axis=-1)

def attend_layer(hidden, gain, w_qkv, bias, w_out):
    rows, length, width = hidden.shape
    group_size = HEADS // KV_HEADS
    kv_width = KV_HEADS * HEAD_DIM
    wide = hidden.astype(jnp.float32)
    inv_rms = lax.rsqrt(lax.optimization_barrier(jnp.mean(wide * wide, axis=-1, keepdims=True)) + EPS)
    normed = (wide * inv_rms * gain).astype(jnp.bfloat16)
    projected = jnp.dot(normed.reshape(rows * length, width), w_qkv, preferred_element_type=jnp.float32) + bias
    projected = projected.reshape(rows, length, width + 2 * kv_width)
    queries = projected[..., :width].reshape(rows, length, KV_HEADS, group_size, HEAD_DIM)
    key_rows = projected[..., width:width + kv_width].reshape(rows, length, KV_HEADS, HEAD_DIM)
    value_rows = projected[..., width + kv_width:].astype(jnp.bfloat16).reshape(rows, length, KV_HEADS, HEAD_DIM)
    half_dim = HEAD_DIM // 2
    frequency = jnp.exp(jnp.arange(half_dim, dtype=jnp.float32) * (-2.0 * math.log(THETA) / HEAD_DIM))
    angles = jnp.arange(length, dtype=jnp.float32)[:, None] * frequency[None, :]
    cosine = jnp.cos(angles)
    sine_part = jnp.sin(angles)
    queries = rotate(queries, cosine[None, :, None, None, :], sine_part[None, :, None, None, :])
    key_rows = rotate(key_rows, cosine[None, :, None, :], sine_part[None, :, None, :])
    scores = jnp.einsum('rqkgd,rpkd->rkgqp', queries, key_rows, precision=lax.Precision.HIGHEST) / math.sqrt(HEAD_DIM)
    causal = jnp.arange(length)[:, None] >= jnp.arange(length)[None, :]
    scores = jnp.where(causal, scores, -1e+30)
    row_max = lax.optimization_barrier(jnp.max(scores, axis=-1, keepdims=True))
    weights = jnp.exp(scores - row_max)
    probability = (weights / lax.optimization_barrier(jnp.sum(weights, axis=-1, keepdims=True))).astype(jnp.bfloat16)
    context = jnp.einsum('rkgqp,rpkd->rqkgd', probability.astype(jnp.float32), value_rows.astype(jnp.float32), precision=lax.Precision.HIGHEST)
    context = context.reshape(rows, length, width).astype(jnp.bfloat16)
    update = jnp.dot(context.reshape(rows * length, width), w_out, preferred_element_type=jnp.float32)
    return (wide + update.reshape(rows, length, width)).astype(jnp.bfloat16)

def reference(hidden_in, norm_gain, qkv_weight, qkv_bias, out_weight):
    hidden = hidden_in
    for span_no in range(norm_gain.shape[0]):
        for section_no in range(norm_gain.shape[1]):

            def apply_layer(block_rows, span_no=span_no, section_no=section_no):
                return attend_layer(block_rows, norm_gain[span_no, section_no], qkv_weight[span_no, section_no], qkv_bias[span_no, section_no], out_weight[span_no, section_no])
            hidden = lax.map(apply_layer, hidden)
    return hidden
```

```python
import heapq
from functools import partial
import math

import jax
import jax.numpy as jnp
import numpy as np
from jax import lax
from jax.experimental import pallas as pl
from jax.experimental.pallas import tpu as pltpu
from jax.sharding import PartitionSpec as P

HEADS = 12
KV_HEADS = 2
HEAD_DIM = 128


THETA = 1000000.0
EPS = 1.0


def as_sent(array):

    def short(part):
        return part.astype(jnp.bfloat16) if part.dtype == jnp.float32 else part

    return jax.tree.map(short, array)


def passed_along(block, axis, distance):
    devices = range(lax.axis_size(axis))
    route = [((i - distance) % len(devices), i) for i in devices]
    return lax.ppermute(block, axis, route)


def from_root(value, axis, source):
    kept = jnp.where(lax.axis_index(axis) == source, value, 0).astype(value.dtype)
    return lax.psum(kept, axis)


def rotate(tensor, cosine, sine_part):
    half_dim = tensor.shape[-1] // 2
    leading = tensor[..., :half_dim]
    second = tensor[..., half_dim:]
    return jnp.concatenate(
        [leading * cosine - second * sine_part, second * cosine + leading * sine_part], axis=-1
    )


def attend_layer(hidden, gain, w_qkv, bias, w_out):
    rows, length, width = hidden.shape
    group_size = HEADS // KV_HEADS
    kv_width = KV_HEADS * HEAD_DIM
    wide = hidden.astype(jnp.float32)
    inv_rms = lax.rsqrt(jnp.mean(wide * wide, axis=-1, keepdims=True) + EPS)
    normed = (wide * inv_rms * gain).astype(jnp.bfloat16)
    projected = (
        jnp.dot(normed.reshape(rows * length, width), w_qkv, preferred_element_type=jnp.float32)
        + bias
    )
    projected = projected.reshape(rows, length, width + 2 * kv_width)
    queries = projected[..., :width].reshape(rows, length, KV_HEADS, group_size, HEAD_DIM)
    key_rows = projected[..., width : width + kv_width].reshape(rows, length, KV_HEADS, HEAD_DIM)
    value_rows = (
        projected[..., width + kv_width :]
        .astype(jnp.bfloat16)
        .reshape(rows, length, KV_HEADS, HEAD_DIM)
    )
    half_dim = HEAD_DIM // 2
    frequency = jnp.exp(
        jnp.arange(half_dim, dtype=jnp.float32) * (-2.0 * math.log(THETA) / HEAD_DIM)
    )
    angles = jnp.arange(length, dtype=jnp.float32)[:, None] * frequency[None, :]
    cosine = jnp.cos(angles)
    sine_part = jnp.sin(angles)
    queries = rotate(queries, cosine[None, :, None, None, :], sine_part[None, :, None, None, :])
    key_rows = rotate(key_rows, cosine[None, :, None, :], sine_part[None, :, None, :])
    scores = jnp.einsum(
        "rqkgd,rpkd->rkgqp", queries, key_rows, precision=lax.Precision.HIGHEST
    ) / math.sqrt(HEAD_DIM)
    causal = jnp.arange(length)[:, None] >= jnp.arange(length)[None, :]
    scores = jnp.where(causal, scores, -1e30)
    row_max = jnp.max(scores, axis=-1, keepdims=True)
    weights = jnp.exp(scores - row_max)
    probability = (weights / jnp.sum(weights, axis=-1, keepdims=True)).astype(jnp.bfloat16)
    context = jnp.einsum(
        "rkgqp,rpkd->rqkgd", probability, value_rows, preferred_element_type=jnp.float32
    )
    context = context.reshape(rows, length, width).astype(jnp.bfloat16)
    update = jnp.dot(
        context.reshape(rows * length, width), w_out, preferred_element_type=jnp.float32
    )
    return (wide + update.reshape(rows, length, width)).astype(jnp.bfloat16)


def run_span(weight_pair, gain, bias, block_rows):
    return attend_layer(block_rows, gain, weight_pair[0], bias, weight_pair[1])


def vanish(block_rows):
    return jnp.zeros_like(block_rows)


def per_device(hidden_in, norm_gain, qkv_weight, qkv_bias, out_weight):
    sections = lax.axis_size("section")
    my_section = lax.axis_index("section")
    micro_count = hidden_in.shape[0]
    owned_count = micro_count // sections
    tick_count = 2 * micro_count + sections - 1
    span_gains = norm_gain[:, 0]
    biases = qkv_bias[:, 0]
    waiting = jnp.zeros_like(hidden_in)
    result = jnp.zeros_like(hidden_in)

    def make_tick(layers):
        branches = [vanish]
        for span_no in range(2):
            branches.append(
                partial(run_span, layers[span_no], span_gains[span_no], biases[span_no])
            )

        def advance(moment, state_pair):
            waiting, result = state_pair
            work_item = moment - my_section
            active = (work_item >= 0) & (work_item < 2 * micro_count)
            span_id = jnp.clip(work_item // micro_count, 0, 1)
            slot_id = jnp.mod(work_item, micro_count)
            entering = lax.dynamic_index_in_dim(hidden_in, slot_id, 0, keepdims=False)
            stored = lax.dynamic_index_in_dim(waiting, slot_id, 0, keepdims=False)
            block_in = jnp.where((span_id == 0) & (my_section == 0), entering, stored)
            selector = jnp.where(active, span_id + 1, 0)
            block_out = lax.switch(selector, branches, block_in)
            arrived = jax.tree.map(
                lambda part, own: part.astype(own.dtype),
                passed_along(as_sent(block_out), "section", 1),
                block_out,
            )
            sender = jnp.mod(my_section - 1, sections)
            sent_item = moment - sender
            accept = (
                (sent_item >= 0)
                & (sent_item < 2 * micro_count)
                & jnp.logical_not((sender == sections - 1) & (sent_item >= micro_count))
            )
            got_slot = jnp.mod(sent_item, micro_count)
            before = lax.dynamic_index_in_dim(waiting, got_slot, 0, keepdims=False)
            waiting = lax.dynamic_update_index_in_dim(
                waiting, jnp.where(accept, arrived, before), got_slot, 0
            )
            finish = moment - (sections - 1) - micro_count
            completed = (finish >= 0) & (finish < micro_count)
            final_slot = jnp.clip(finish, 0, micro_count - 1)
            previous = lax.dynamic_index_in_dim(result, final_slot, 0, keepdims=False)
            owned = completed & (my_section == sections - 1)
            result = lax.dynamic_update_index_in_dim(
                result, jnp.where(owned, block_out, previous), final_slot, 0
            )
            return (waiting, result)

        return advance

    first_pair = (
        lax.all_gather(qkv_weight[0, 0], "fsdp", axis=0, tiled=True),
        lax.all_gather(out_weight[0, 0], "fsdp", axis=0, tiled=True),
    )
    state_pair = lax.fori_loop(
        0, micro_count, make_tick((first_pair, first_pair)), (waiting, result)
    )
    second_pair = (
        lax.all_gather(qkv_weight[1, 0], "fsdp", axis=0, tiled=True),
        lax.all_gather(out_weight[1, 0], "fsdp", axis=0, tiled=True),
    )
    state_pair = lax.fori_loop(
        micro_count, tick_count, make_tick((first_pair, second_pair)), state_pair
    )
    waiting, result = state_pair
    result = from_root(result, "section", sections - 1)
    return lax.dynamic_slice_in_dim(result, my_section * owned_count, owned_count, 0)


MESH = pl.DeviceIdType.MESH
LANES = 128
KINDS = ("y", "up", "down", "own", "core_y", "core_z")
LINK = 46650.0
LAG = 1.8
CHUNKS = 4
SPLITS = ((("zy", 12), ("zy", 11), ("yz", 5)), (("zy", 12), ("zy", 11), ("yz", 5)))
RELEASES = (0.0, 47.0)
PARTS = 3


class Stream:
    def __init__(self, number, slot, order, first, tiles):
        self.number, self.slot, self.order = number, slot, order
        self.columns = pl.ds(first * LANES, tiles * LANES)
        self.tiles = tiles


def make_streams(columns, depths):
    total = columns // LANES
    streams = []
    for depth in range(depths):
        split = SPLITS[min(depth, len(SPLITS) - 1)]
        whole = sum(tiles for _, tiles in split)
        edges = [0]
        for _, tiles in split:
            edges.append(edges[-1] + tiles)
        edges = [edge * total // whole for edge in edges]
        for (order, _), low, high in zip(split, edges, edges[1:]):
            streams.append(Stream(len(streams), depth, order, low, high - low))
    return streams


def arrivals(count_z, shard, streams, releases):
    free, heard, events = {}, {}, []
    unit = shard * LANES * 2 / LINK

    def push(now, kind, *rest):
        heapq.heappush(events, (now, len(heard), kind, rest))

    def issue(now, kind, stream, stage, source, z):
        size = stream.tiles * unit * (2 if "y" in stream.order[:stage] else 1)
        done = max(now, free.get((z, kind), 0.0)) + size
        free[z, kind] = done
        to = z + {"up": 1, "down": -1}.get(kind, 0)
        push(done + LAG, "arrive", stream.number, stage, source, to)

    def have(now, stream, stage, source, z):
        if stage == len(stream.order):
            return
        if stream.order[stage] == "y":
            issue(now, "y", stream, stage, source, z)
            return
        if z < count_z - 1:
            issue(now, "up", stream, stage, source, z)
        if z > 0:
            issue(now, "down", stream, stage, source, z)
        have(now, stream, stage + 1, source, z)

    for stream in streams:
        for z in range(count_z):
            push(releases[stream.slot], "start", stream.number, 0, z, z)
    while events:
        now, _, kind, (number, stage, source, z) = heapq.heappop(events)
        stream = streams[number]
        if kind == "start":
            heard.setdefault((number, -1, 0), []).append(now)
            have(now, stream, 0, source, z)
            continue
        heard.setdefault((number, stage, source - z), []).append(now)
        if stream.order[stage] == "z" and 0 < z < count_z - 1:
            issue(now, "up" if source < z else "down", stream, stage, source, z)
        have(now, stream, stage + 1, source, z)
    mean = {key: sum(times) / len(times) for key, times in heard.items()}
    last = {}
    for key, times in heard.items():
        slot = streams[key[0]].slot
        last[slot] = max(last.get(slot, 0.0), *times)
    return mean, last


def both(first, second):
    if first is None or second is None:
        return second if first is None else first
    return first & second


def under(when, action):
    if when is None:
        action()
    else:
        pl.when(when)(action)


class Place:
    def __init__(self, count_z):
        self.x = lax.axis_index("section")
        self.f = lax.axis_index("fsdp")
        self.p, self.y, self.z = self.f % 2, (self.f // 2) % 2, self.f // 4
        self.count_z = count_z

    def target(self, kind):
        if kind == "x":
            return {"section": 1 - self.x, "fsdp": self.f}
        step = {"y": 2 - 4 * self.y, "up": 4, "down": -4}.get(kind, 1 - 2 * self.p)
        return {"section": self.x, "fsdp": self.f + step}


class Gather:
    def __init__(self, stream, held, place, send_sems, recv_sems, sent):
        self.stream, self.held, self.place = stream, held, place
        self.send_sems, self.recv_sems, self.sent = send_sems, recv_sems, sent

    def valid(self, d):
        z = self.place.z + d
        return (z >= 0) & (z < self.place.count_z)

    def region(self, shift, rows, p):
        stream = self.stream
        return self.held.at[stream.slot, self.place.z + shift, rows, p, :, stream.columns]

    def copy(self, kind, ref, shift):
        slot = self.place.z + shift
        kind_no = KINDS.index(kind)
        recv_no = KINDS.index("up") if kind == "down" else kind_no
        number = self.stream.number
        return pltpu.make_async_remote_copy(
            src_ref=ref,
            dst_ref=ref,
            send_sem=self.send_sems.at[number, kind_no, slot],
            recv_sem=self.recv_sems.at[number, recv_no, slot],
            device_id=self.place.target(kind),
            device_id_type=MESH,
        )

    def rows(self, got, other=False):
        if got:
            return pl.ds(0, 2)
        return 1 - self.place.y if other else self.place.y

    def send(self, kind, ref, shift, when=None):
        under(when, lambda: self.copy(kind, ref, shift).start())
        self.sent.append(lambda: under(when, lambda: self.copy(kind, ref, shift).wait_send()))

    def have(self, stage, shift, when=None):
        order, place = self.stream.order, self.place
        if stage == len(order):
            return
        ref = self.region(shift, self.rows("y" in order[:stage]), place.p)
        if order[stage] == "y":
            self.send("y", ref, shift, when)
            return
        self.send("up", ref, shift, place.z < place.count_z - 1)
        self.send("down", ref, shift, place.z > 0)
        self.have(stage + 1, shift)

    def shifts(self):
        pairs = [(-r, r) for r in range(1, self.place.count_z)]
        return [d for pair in pairs for d in pair]

    def arrive(self, stage, shift, partner=False):
        order, place = self.stream.order, self.place
        rows = self.rows("y" in order[:stage], other=order[stage] == "y")
        return self.region(shift, rows, 1 - place.p if partner else place.p)

    def start(self):
        self.have(0, 0)
        ref = self.region(0, self.rows(False), self.place.p)
        self.send("own", ref, 0)

    def step(self, stage, shift):
        place = self.place
        dim = self.stream.order[stage]
        when = self.valid(shift) if shift else None
        kind = ("up" if shift < 0 else "down") if dim == "z" else dim
        ref = self.arrive(stage, shift)
        under(when, lambda: self.copy(kind, ref, shift).wait_recv())
        if dim == "z":
            onward = place.z < place.count_z - 1 if shift < 0 else place.z > 0
            self.send(kind, ref, shift, both(when, onward))
        self.have(stage + 1, shift, when)
        self.send("core_" + dim, ref, shift, when)

    def from_partner(self):
        order, place = self.stream.order, self.place
        ref = self.region(0, self.rows(False), 1 - place.p)
        self.copy("own", ref, 0).wait_recv()
        for stage, dim in enumerate(order):
            spread = "z" in order[:stage]
            shifts = self.shifts() if dim == "z" else [0] + (self.shifts() if spread else [])
            for shift in shifts:
                ref = self.arrive(stage, shift, partner=True)

                def wait(ref=ref, shift=shift):
                    self.copy("core_" + dim, ref, shift).wait_recv()

                under(self.valid(shift) if shift else None, wait)


def greet(place):
    barrier = pltpu.get_barrier_semaphore()
    z, count_z = place.z, place.count_z

    def signal(kind):
        pl.semaphore_signal(barrier, inc=1, device_id=place.target(kind), device_id_type=MESH)

    signal("x")
    signal("y")
    signal("own")
    pl.when(z < count_z - 1)(lambda: signal("up"))
    pl.when(z > 0)(lambda: signal("down"))
    ends = jnp.where(z < count_z - 1, 1, 0) + jnp.where(z > 0, 1, 0)
    pl.semaphore_wait(barrier, 3 + ends)


def turned(tensor, cosine, sine_part):
    return tensor * cosine + pltpu.roll(tensor, tensor.shape[-1] // 2, 1) * sine_part


def thirds(tensor):
    parts = []
    for _ in range(3):
        part = tensor.astype(jnp.bfloat16)
        parts.append(part)
        tensor = tensor - part.astype(jnp.float32)
    return parts


def exact_scores(queries, keys):
    q1, q2, q3 = thirds(queries)
    k1, k2, k3 = thirds(keys)
    left = jnp.concatenate([q1, q2, q1, q2, q1, q3], axis=1)
    right = jnp.concatenate([k1, k1, k2, k2, k3, k1], axis=1)
    return lax.dot_general(
        left, right, (((1,), (1,)), ((), ())), preferred_element_type=jnp.float32
    )


def layer_pieces(depth, here, length, held, gains, biases, angles, before, after, scratch):
    normed, projected, context = scratch
    rows, width = normed.shape
    depth_rows = held.shape[1] * held.shape[2] * held.shape[3] * held.shape[4]
    group_size = HEADS // KV_HEADS
    kv_width = KV_HEADS * HEAD_DIM
    tile = 2 * LANES

    def weight(column):
        return held[depth, :, :, :, :, pl.ds(column, tile)].reshape(depth_rows, tile)

    def project():
        wide = before[depth, here, :].astype(jnp.float32)
        inv_rms = lax.rsqrt(jnp.mean(wide * wide, axis=-1, keepdims=True) + EPS)
        normed[...] = (wide * inv_rms * gains[depth, 0]).astype(jnp.bfloat16)

        @pl.loop(0, projected.shape[1] // tile)
        def _(j):
            column = pl.multiple_of(j * tile, tile)
            block = jnp.dot(normed[...], weight(column), preferred_element_type=jnp.float32)
            projected[:, pl.ds(column, tile)] = block + biases[depth, 0, :, pl.ds(column, tile)]

    def attend():
        cosine, sine_part = angles[0], angles[1]
        shape = (group_size * length, length)
        query_at = lax.rem(lax.broadcasted_iota(jnp.int32, shape, 0), length)
        causal = query_at >= lax.broadcasted_iota(jnp.int32, shape, 1)

        @pl.loop(0, rows // length)
        def _(unit):
            there = pl.ds(pl.multiple_of(unit * length, length), length)
            for head in range(KV_HEADS):
                first = head * group_size * HEAD_DIM

                def columns(start):
                    return projected[there, start : start + HEAD_DIM]

                queries = jnp.concatenate(
                    [
                        turned(columns(first + h * HEAD_DIM), cosine, sine_part)
                        for h in range(group_size)
                    ],
                    axis=0,
                )
                keys = turned(columns(width + head * HEAD_DIM), cosine, sine_part)
                values = columns(width + kv_width + head * HEAD_DIM).astype(jnp.bfloat16)
                scores = exact_scores(queries, keys) * (1.0 / math.sqrt(HEAD_DIM))
                scores = jnp.where(causal, scores, -1e30)
                weights = jnp.exp(scores - jnp.max(scores, axis=-1, keepdims=True))
                total = jnp.sum(weights, axis=-1, keepdims=True)
                probability = (weights / total).astype(jnp.bfloat16)
                block = jnp.dot(probability, values, preferred_element_type=jnp.float32)
                block = block.astype(jnp.bfloat16)
                for h in range(group_size):
                    to = slice(first + h * HEAD_DIM, first + (h + 1) * HEAD_DIM)
                    context[there, to] = block[h * length : (h + 1) * length]

    def update():
        @pl.loop(0, width // tile)
        def _(j):
            column = pl.multiple_of(j * tile, tile)
            to = pl.ds(column, tile)
            block = jnp.dot(
                context[...], weight(projected.shape[1] + column), preferred_element_type=jnp.float32
            )
            wide = before[depth, here, to].astype(jnp.float32)
            after[depth, here, to] = (wide + block).astype(jnp.bfloat16)

    return project, attend, update


def time_line(chunks, ready):
    pace = 33.7 / chunks
    spots = []
    for depth in range(len(ready)):
        for chunk in range(chunks):
            start = ready[depth] + 2.0 + pace * chunk
            spots.append((start, 0, depth, chunk))
            spots.append((start + 7.0 + pace, 1, depth, chunk))
    return spots


def section_kernel(
    count_z,
    depths,
    length,
    hidden_ref,
    gain_ref,
    qkv_ref,
    bias_ref,
    out_ref,
    angles,
    result,
    held,
    gains,
    biases,
    before,
    after,
    normed,
    projected,
    context,
    send_sems,
    recv_sems,
    act_sems,
    local_sems,
):
    place = Place(count_z)
    x, y, z, p = place.x, place.y, place.z, place.p
    qkv = qkv_ref.shape[-1]
    width = out_ref.shape[-1]
    owned = result.shape[0]
    rows = normed.shape[0]
    chunks = before.shape[1] // rows

    loads = [
        (None, pltpu.make_async_copy(gain_ref, gains, local_sems.at[0])),
        (None, pltpu.make_async_copy(bias_ref, biases, local_sems.at[1])),
        (x == 0, pltpu.make_async_copy(hidden_ref, before.at[0], local_sems.at[2])),
    ]
    for depth in range(depths):
        home = held.at[depth, z, y, p]
        loads.append(
            (
                None,
                pltpu.make_async_copy(
                    qkv_ref.at[depth, 0], home.at[:, pl.ds(0, qkv)], local_sems.at[3 + 2 * depth]
                ),
            )
        )
        loads.append(
            (
                None,
                pltpu.make_async_copy(
                    out_ref.at[depth, 0], home.at[:, pl.ds(qkv, width)], local_sems.at[4 + 2 * depth]
                ),
            )
        )
    for when, load in loads:
        under(when, load.start)
    greet(place)
    for when, load in loads:
        under(when, load.wait)

    sent = []
    streams = make_streams(qkv + width, depths)
    gathers = [Gather(stream, held, place, send_sems, recv_sems, sent) for stream in streams]
    mean, last = arrivals(count_z, held.shape[4], streams, RELEASES)
    ready = [last[depth] for depth in range(depths)]

    def crossing(slot, chunk, depth):
        here = pl.ds(chunk * rows, rows)
        return pltpu.make_async_remote_copy(
            src_ref=after.at[depth, here],
            dst_ref=before.at[slot, here],
            send_sem=act_sems.at[0, depth, chunk],
            recv_sem=act_sems.at[1, slot, chunk],
            device_id=place.target("x"),
            device_id_type=MESH,
        )

    def spot(section, depth, chunk):
        here = pl.ds(chunk * rows, rows)
        pieces = layer_pieces(
            depth, here, length, held, gains, biases, angles, before, after,
            (normed, projected, context),
        )
        first = section == 0 and depth == 0
        final = section == 1 and depth == depths - 1 and chunk >= chunks // 2

        def begin():
            if not first:
                crossing(depth, chunk, 0).wait_recv()
            pieces[0]()

        def end():
            pieces[2]()
            if not final:
                crossing(depth + section, chunk, depth).start()

        if not final:
            sent.append(
                lambda: pl.when(x == section)(
                    lambda: crossing(depth + section, chunk, depth).wait_send()
                )
            )
        return [lambda f=f: pl.when(x == section)(f) for f in (begin, pieces[1], end)]

    def partner(depth):
        for gather in gathers:
            if gather.stream.slot == depth:
                gather.from_partner()

    plan = []
    for (number, stage, shift), time in mean.items():
        gather = gathers[number]
        if stage < 0:
            plan.append((time, 0, len(plan), gather.start))
        else:
            plan.append((time, 1, len(plan), partial(gather.step, stage, shift)))
    for depth in range(depths):
        plan.append((ready[depth] + 0.5, 2, len(plan), partial(partner, depth)))
    for time, section, depth, chunk in time_line(chunks, ready):
        for number, piece in enumerate(spot(section, depth, chunk)):
            plan.append((time + 1.6 * number, 3, len(plan), piece))
    for _, _, _, action in sorted(plan, key=lambda entry: entry[:3]):
        action()

    def take():
        for chunk in range(chunks // 2):
            crossing(depths, chunk, 0).wait_recv()
        result[...] = before[depths, pl.ds(0, owned), :]

    def keep():
        result[...] = after[depths - 1, pl.ds(owned, owned), :]

    pl.when(x == 0)(take)
    pl.when(x == 1)(keep)
    for finish in sent:
        finish()


def own_micros(sections, fsdp, hidden_in, norm_gain, qkv_weight, qkv_bias, out_weight):
    depths, _, shard, qkv = qkv_weight.shape
    micros, seqs, length, width = hidden_in.shape
    rows = micros * seqs * length
    owned = rows // sections
    chunk = rows // CHUNKS
    count_z = fsdp // 4
    half_dim = HEAD_DIM // 2
    frequency = np.exp(np.arange(half_dim) * (-2.0 * math.log(THETA) / HEAD_DIM))
    turn = np.arange(length)[:, None] * frequency[None, :]
    cosine, sine_part = np.cos(turn), np.sin(turn)
    angles = np.stack(
        [
            np.concatenate([cosine, cosine], axis=-1),
            np.concatenate([-sine_part, sine_part], axis=-1),
        ]
    ).astype(np.float32)
    count = len(make_streams(qkv + width, depths))
    sems = (count, len(KINDS), count_z)
    anywhere = pl.BlockSpec(memory_space=pl.ANY)
    in_vmem = pl.BlockSpec(memory_space=pltpu.VMEM)
    result = pl.pallas_call(
        partial(section_kernel, count_z, depths, length),
        out_shape=jax.ShapeDtypeStruct((owned, width), hidden_in.dtype),
        in_specs=[anywhere] * 5 + [in_vmem],
        out_specs=in_vmem,
        scratch_shapes=[
            pltpu.VMEM((depths, count_z, 2, 2, shard, qkv + width), qkv_weight.dtype),
            pltpu.VMEM((depths, 1, 1, width), jnp.float32),
            pltpu.VMEM((depths, 1, 1, qkv), jnp.float32),
            pltpu.VMEM((depths + 1, rows, width), jnp.bfloat16),
            pltpu.VMEM((depths, rows, width), jnp.bfloat16),
            pltpu.VMEM((chunk, width), jnp.bfloat16),
            pltpu.VMEM((chunk, qkv), jnp.float32),
            pltpu.VMEM((chunk, width), jnp.bfloat16),
            pltpu.SemaphoreType.DMA(sems),
            pltpu.SemaphoreType.DMA(sems),
            pltpu.SemaphoreType.DMA((2, depths + 1, CHUNKS)),
            pltpu.SemaphoreType.DMA((3 + 2 * depths,)),
        ],
        compiler_params=pltpu.CompilerParams(
            collective_id=0, has_side_effects=True, vmem_limit_bytes=62 * 1024 * 1024
        ),
    )(
        hidden_in.reshape(rows, width),
        norm_gain.reshape(depths, 1, 1, width),
        qkv_weight,
        qkv_bias.reshape(depths, 1, 1, qkv),
        out_weight,
        jnp.asarray(angles),
    )
    return result.reshape(micros // sections, seqs, length, width)


def solution(mesh):
    in_specs = (
        P(None, "fsdp", None, None),
        P(None, "section", None),
        P(None, "section", "fsdp", None),
        P(None, "section", None),
        P(None, "section", "fsdp", None),
    )
    out_specs = P("section", "fsdp", None, None)
    whole_fits = mesh.shape["section"] == 2 and mesh.shape["fsdp"] % 4 == 0
    body = partial(own_micros, mesh.shape["section"], mesh.shape["fsdp"]) if whole_fits else per_device
    return jax.shard_map(
        body, mesh=mesh, in_specs=in_specs, out_specs=out_specs, check_vma=False
    )
```

```python
import heapq
from functools import partial
import math

import jax
import jax.numpy as jnp
import numpy as np
from jax import lax
from jax.experimental import pallas as pl
from jax.experimental.pallas import tpu as pltpu
from jax.sharding import PartitionSpec as P

HEADS = 12
KV_HEADS = 2
HEAD_DIM = 128


THETA = 1000000.0
EPS = 1.0


def as_sent(array):

    def short(part):
        return part.astype(jnp.bfloat16) if part.dtype == jnp.float32 else part

    return jax.tree.map(short, array)


def passed_along(block, axis, distance):
    devices = range(lax.axis_size(axis))
    route = [((i - distance) % len(devices), i) for i in devices]
    return lax.ppermute(block, axis, route)


def from_root(value, axis, source):
    kept = jnp.where(lax.axis_index(axis) == source, value, 0).astype(value.dtype)
    return lax.psum(kept, axis)


def rotate(tensor, cosine, sine_part):
    half_dim = tensor.shape[-1] // 2
    leading = tensor[..., :half_dim]
    second = tensor[..., half_dim:]
    return jnp.concatenate(
        [leading * cosine - second * sine_part, second * cosine + leading * sine_part], axis=-1
    )


def attend_layer(hidden, gain, w_qkv, bias, w_out):
    rows, length, width = hidden.shape
    group_size = HEADS // KV_HEADS
    kv_width = KV_HEADS * HEAD_DIM
    wide = hidden.astype(jnp.float32)
    inv_rms = lax.rsqrt(jnp.mean(wide * wide, axis=-1, keepdims=True) + EPS)
    normed = (wide * inv_rms * gain).astype(jnp.bfloat16)
    projected = (
        jnp.dot(normed.reshape(rows * length, width), w_qkv, preferred_element_type=jnp.float32)
        + bias
    )
    projected = projected.reshape(rows, length, width + 2 * kv_width)
    queries = projected[..., :width].reshape(rows, length, KV_HEADS, group_size, HEAD_DIM)
    key_rows = projected[..., width : width + kv_width].reshape(rows, length, KV_HEADS, HEAD_DIM)
    value_rows = (
        projected[..., width + kv_width :]
        .astype(jnp.bfloat16)
        .reshape(rows, length, KV_HEADS, HEAD_DIM)
    )
    half_dim = HEAD_DIM // 2
    frequency = jnp.exp(
        jnp.arange(half_dim, dtype=jnp.float32) * (-2.0 * math.log(THETA) / HEAD_DIM)
    )
    angles = jnp.arange(length, dtype=jnp.float32)[:, None] * frequency[None, :]
    cosine = jnp.cos(angles)
    sine_part = jnp.sin(angles)
    queries = rotate(queries, cosine[None, :, None, None, :], sine_part[None, :, None, None, :])
    key_rows = rotate(key_rows, cosine[None, :, None, :], sine_part[None, :, None, :])
    scores = jnp.einsum(
        "rqkgd,rpkd->rkgqp", queries, key_rows, precision=lax.Precision.HIGHEST
    ) / math.sqrt(HEAD_DIM)
    causal = jnp.arange(length)[:, None] >= jnp.arange(length)[None, :]
    scores = jnp.where(causal, scores, -1e30)
    row_max = jnp.max(scores, axis=-1, keepdims=True)
    weights = jnp.exp(scores - row_max)
    probability = (weights / jnp.sum(weights, axis=-1, keepdims=True)).astype(jnp.bfloat16)
    context = jnp.einsum(
        "rkgqp,rpkd->rqkgd", probability, value_rows, preferred_element_type=jnp.float32
    )
    context = context.reshape(rows, length, width).astype(jnp.bfloat16)
    update = jnp.dot(
        context.reshape(rows * length, width), w_out, preferred_element_type=jnp.float32
    )
    return (wide + update.reshape(rows, length, width)).astype(jnp.bfloat16)


def run_span(weight_pair, gain, bias, block_rows):
    return attend_layer(block_rows, gain, weight_pair[0], bias, weight_pair[1])


def vanish(block_rows):
    return jnp.zeros_like(block_rows)


def per_device(hidden_in, norm_gain, qkv_weight, qkv_bias, out_weight):
    sections = lax.axis_size("section")
    my_section = lax.axis_index("section")
    micro_count = hidden_in.shape[0]
    owned_count = micro_count // sections
    tick_count = 2 * micro_count + sections - 1
    span_gains = norm_gain[:, 0]
    biases = qkv_bias[:, 0]
    waiting = jnp.zeros_like(hidden_in)
    result = jnp.zeros_like(hidden_in)

    def make_tick(layers):
        branches = [vanish]
        for span_no in range(2):
            branches.append(
                partial(run_span, layers[span_no], span_gains[span_no], biases[span_no])
            )

        def advance(moment, state_pair):
            waiting, result = state_pair
            work_item = moment - my_section
            active = (work_item >= 0) & (work_item < 2 * micro_count)
            span_id = jnp.clip(work_item // micro_count, 0, 1)
            slot_id = jnp.mod(work_item, micro_count)
            entering = lax.dynamic_index_in_dim(hidden_in, slot_id, 0, keepdims=False)
            stored = lax.dynamic_index_in_dim(waiting, slot_id, 0, keepdims=False)
            block_in = jnp.where((span_id == 0) & (my_section == 0), entering, stored)
            selector = jnp.where(active, span_id + 1, 0)
            block_out = lax.switch(selector, branches, block_in)
            arrived = jax.tree.map(
                lambda part, own: part.astype(own.dtype),
                passed_along(as_sent(block_out), "section", 1),
                block_out,
            )
            sender = jnp.mod(my_section - 1, sections)
            sent_item = moment - sender
            accept = (
                (sent_item >= 0)
                & (sent_item < 2 * micro_count)
                & jnp.logical_not((sender == sections - 1) & (sent_item >= micro_count))
            )
            got_slot = jnp.mod(sent_item, micro_count)
            before = lax.dynamic_index_in_dim(waiting, got_slot, 0, keepdims=False)
            waiting = lax.dynamic_update_index_in_dim(
                waiting, jnp.where(accept, arrived, before), got_slot, 0
            )
            finish = moment - (sections - 1) - micro_count
            completed = (finish >= 0) & (finish < micro_count)
            final_slot = jnp.clip(finish, 0, micro_count - 1)
            previous = lax.dynamic_index_in_dim(result, final_slot, 0, keepdims=False)
            owned = completed & (my_section == sections - 1)
            result = lax.dynamic_update_index_in_dim(
                result, jnp.where(owned, block_out, previous), final_slot, 0
            )
            return (waiting, result)

        return advance

    first_pair = (
        lax.all_gather(qkv_weight[0, 0], "fsdp", axis=0, tiled=True),
        lax.all_gather(out_weight[0, 0], "fsdp", axis=0, tiled=True),
    )
    state_pair = lax.fori_loop(
        0, micro_count, make_tick((first_pair, first_pair)), (waiting, result)
    )
    second_pair = (
        lax.all_gather(qkv_weight[1, 0], "fsdp", axis=0, tiled=True),
        lax.all_gather(out_weight[1, 0], "fsdp", axis=0, tiled=True),
    )
    state_pair = lax.fori_loop(
        micro_count, tick_count, make_tick((first_pair, second_pair)), state_pair
    )
    waiting, result = state_pair
    result = from_root(result, "section", sections - 1)
    return lax.dynamic_slice_in_dim(result, my_section * owned_count, owned_count, 0)


MESH = pl.DeviceIdType.MESH
LANES = 128
KINDS = ("y", "up", "down", "own", "core_y", "core_z", "x_y", "x_z", "x_own")
LINK = 46650.0
LAG = 1.8
CHUNKS = 4
FRONT, BACK = 3.4, 1.4
FIRST = ((0.0, "zy", 13, "q"), (0.0, "zy", 10, "q"), (0.0, "yz", 5, "q"))
SECOND = ((44.0, "zy", 8, "q"), (44.0, "zy", 8, "q"), (55.0, "zy", 8, "o"), (50.0, "yz", 4, "o"))
LAST = (
    (0.0, "zy", 9, "q", None),
    (25.0, "zy", 7, "q", None),
    (60.0, "zy", 8, "o", 85.0),
    (70.0, "yz", 2, "o", 85.0),
    (45.0, "yz", 2, "o", None),
)


class Stream:
    def __init__(self, number, slot, section, order, low, high, group, release, mode=None):
        self.number, self.slot, self.section, self.order = number, slot, section, order
        self.low, self.tiles, self.group = low, high - low, group
        self.release, self.mode = release, mode


def make_streams(projected, columns):
    split, total = projected // LANES, columns // LANES
    streams = []

    def add(table, slot, section):
        for group, low, high in (("q", 0, split), ("o", split, total)):
            rows = [row for row in table if row[3] == group]
            if len({row[3] for row in table}) == 1:
                low, high = 0, total
            whole, done = sum(row[2] for row in rows), 0
            for row in rows:
                start = low + done * (high - low) // whole
                done += row[2]
                end = low + done * (high - low) // whole
                late = row[4] if len(row) > 4 else 0.0
                mode = "forward" if late is None else None
                streams.append(
                    Stream(len(streams), slot, section, row[1], start, end, group, row[0], mode)
                )
                if late:
                    streams.append(
                        Stream(len(streams), 2, 0, row[1], start, end, group, late, "across")
                    )

    add(FIRST, 0, 0)
    add(FIRST, 0, 1)
    add(SECOND, 1, 0)
    add(LAST, 1, 1)
    return streams


def arrivals(count_z, shard, streams, crossings):
    free, heard, events = {}, {}, []
    unit = shard * LANES * 2 / LINK

    def push(now, *rest):
        heapq.heappush(events, (now, len(pushed), rest))
        pushed.append(now)

    pushed = []

    def issue(now, x, z, kind, size, rest):
        done = max(now, free.get((x, z, kind), 0.0)) + size
        free[x, z, kind] = done
        push(done + LAG, *rest)

    def size_of(stream, stage):
        return stream.tiles * unit * (2 if "y" in stream.order[: max(stage, 0)] else 1)

    def have(now, x, stream, stage, source, z):
        if stage == len(stream.order):
            return
        size = size_of(stream, stage)
        if stream.order[stage] == "y":
            issue(now, x, z, "y", size, ("arrive", x, stream, stage, source, z))
            return
        if z < count_z - 1:
            issue(now, x, z, "up", size, ("arrive", x, stream, stage, source, z + 1))
        if z > 0:
            issue(now, x, z, "down", size, ("arrive", x, stream, stage, source, z - 1))
        have(now, x, stream, stage + 1, source, z)

    def note(now, x, kind, stream, stage, shift):
        heard.setdefault((x, kind, stream.number, stage, shift), []).append(now)

    def begin(now, x, stream, z):
        have(now, x, stream, 0, z, z)
        if stream.mode == "forward":
            issue(now, x, z, "x", size_of(stream, -1), ("mirror", 1 - x, stream, -1, z, z))

    for stream in streams:
        for x in (0, 1):
            if stream.section == x:
                for z in range(count_z):
                    push(stream.release, "start", x, stream, -1, z, z)
    for time, x, size in crossings:
        for z in range(count_z):
            push(time, "act", x, size, 0, z, z)
    while events:
        now, _, (kind, x, stream, stage, source, z) = heapq.heappop(events)
        if kind == "act":
            issue(now, x, z, "x", stream, ("none", x, None, 0, z, z))
        elif kind == "start":
            if stream.mode == "across":
                note(now, 1 - x, "give", stream, -1, 0)
                issue(now, 1 - x, z, "x", size_of(stream, -1), ("given", x, stream, -1, z, z))
            else:
                note(now, x, "start", stream, -1, 0)
                begin(now, x, stream, z)
        elif kind == "given":
            note(now, x, "given", stream, -1, 0)
            begin(now, x, stream, z)
        elif kind == "mirror":
            note(now, x, "mirror", stream, stage, source - z)
        elif kind == "arrive":
            note(now, x, "arrive", stream, stage, source - z)
            size = size_of(stream, stage)
            if stream.order[stage] == "z" and 0 < z < count_z - 1:
                way, to = ("up", z + 1) if source < z else ("down", z - 1)
                issue(now, x, z, way, size, ("arrive", x, stream, stage, source, to))
            have(now, x, stream, stage + 1, source, z)
            if stream.mode == "forward":
                issue(now, x, z, "x", size, ("mirror", 1 - x, stream, stage, source, z))
    mean = {key: sum(times) / len(times) for key, times in heard.items()}
    last = {}
    for (x, kind, number, _, _), times in heard.items():
        if kind in ("arrive", "mirror"):
            stream = streams[number]
            slot = 2 if kind == "mirror" else stream.slot
            for group in (stream.group, "all"):
                key = (x, slot, group)
                last[key] = max(last.get(key, 0.0), *times)
    return mean, last


def chunk_order(chunks):
    return list(range(chunks // 2, chunks)) + list(range(chunks // 2))


def time_line(chunks, last, pace):
    spots, crossings, link = [], [], [0.0, 0.0]
    order = chunk_order(chunks)
    ready = {key: time + 1.5 for key, time in last.items()}

    def cross(now, x):
        start = max(link[x], now)
        crossings.append((start, x, pace))
        link[x] = start + pace
        return link[x] + LAG

    def piece(now, cost, *what):
        spots.append((now, *what))
        return now + cost

    now, got = 0.0, {}
    for chunk in order:
        now = piece(max(now, ready[0, 0, "all"]), FRONT, 0, 0, chunk, "front")
        now = piece(now, BACK, 0, 0, chunk, "back")
        got[chunk] = cross(now, 0)
    first, now, back = now, 0.0, {}
    for chunk in order:
        now = piece(max(now, ready[1, 0, "all"], got[chunk]), FRONT, 1, 0, chunk, "front")
        now = piece(now, BACK, 1, 0, chunk, "back")
        back[chunk] = cross(now, 1)
    other, now, got = now, first, {}
    ahead = []
    for number, chunk in enumerate(order):
        now = piece(max(now, ready[0, 1, "q"], back[chunk]), FRONT, 0, 1, chunk, "front")
        ahead.append(chunk)
        following = order[number + 1] if number + 1 < len(order) else None
        waits = following is not None and max(now, back[following]) < ready[0, 1, "all"]
        if waits and len(ahead) < 2:
            continue
        for held in ahead:
            now = piece(max(now, ready[0, 1, "all"]), BACK, 0, 1, held, "back")
            if held >= chunks // 2:
                got[held] = cross(now, 0)
        ahead = []
    now = piece(max(now, ready[0, 2, "q"]), 2 * FRONT, 0, 2, 0, "front")
    end0 = piece(max(now, ready[0, 2, "all"]), 2 * BACK, 0, 2, 0, "back")
    now = other
    for chunk in order[: chunks // 2]:
        now = piece(max(now, ready[1, 1, "all"], got[chunk]), FRONT, 1, 1, chunk, "front")
        now = piece(now, BACK, 1, 1, chunk, "back")
    return spots, crossings, max(end0, now)


def make_plan(count_z, shard, streams, chunks, pace):
    crossings = []
    for _ in range(3):
        mean, last = arrivals(count_z, shard, streams, crossings)
        spots, crossings, end = time_line(chunks, last, pace)
    return mean, last, spots, end


def both(first, second):
    if first is None or second is None:
        return second if first is None else first
    return first & second


def under(when, action):
    if when is None:
        action()
    else:
        pl.when(when)(action)


class Place:
    def __init__(self, count_z):
        self.x = lax.axis_index("section")
        self.f = lax.axis_index("fsdp")
        self.p, self.y, self.z = self.f % 2, (self.f // 2) % 2, self.f // 4
        self.count_z = count_z

    def target(self, kind):
        if kind.startswith("x"):
            return {"section": 1 - self.x, "fsdp": self.f}
        step = {"y": 2 - 4 * self.y, "up": 4, "down": -4}.get(kind, 1 - 2 * self.p)
        return {"section": self.x, "fsdp": self.f + step}


class Gather:
    def __init__(self, stream, section, slot, held, place, send_sems, recv_sems, sent):
        self.stream, self.slot, self.held, self.place = stream, slot, held, place
        self.send_sems, self.recv_sems, self.sent = send_sems, recv_sems, sent
        self.here = place.x == section

    def valid(self, d):
        z = self.place.z + d
        return (z >= 0) & (z < self.place.count_z)

    def region(self, shift, rows, p, slot=None):
        columns = pl.ds(self.stream.low * LANES, self.stream.tiles * LANES)
        slot = self.slot if slot is None else slot
        return self.held.at[slot, self.place.z + shift, rows, p, :, columns]

    def copy(self, kind, ref, shift, to=None):
        slot = self.place.z + shift
        kind_no = KINDS.index(kind)
        recv_no = KINDS.index("up") if kind == "down" else kind_no
        number = self.stream.number
        return pltpu.make_async_remote_copy(
            src_ref=ref,
            dst_ref=ref if to is None else to,
            send_sem=self.send_sems.at[number, kind_no, slot],
            recv_sem=self.recv_sems.at[number, recv_no, slot],
            device_id=self.place.target(kind),
            device_id_type=MESH,
        )

    def rows(self, got, other=False):
        if got:
            return pl.ds(0, 2)
        return 1 - self.place.y if other else self.place.y

    def send(self, kind, ref, shift, when=None, to=None):
        when = both(self.here, when)
        under(when, lambda: self.copy(kind, ref, shift, to).start())
        self.sent.append(lambda: under(when, lambda: self.copy(kind, ref, shift, to).wait_send()))

    def wait(self, kind, ref, shift, when=None):
        under(both(self.here, when), lambda: self.copy(kind, ref, shift).wait_recv())

    def have(self, stage, shift, when=None):
        order, place = self.stream.order, self.place
        if stage == len(order):
            return
        ref = self.region(shift, self.rows("y" in order[:stage]), place.p)
        if order[stage] == "y":
            self.send("y", ref, shift, when)
            return
        self.send("up", ref, shift, place.z < place.count_z - 1)
        self.send("down", ref, shift, place.z > 0)
        self.have(stage + 1, shift)

    def shifts(self):
        pairs = [(-r, r) for r in range(1, self.place.count_z)]
        return [d for pair in pairs for d in pair]

    def rows_at(self, stage):
        order = self.stream.order
        if stage < 0:
            return self.rows(False)
        return self.rows("y" in order[:stage], other=order[stage] == "y")

    def forward(self, kind, stage, shift, when=None):
        if self.stream.mode == "forward":
            ref = self.region(shift, self.rows_at(stage), self.place.p)
            to = self.region(shift, self.rows_at(stage), self.place.p, 2)
            self.send("x_" + kind, ref, shift, when, to)

    def start(self):
        self.have(0, 0)
        self.forward("own", -1, 0)
        self.send("own", self.region(0, self.rows(False), self.place.p), 0)

    def give(self):
        ref = self.region(0, self.rows(False), self.place.p)
        to = self.region(0, self.rows(False), self.place.p, 2)
        self.send("x_own", ref, 0, None, to)

    def given(self):
        self.wait("x_own", self.region(0, self.rows(False), self.place.p), 0)
        self.start()

    def arrive(self, stage, shift):
        place = self.place
        dim = self.stream.order[stage]
        when = self.valid(shift) if shift else None
        kind = ("up" if shift < 0 else "down") if dim == "z" else dim
        ref = self.region(shift, self.rows_at(stage), place.p)
        self.wait(kind, ref, shift, when)
        if dim == "z":
            onward = place.z < place.count_z - 1 if shift < 0 else place.z > 0
            self.send(kind, ref, shift, both(when, onward))
        self.have(stage + 1, shift, when)
        self.forward(dim, stage, shift, when)
        self.send("core_" + dim, ref, shift, when)

    def mirror(self, stage, shift):
        kind = "own" if stage < 0 else self.stream.order[stage]
        when = self.valid(shift) if shift else None
        ref = self.region(shift, self.rows_at(stage), self.place.p)
        self.wait("x_" + kind, ref, shift, when)
        self.send("own" if stage < 0 else "core_" + kind, ref, shift, when)

    def from_partner(self):
        order, place = self.stream.order, self.place
        self.wait("own", self.region(0, self.rows(False), 1 - place.p), 0)
        for stage, dim in enumerate(order):
            spread = "z" in order[:stage]
            shifts = self.shifts() if dim == "z" else [0] + (self.shifts() if spread else [])
            for shift in shifts:
                ref = self.region(shift, self.rows_at(stage), 1 - place.p)
                self.wait("core_" + dim, ref, shift, self.valid(shift) if shift else None)


def greet(place):
    barrier = pltpu.get_barrier_semaphore()
    z, count_z = place.z, place.count_z

    def signal(kind):
        pl.semaphore_signal(barrier, inc=1, device_id=place.target(kind), device_id_type=MESH)

    signal("x")
    signal("y")
    signal("own")
    pl.when(z < count_z - 1)(lambda: signal("up"))
    pl.when(z > 0)(lambda: signal("down"))
    ends = jnp.where(z < count_z - 1, 1, 0) + jnp.where(z > 0, 1, 0)
    pl.semaphore_wait(barrier, 3 + ends)


def turned(tensor, cosine, sine_part):
    return tensor * cosine + pltpu.roll(tensor, tensor.shape[-1] // 2, 1) * sine_part


def thirds(tensor):
    parts = []
    for _ in range(3):
        part = tensor.astype(jnp.bfloat16)
        parts.append(part)
        tensor = tensor - part.astype(jnp.float32)
    return parts


def exact_scores(queries, keys):
    q1, q2, q3 = thirds(queries)
    k1, k2, k3 = thirds(keys)
    left = jnp.concatenate([q1, q2, q1, q2, q1, q3], axis=1)
    right = jnp.concatenate([k1, k1, k2, k2, k3, k1], axis=1)
    return lax.dot_general(
        left, right, (((1,), (1,)), ((), ())), preferred_element_type=jnp.float32
    )


def layer_pieces(depth, source, length, held, gains, biases, angles, scratch, store):
    normed, projected, context = scratch
    rows, width = normed.shape
    depth_rows = held.shape[1] * held.shape[2] * held.shape[3] * held.shape[4]
    group_size = HEADS // KV_HEADS
    kv_width = KV_HEADS * HEAD_DIM
    tile = 2 * LANES

    def weight(column):
        return held[depth, :, :, :, :, pl.ds(column, tile)].reshape(depth_rows, tile)

    def project():
        wide = source[...].astype(jnp.float32)
        inv_rms = lax.rsqrt(jnp.mean(wide * wide, axis=-1, keepdims=True) + EPS)
        normed[...] = (wide * inv_rms * gains[depth, 0]).astype(jnp.bfloat16)

        @pl.loop(0, projected.shape[1] // tile)
        def _(j):
            column = pl.multiple_of(j * tile, tile)
            block = jnp.dot(normed[...], weight(column), preferred_element_type=jnp.float32)
            projected[:, pl.ds(column, tile)] = block + biases[depth, 0, :, pl.ds(column, tile)]

    def attend():
        cosine, sine_part = angles[0], angles[1]
        shape = (group_size * length, length)
        query_at = lax.rem(lax.broadcasted_iota(jnp.int32, shape, 0), length)
        causal = query_at >= lax.broadcasted_iota(jnp.int32, shape, 1)

        @pl.loop(0, rows // length)
        def _(unit):
            there = pl.ds(pl.multiple_of(unit * length, length), length)
            for head in range(KV_HEADS):
                first = head * group_size * HEAD_DIM

                def columns(start):
                    return projected[there, start : start + HEAD_DIM]

                queries = jnp.concatenate(
                    [
                        turned(columns(first + h * HEAD_DIM), cosine, sine_part)
                        for h in range(group_size)
                    ],
                    axis=0,
                )
                keys = turned(columns(width + head * HEAD_DIM), cosine, sine_part)
                values = columns(width + kv_width + head * HEAD_DIM).astype(jnp.bfloat16)
                scores = exact_scores(queries, keys) * (1.0 / math.sqrt(HEAD_DIM))
                scores = jnp.where(causal, scores, -1e30)
                weights = jnp.exp(scores - jnp.max(scores, axis=-1, keepdims=True))
                total = jnp.sum(weights, axis=-1, keepdims=True)
                probability = (weights / total).astype(jnp.bfloat16)
                block = jnp.dot(probability, values, preferred_element_type=jnp.float32)
                block = block.astype(jnp.bfloat16)
                for h in range(group_size):
                    to = slice(first + h * HEAD_DIM, first + (h + 1) * HEAD_DIM)
                    context[there, to] = block[h * length : (h + 1) * length]

    def update():
        @pl.loop(0, width // tile)
        def _(j):
            column = pl.multiple_of(j * tile, tile)
            to = pl.ds(column, tile)
            block = jnp.dot(
                context[...], weight(projected.shape[1] + column), preferred_element_type=jnp.float32
            )
            wide = source[:, to].astype(jnp.float32)
            store[:, to] = (wide + block).astype(jnp.bfloat16)

    return project, attend, update


def section_kernel(
    count_z,
    length,
    chunks,
    hidden_ref,
    gain_ref,
    qkv_ref,
    bias_ref,
    out_ref,
    angles,
    result,
    held,
    gains,
    biases,
    before,
    after,
    normed,
    projected,
    context,
    send_sems,
    recv_sems,
    act_sems,
    small_sems,
    local_sems,
):
    place = Place(count_z)
    x, y, z, p = place.x, place.y, place.z, place.p
    qkv = qkv_ref.shape[-1]
    width = out_ref.shape[-1]
    rows = before.shape[1] // chunks
    half = chunks // 2
    on = [x == 0, x == 1]

    loads = [
        (None, pltpu.make_async_copy(gain_ref, gains.at[pl.ds(0, 2)], local_sems.at[0])),
        (None, pltpu.make_async_copy(bias_ref, biases.at[pl.ds(0, 2)], local_sems.at[1])),
        (on[0], pltpu.make_async_copy(hidden_ref, before.at[0], local_sems.at[2])),
    ]
    for depth in range(2):
        home = held.at[depth, z, y, p]
        parts = ((qkv_ref, pl.ds(0, qkv)), (out_ref, pl.ds(qkv, width)))
        for number, (ref, columns) in enumerate(parts):
            sem = local_sems.at[3 + 2 * depth + number]
            load = pltpu.make_async_copy(ref.at[depth, 0], home.at[:, columns], sem)
            loads.append((None, load))
    for when, load in loads:
        under(when, load.start)
    greet(place)
    for when, load in loads:
        under(when, load.wait)

    def small(array, number):
        return pltpu.make_async_remote_copy(
            src_ref=array.at[1],
            dst_ref=array.at[2],
            send_sem=small_sems.at[0, number],
            recv_sem=small_sems.at[1, number],
            device_id=place.target("x"),
            device_id_type=MESH,
        )

    smalls = [small(gains, 0), small(biases, 1)]
    sent = []
    for copy in smalls:
        pl.when(on[1])(copy.start)
    streams = make_streams(qkv, qkv + width)
    pace = 2 * rows * width / LINK
    mean, last, spots, _ = make_plan(count_z, held.shape[4], streams, chunks, pace)

    def gather(stream, section, slot):
        return Gather(stream, section, slot, held, place, send_sems, recv_sems, sent)

    plan, seen = [], {}
    for (section, kind, number, stage, shift), time in mean.items():
        stream = streams[number]
        slot = {"give": 1, "mirror": 2}.get(kind, stream.slot)
        if (section, number) not in seen:
            seen[section, number] = gather(stream, section, slot)
        part = seen[section, number]
        action = {
            "start": part.start,
            "give": part.give,
            "given": part.given,
            "arrive": partial(part.arrive, stage, shift),
            "mirror": partial(part.mirror, stage, shift),
        }[kind]
        plan.append((time, 1, len(plan), action))

    met = set()

    def partners(section, slot, groups):
        for (owner, number), part in seen.items():
            stream = streams[number]
            if part.slot != slot or stream.group not in groups or (owner, number) in met:
                continue
            if stream.mode == "across" and owner == 1:
                continue
            if owner == section:
                met.add((owner, number))
                part.from_partner()

    def crossing(slot, chunk, depth):
        here = pl.ds(chunk * rows, rows)
        return pltpu.make_async_remote_copy(
            src_ref=after.at[depth, here],
            dst_ref=before.at[slot, here],
            send_sem=act_sems.at[0, depth, chunk],
            recv_sem=act_sems.at[1, slot, chunk],
            device_id=place.target("x"),
            device_id_type=MESH,
        )

    def item(section, depth, chunk):
        count = rows * half if depth == 2 else rows
        here = pl.ds(chunk * rows, count)
        first = section == 0 and depth == 0
        final = depth == (2 if section == 0 else 1)
        source = before.at[depth, here]
        store = after.at[depth, here] if depth < 2 else None
        crosses = not final
        if final:
            store = result.at[pl.ds((chunk - half * section) * rows, count)]
        elif section == 0 and depth == 1 and chunk < half:
            store, crosses = before.at[2, here], False
        at = 0 if depth == 2 else (chunk % 2) * rows
        scratch = (
            normed.at[pl.ds(0, count)],
            projected.at[pl.ds(0, count)],
            context.at[pl.ds(at, count)],
        )
        pieces = layer_pieces(
            depth, source, length, held, gains, biases, angles, scratch, store
        )

        def begin():
            if not first and depth < 2:
                crossing(depth, chunk, 0).wait_recv()
            pieces[0]()

        def end():
            pieces[2]()
            if crosses:
                crossing(depth + section, chunk, depth).start()

        if crosses:
            sent.append(
                lambda: pl.when(on[section])(
                    lambda: crossing(depth + section, chunk, depth).wait_send()
                )
            )
        return begin, pieces[1], end

    items = {}
    for time, section, depth, chunk, kind in spots:
        key = (section, depth, chunk)
        if key not in items:
            items[key] = item(*key)
        begin, middle, end = items[key]
        whole = not (section == 0 and depth > 0)
        groups = "q" if kind == "front" and not whole else "qo"
        plan.append((time, 2, len(plan), partial(partners, section, depth, groups)))
        if kind == "front":
            if section == 0 and depth == 2:
                for copy in smalls:
                    plan.append((time, 2, len(plan), lambda c=copy: pl.when(on[0])(c.wait_recv)))
            plan.append((time, 3, len(plan), lambda f=begin, s=section: pl.when(on[s])(f)))
            plan.append((time + 2.0, 3, len(plan), lambda f=middle, s=section: pl.when(on[s])(f)))
        else:
            plan.append((time, 3, len(plan), lambda f=end, s=section: pl.when(on[s])(f)))
    for _, _, _, action in sorted(plan, key=lambda entry: entry[:3]):
        action()
    for copy in smalls:
        pl.when(on[1])(copy.wait_send)
    for finish in sent:
        finish()


def own_micros(sections, fsdp, hidden_in, norm_gain, qkv_weight, qkv_bias, out_weight):
    depths, _, shard, qkv = qkv_weight.shape
    micros, seqs, length, width = hidden_in.shape
    rows = micros * seqs * length
    owned = rows // sections
    count_z = fsdp // 4
    half_dim = HEAD_DIM // 2
    frequency = np.exp(np.arange(half_dim) * (-2.0 * math.log(THETA) / HEAD_DIM))
    turn = np.arange(length)[:, None] * frequency[None, :]
    cosine, sine_part = np.cos(turn), np.sin(turn)
    angles = np.stack(
        [
            np.concatenate([cosine, cosine], axis=-1),
            np.concatenate([-sine_part, sine_part], axis=-1),
        ]
    ).astype(np.float32)
    count = len(make_streams(qkv, qkv + width))
    sems = (count, len(KINDS), count_z)
    anywhere = pl.BlockSpec(memory_space=pl.ANY)
    in_vmem = pl.BlockSpec(memory_space=pltpu.VMEM)
    result = pl.pallas_call(
        partial(section_kernel, count_z, length, CHUNKS),
        out_shape=jax.ShapeDtypeStruct((owned, width), hidden_in.dtype),
        in_specs=[anywhere] * 5 + [in_vmem],
        out_specs=in_vmem,
        scratch_shapes=[
            pltpu.VMEM((3, count_z, 2, 2, shard, qkv + width), qkv_weight.dtype),
            pltpu.VMEM((3, 1, 1, width), jnp.float32),
            pltpu.VMEM((3, 1, 1, qkv), jnp.float32),
            pltpu.VMEM((3, rows, width), jnp.bfloat16),
            pltpu.VMEM((2, rows, width), jnp.bfloat16),
            pltpu.VMEM((owned, width), jnp.bfloat16),
            pltpu.VMEM((owned, qkv), jnp.float32),
            pltpu.VMEM((owned, width), jnp.bfloat16),
            pltpu.SemaphoreType.DMA(sems),
            pltpu.SemaphoreType.DMA(sems),
            pltpu.SemaphoreType.DMA((2, 3, CHUNKS)),
            pltpu.SemaphoreType.DMA((2, 2)),
            pltpu.SemaphoreType.DMA((7,)),
        ],
        compiler_params=pltpu.CompilerParams(
            collective_id=0, has_side_effects=True, vmem_limit_bytes=62 * 1024 * 1024
        ),
    )(
        hidden_in.reshape(rows, width),
        norm_gain.reshape(depths, 1, 1, width),
        qkv_weight,
        qkv_bias.reshape(depths, 1, 1, qkv),
        out_weight,
        jnp.asarray(angles),
    )
    return result.reshape(micros // sections, seqs, length, width)


def solution(mesh):
    in_specs = (
        P(None, "fsdp", None, None),
        P(None, "section", None),
        P(None, "section", "fsdp", None),
        P(None, "section", None),
        P(None, "section", "fsdp", None),
    )
    out_specs = P("section", "fsdp", None, None)
    whole_fits = mesh.shape["section"] == 2 and mesh.shape["fsdp"] % 4 == 0
    body = partial(own_micros, mesh.shape["section"], mesh.shape["fsdp"]) if whole_fits else per_device
    return jax.shard_map(
        body, mesh=mesh, in_specs=in_specs, out_specs=out_specs, check_vma=False
    )
```

```python
import heapq
from functools import partial
import math

import jax
import jax.numpy as jnp
import numpy as np
from jax import lax
from jax.experimental import pallas as pl
from jax.experimental.pallas import tpu as pltpu
from jax.sharding import PartitionSpec as P

HEADS = 12
KV_HEADS = 2
HEAD_DIM = 128


THETA = 1000000.0
EPS = 1.0


def as_sent(array):

    def short(part):
        return part.astype(jnp.bfloat16) if part.dtype == jnp.float32 else part

    return jax.tree.map(short, array)


def passed_along(block, axis, distance):
    devices = range(lax.axis_size(axis))
    route = [((i - distance) % len(devices), i) for i in devices]
    return lax.ppermute(block, axis, route)


def from_root(value, axis, source):
    kept = jnp.where(lax.axis_index(axis) == source, value, 0).astype(value.dtype)
    return lax.psum(kept, axis)


def rotate(tensor, cosine, sine_part):
    half_dim = tensor.shape[-1] // 2
    leading = tensor[..., :half_dim]
    second = tensor[..., half_dim:]
    return jnp.concatenate(
        [leading * cosine - second * sine_part, second * cosine + leading * sine_part], axis=-1
    )


def attend_layer(hidden, gain, w_qkv, bias, w_out):
    rows, length, width = hidden.shape
    group_size = HEADS // KV_HEADS
    kv_width = KV_HEADS * HEAD_DIM
    wide = hidden.astype(jnp.float32)
    inv_rms = lax.rsqrt(jnp.mean(wide * wide, axis=-1, keepdims=True) + EPS)
    normed = (wide * inv_rms * gain).astype(jnp.bfloat16)
    projected = (
        jnp.dot(normed.reshape(rows * length, width), w_qkv, preferred_element_type=jnp.float32)
        + bias
    )
    projected = projected.reshape(rows, length, width + 2 * kv_width)
    queries = projected[..., :width].reshape(rows, length, KV_HEADS, group_size, HEAD_DIM)
    key_rows = projected[..., width : width + kv_width].reshape(rows, length, KV_HEADS, HEAD_DIM)
    value_rows = (
        projected[..., width + kv_width :]
        .astype(jnp.bfloat16)
        .reshape(rows, length, KV_HEADS, HEAD_DIM)
    )
    half_dim = HEAD_DIM // 2
    frequency = jnp.exp(
        jnp.arange(half_dim, dtype=jnp.float32) * (-2.0 * math.log(THETA) / HEAD_DIM)
    )
    angles = jnp.arange(length, dtype=jnp.float32)[:, None] * frequency[None, :]
    cosine = jnp.cos(angles)
    sine_part = jnp.sin(angles)
    queries = rotate(queries, cosine[None, :, None, None, :], sine_part[None, :, None, None, :])
    key_rows = rotate(key_rows, cosine[None, :, None, :], sine_part[None, :, None, :])
    scores = jnp.einsum(
        "rqkgd,rpkd->rkgqp", queries, key_rows, precision=lax.Precision.HIGHEST
    ) / math.sqrt(HEAD_DIM)
    causal = jnp.arange(length)[:, None] >= jnp.arange(length)[None, :]
    scores = jnp.where(causal, scores, -1e30)
    row_max = jnp.max(scores, axis=-1, keepdims=True)
    weights = jnp.exp(scores - row_max)
    probability = (weights / jnp.sum(weights, axis=-1, keepdims=True)).astype(jnp.bfloat16)
    context = jnp.einsum(
        "rkgqp,rpkd->rqkgd", probability, value_rows, preferred_element_type=jnp.float32
    )
    context = context.reshape(rows, length, width).astype(jnp.bfloat16)
    update = jnp.dot(
        context.reshape(rows * length, width), w_out, preferred_element_type=jnp.float32
    )
    return (wide + update.reshape(rows, length, width)).astype(jnp.bfloat16)


def run_span(weight_pair, gain, bias, block_rows):
    return attend_layer(block_rows, gain, weight_pair[0], bias, weight_pair[1])


def vanish(block_rows):
    return jnp.zeros_like(block_rows)


def per_device(hidden_in, norm_gain, qkv_weight, qkv_bias, out_weight):
    sections = lax.axis_size("section")
    my_section = lax.axis_index("section")
    micro_count = hidden_in.shape[0]
    owned_count = micro_count // sections
    tick_count = 2 * micro_count + sections - 1
    span_gains = norm_gain[:, 0]
    biases = qkv_bias[:, 0]
    waiting = jnp.zeros_like(hidden_in)
    result = jnp.zeros_like(hidden_in)

    def make_tick(layers):
        branches = [vanish]
        for span_no in range(2):
            branches.append(
                partial(run_span, layers[span_no], span_gains[span_no], biases[span_no])
            )

        def advance(moment, state_pair):
            waiting, result = state_pair
            work_item = moment - my_section
            active = (work_item >= 0) & (work_item < 2 * micro_count)
            span_id = jnp.clip(work_item // micro_count, 0, 1)
            slot_id = jnp.mod(work_item, micro_count)
            entering = lax.dynamic_index_in_dim(hidden_in, slot_id, 0, keepdims=False)
            stored = lax.dynamic_index_in_dim(waiting, slot_id, 0, keepdims=False)
            block_in = jnp.where((span_id == 0) & (my_section == 0), entering, stored)
            selector = jnp.where(active, span_id + 1, 0)
            block_out = lax.switch(selector, branches, block_in)
            arrived = jax.tree.map(
                lambda part, own: part.astype(own.dtype),
                passed_along(as_sent(block_out), "section", 1),
                block_out,
            )
            sender = jnp.mod(my_section - 1, sections)
            sent_item = moment - sender
            accept = (
                (sent_item >= 0)
                & (sent_item < 2 * micro_count)
                & jnp.logical_not((sender == sections - 1) & (sent_item >= micro_count))
            )
            got_slot = jnp.mod(sent_item, micro_count)
            before = lax.dynamic_index_in_dim(waiting, got_slot, 0, keepdims=False)
            waiting = lax.dynamic_update_index_in_dim(
                waiting, jnp.where(accept, arrived, before), got_slot, 0
            )
            finish = moment - (sections - 1) - micro_count
            completed = (finish >= 0) & (finish < micro_count)
            final_slot = jnp.clip(finish, 0, micro_count - 1)
            previous = lax.dynamic_index_in_dim(result, final_slot, 0, keepdims=False)
            owned = completed & (my_section == sections - 1)
            result = lax.dynamic_update_index_in_dim(
                result, jnp.where(owned, block_out, previous), final_slot, 0
            )
            return (waiting, result)

        return advance

    first_pair = (
        lax.all_gather(qkv_weight[0, 0], "fsdp", axis=0, tiled=True),
        lax.all_gather(out_weight[0, 0], "fsdp", axis=0, tiled=True),
    )
    state_pair = lax.fori_loop(
        0, micro_count, make_tick((first_pair, first_pair)), (waiting, result)
    )
    second_pair = (
        lax.all_gather(qkv_weight[1, 0], "fsdp", axis=0, tiled=True),
        lax.all_gather(out_weight[1, 0], "fsdp", axis=0, tiled=True),
    )
    state_pair = lax.fori_loop(
        micro_count, tick_count, make_tick((first_pair, second_pair)), state_pair
    )
    waiting, result = state_pair
    result = from_root(result, "section", sections - 1)
    return lax.dynamic_slice_in_dim(result, my_section * owned_count, owned_count, 0)


MESH = pl.DeviceIdType.MESH
LANES = 128
KINDS = ("y", "up", "down", "own", "core_y", "core_z", "x_y", "x_z", "x_own")
LINK = 46650.0
SLOWER = 1.03
LAG = 1.9
CHUNKS = 4
COSTS = {"project": 2.1, "attend": 1.5, "update": 1.5}
FIRST = (
    (0.0, "zy", 12, "q"),
    (0.0, "zy", 12, "q"),
    (20.0, "yz", 1, "q"),
    (0.0, "yz", 3, "q"),
)
OTHER = (
    (0.0, "zy", 11, "q"),
    (0.0, "zy", 12, "q"),
    (0.0, "yz", 5, "q"),
)
SECOND = (
    (47.0, "zy", 13, "q"),
    (47.0, "yz", 3, "q"),
    (55.0, "zy", 6, "o"),
    (0.0, "zy", 6, "o", "relay"),
)
LAST = (
    (60.0, "zy", 13, "q"),
    (55.0, "zy", 3, "q"),
    (65.0, "zy", 8, "o"),
    (65.0, "yz", 4, "o"),
)
SHIFTS = {(0, 1): -2, (0, 0): 2}
BLEND = 0.4
EARLY = -2.0
ROUNDS = 4


class Stream:
    def __init__(self, number, slot, section, order, low, high, group, release, mode=None):
        self.number, self.slot, self.section, self.order = number, slot, section, order
        self.low, self.tiles, self.group = low, high - low, group
        self.release, self.mode = release, mode


def make_streams(projected, columns):
    split, total = projected // LANES, columns // LANES
    streams = []

    def add(table, slot, section):
        single = len({row[3] for row in table}) == 1
        for group, low, high in (("q", 0, split), ("o", split, total)):
            rows = [row for row in table if row[3] == group]
            if single:
                low, high = 0, total
            whole, done = sum(row[2] for row in rows), 0
            for row in rows:
                start = low + done * (high - low) // whole
                done += row[2]
                end = low + done * (high - low) // whole
                place = (2, 1) if len(row) > 4 else (slot, section)
                mode = row[4] if len(row) > 4 else None
                streams.append(
                    Stream(len(streams), *place, row[1], start, end, group, row[0], mode)
                )

    add(FIRST, 0, 0)
    add(OTHER, 0, 1)
    add(SECOND, 1, 0)
    add(LAST, 1, 1)
    return streams


def arrivals(count_z, shard, streams):
    free, heard, events, pushed = {}, {}, [], []
    unit = shard * LANES * 2 / LINK * SLOWER

    def push(now, *rest):
        heapq.heappush(events, (now, len(pushed), rest))
        pushed.append(now)

    def issue(now, x, z, kind, size, rest):
        done = max(now, free.get((x, z, kind), 0.0)) + size
        free[x, z, kind] = done
        push(done + LAG, *rest)

    def size_of(stream, stage):
        return stream.tiles * unit * (2 if "y" in stream.order[: max(stage, 0)] else 1)

    def have(now, x, stream, stage, source, z):
        if stage == len(stream.order):
            return
        size = size_of(stream, stage)
        if stream.order[stage] == "y":
            issue(now, x, z, "y", size, ("arrive", x, stream, stage, source, z))
            return
        if z < count_z - 1:
            issue(now, x, z, "up", size, ("arrive", x, stream, stage, source, z + 1))
        if z > 0:
            issue(now, x, z, "down", size, ("arrive", x, stream, stage, source, z - 1))
        have(now, x, stream, stage + 1, source, z)

    def note(now, x, kind, stream, stage, shift):
        heard.setdefault((x, kind, stream.number, stage, shift), []).append(now)

    for stream in streams:
        for z in range(count_z):
            push(stream.release, "start", stream.section, stream, -1, z, z)
    while events:
        now, _, (kind, x, stream, stage, source, z) = heapq.heappop(events)
        if kind == "start" and stream.mode == "relay":
            note(now, 1 - x, "give", stream, -1, 0)
            issue(now, 1 - x, z, "x", size_of(stream, -1), ("given", x, stream, -1, z, z))
            continue
        note(now, x, kind, stream, stage, source - z)
        if kind in ("start", "given"):
            have(now, x, stream, 0, source, z)
        if kind == "arrive":
            size = size_of(stream, stage)
            if stream.order[stage] == "z" and 0 < z < count_z - 1:
                way, to = ("up", z + 1) if source < z else ("down", z - 1)
                issue(now, x, z, way, size, ("arrive", x, stream, stage, source, to))
            have(now, x, stream, stage + 1, source, z)
            if stream.mode == "relay":
                issue(now, x, z, "x", size, ("mirror", 1 - x, stream, stage, source, z))
    return heard


def slot_of(kind, stream):
    return 1 if kind == "mirror" else stream.slot


def needs(streams, program):
    last = {}
    for time, x, what in program:
        if what[0] in ("arrive", "mirror"):
            stream = streams[what[1]]
            for group in (stream.group, "all"):
                key = (x, slot_of(what[0], stream), group)
                last[key] = max(last.get(key, 0.0), time)
    return last


def time_line(chunks, last, pace):
    spots, link = [], [0.0, 0.0]
    ready = {key: time + 1.0 for key, time in last.items()}

    def cross(now, x):
        link[x] = max(link[x], now) + pace
        return link[x] + LAG

    def front(now, x, depth, chunk):
        for kind in ("project", "attend"):
            spots.append((now, x, (kind, depth, chunk)))
            now += COSTS[kind]
        return now

    def back(now, x, depth, chunk):
        spots.append((now, x, ("update", depth, chunk)))
        return now + COSTS["update"]

    ends, got = [0.0, 0.0], {}
    for x, depth in ((0, 0), (1, 0), (0, 1), (1, 1)):
        now, sent, waiting = ends[x], {}, []
        for chunk in range(chunks):
            whole = ready[x, depth, "all"]
            first = ready.get((x, depth, "q"), whole)
            now = front(max(now, first, got.get(chunk, 0.0)), x, depth, chunk)
            waiting.append(chunk)
            if chunk + 1 < chunks and max(now, got.get(chunk + 1, 0.0)) < whole - 2.0:
                continue
            for held in waiting:
                now = back(max(now, whole), x, depth, held)
                sent[held] = cross(now, x)
            waiting = []
        ends[x], got = now, sent
    return spots


def run(count_z, shard, streams, program, chunks, pace):
    unit = shard * LANES * 2 / LINK * SLOWER
    devices = [(x, z) for x in (0, 1) for z in range(count_z)]
    lists = [[what for _, x, what in program if x == section] for section in (0, 1)]
    now = {d: 0.0 for d in devices}
    at = {d: 0 for d in devices}
    free, arrived, record = {}, {}, {}

    def size_of(stream, stage):
        return stream.tiles * unit * (2 if "y" in stream.order[: max(stage, 0)] else 1)

    def send(d, kind, size, to, *key):
        done = max(now[d], free.get((d, kind), 0.0)) + size
        free[d, kind] = done
        arrived[(to, *key)] = done + LAG

    def have(d, stream, stage, source):
        x, z = d
        if stage == len(stream.order):
            return
        size = size_of(stream, stage)
        if stream.order[stage] == "y":
            send(d, "y", size, d, "arrive", stream.number, stage, source)
            return
        if z < count_z - 1:
            send(d, "up", size, (x, z + 1), "arrive", stream.number, stage, source)
        if z > 0:
            send(d, "down", size, (x, z - 1), "arrive", stream.number, stage, source)
        have(d, stream, stage + 1, source)

    def wait(d, what, *key):
        if (d, *key) not in arrived:
            return False
        now[d] = max(now[d], arrived[(d, *key)])
        record.setdefault((d[0], what), []).append(arrived[(d, *key)])
        return True

    def piece(d, what):
        x, z = d
        kind, depth, chunk = what
        if kind == "project" and (x or depth):
            if not wait(d, what, "act", depth, chunk):
                return False
        else:
            record.setdefault((x, what), []).append(now[d])
        now[d] += COSTS[kind]
        if kind == "update":
            to = (0, depth + 1) if x else (1, depth)
            if depth + x < 2 or chunk < chunks // 2:
                send(d, "x", pace * SLOWER, (to[0], z), "act", to[1], chunk)
        return True

    def step(d, what):
        if what[0] in COSTS:
            return piece(d, what)
        x, z = d
        kind, number, stage, shift = what
        stream, source = streams[number], z + shift
        if not 0 <= source < count_z:
            return True
        if kind == "start":
            have(d, stream, 0, z)
            return True
        if kind == "give":
            send(d, "x", size_of(stream, -1), (1 - x, z), "given", number, -1, z)
            return True
        if not wait(d, what, kind, number, stage, source):
            return False
        size = size_of(stream, stage)
        if kind == "given":
            have(d, stream, 0, z)
        if kind == "arrive":
            if stream.order[stage] == "z":
                if source < z < count_z - 1:
                    send(d, "up", size, (x, z + 1), "arrive", number, stage, source)
                if 0 < z < source:
                    send(d, "down", size, (x, z - 1), "arrive", number, stage, source)
            have(d, stream, stage + 1, source)
            if stream.mode == "relay":
                send(d, "x", size, (1 - x, z), "mirror", number, stage, source)
        return True

    moved = True
    while moved:
        moved = False
        for d in devices:
            while at[d] < len(lists[d[0]]) and step(d, lists[d[0]][at[d]]):
                at[d] += 1
                moved = True
    if any(at[d] < len(lists[d[0]]) for d in devices):
        return 1e9, record
    tail = [t for key, t in arrived.items() if key[1:3] == ("act", 2)]
    return max(list(now.values()) + tail), record


def in_order(streams, moves, spots):
    last, ends, pieces = needs(streams, moves), {}, []
    for time, x, what in spots:
        kind, depth, _ = what
        group = "all" if kind == "update" else "q"
        time = max(time, last.get((x, depth, group), last[x, depth, "all"]) + 0.01)
        time = ends[x] = max(time, ends.get(x, 0.0) + 0.001)
        pieces.append((time, x, what))
    entries = [(time, 0, x, what) for time, x, what in moves]
    entries += [(time, 1, x, what) for time, x, what in pieces]
    return [(time, x, what) for time, _, x, what in sorted(entries, key=lambda e: e[:2])]


def make_plan(count_z, shard, streams, chunks, pace):
    heard = arrivals(count_z, shard, streams)
    moves = [(sum(t) / len(t), key[0], key[1:]) for key, t in heard.items()]
    spots = time_line(chunks, needs(streams, moves), pace)
    spots = [(t + SHIFTS.get((x, what[1]), 0.0), x, what) for t, x, what in spots]
    best, kept = 1e10, None
    for _ in range(ROUNDS):
        program = in_order(streams, moves, spots)
        end, record = run(count_z, shard, streams, program, chunks, pace)
        if end < best:
            best, kept = end, program

        def again(entry):
            time, x, what = entry
            seen = record.get((x, what))
            if not seen:
                return entry
            if what[0] in COSTS:
                return (min(seen) + EARLY, x, what)
            return ((1 - BLEND) * sum(seen) / len(seen) + BLEND * max(seen), x, what)

        moves = sorted(map(again, moves), key=lambda entry: entry[0])
        spots = list(map(again, spots))
    return best, kept


def both(first, second):
    if first is None or second is None:
        return second if first is None else first
    return first & second


def under(when, action):
    if when is None:
        action()
    else:
        pl.when(when)(action)


class Place:
    def __init__(self, count_z):
        self.x = lax.axis_index("section")
        self.f = lax.axis_index("fsdp")
        self.p, self.y, self.z = self.f % 2, (self.f // 2) % 2, self.f // 4
        self.count_z = count_z

    def target(self, kind):
        if kind.startswith("x"):
            return {"section": 1 - self.x, "fsdp": self.f}
        step = {"y": 2 - 4 * self.y, "up": 4, "down": -4}.get(kind, 1 - 2 * self.p)
        return {"section": self.x, "fsdp": self.f + step}


class Gather:
    def __init__(self, stream, section, slot, held, place, send_sems, recv_sems, sent):
        self.stream, self.slot, self.held, self.place = stream, slot, held, place
        self.send_sems, self.recv_sems, self.sent = send_sems, recv_sems, sent
        self.here = place.x == section

    def valid(self, d):
        z = self.place.z + d
        return (z >= 0) & (z < self.place.count_z)

    def region(self, shift, rows, p, slot=None):
        columns = pl.ds(self.stream.low * LANES, self.stream.tiles * LANES)
        slot = self.slot if slot is None else slot
        return self.held.at[slot, self.place.z + shift, rows, p, :, columns]

    def copy(self, kind, ref, shift, to=None):
        slot = self.place.z + shift
        kind_no = KINDS.index(kind)
        recv_no = KINDS.index("up") if kind == "down" else kind_no
        number = self.stream.number
        return pltpu.make_async_remote_copy(
            src_ref=ref,
            dst_ref=ref if to is None else to,
            send_sem=self.send_sems.at[number, kind_no, slot],
            recv_sem=self.recv_sems.at[number, recv_no, slot],
            device_id=self.place.target(kind),
            device_id_type=MESH,
        )

    def rows(self, got, other=False):
        if got:
            return pl.ds(0, 2)
        return 1 - self.place.y if other else self.place.y

    def send(self, kind, ref, shift, when=None, to=None):
        when = both(self.here, when)
        under(when, lambda: self.copy(kind, ref, shift, to).start())
        self.sent.append(lambda: under(when, lambda: self.copy(kind, ref, shift, to).wait_send()))

    def wait(self, kind, ref, shift, when=None):
        under(both(self.here, when), lambda: self.copy(kind, ref, shift).wait_recv())

    def have(self, stage, shift, when=None):
        order, place = self.stream.order, self.place
        if stage == len(order):
            return
        ref = self.region(shift, self.rows("y" in order[:stage]), place.p)
        if order[stage] == "y":
            self.send("y", ref, shift, when)
            return
        self.send("up", ref, shift, place.z < place.count_z - 1)
        self.send("down", ref, shift, place.z > 0)
        self.have(stage + 1, shift)

    def shifts(self):
        pairs = [(-r, r) for r in range(1, self.place.count_z)]
        return [d for pair in pairs for d in pair]

    def rows_at(self, stage):
        order = self.stream.order
        if stage < 0:
            return self.rows(False)
        return self.rows("y" in order[:stage], other=order[stage] == "y")

    def start(self):
        self.have(0, 0)
        self.send("own", self.region(0, self.rows(False), self.place.p), 0)

    def give(self):
        ref = self.region(0, self.rows(False), self.place.p)
        self.send("x_own", ref, 0, None, self.region(0, self.rows(False), self.place.p, 2))
        self.send("own", ref, 0)

    def given(self):
        self.wait("x_own", self.region(0, self.rows(False), self.place.p), 0)
        self.have(0, 0)

    def arrive(self, stage, shift):
        place = self.place
        dim = self.stream.order[stage]
        when = self.valid(shift) if shift else None
        kind = ("up" if shift < 0 else "down") if dim == "z" else dim
        ref = self.region(shift, self.rows_at(stage), place.p)
        self.wait(kind, ref, shift, when)
        if dim == "z":
            onward = place.z < place.count_z - 1 if shift < 0 else place.z > 0
            self.send(kind, ref, shift, both(when, onward))
        self.have(stage + 1, shift, when)
        if self.stream.mode == "relay":
            to = self.region(shift, self.rows_at(stage), place.p, 1)
            self.send("x_" + dim, ref, shift, when, to)
        else:
            self.send("core_" + dim, ref, shift, when)

    def mirror(self, stage, shift):
        dim = self.stream.order[stage]
        when = self.valid(shift) if shift else None
        ref = self.region(shift, self.rows_at(stage), self.place.p)
        self.wait("x_" + dim, ref, shift, when)
        self.send("core_" + dim, ref, shift, when)

    def from_partner(self):
        order, place = self.stream.order, self.place
        self.wait("own", self.region(0, self.rows(False), 1 - place.p), 0)
        for stage, dim in enumerate(order):
            spread = "z" in order[:stage]
            shifts = self.shifts() if dim == "z" else [0] + (self.shifts() if spread else [])
            for shift in shifts:
                ref = self.region(shift, self.rows_at(stage), 1 - place.p)
                self.wait("core_" + dim, ref, shift, self.valid(shift) if shift else None)


def greet(place):
    barrier = pltpu.get_barrier_semaphore()
    z, count_z = place.z, place.count_z

    def signal(kind):
        pl.semaphore_signal(barrier, inc=1, device_id=place.target(kind), device_id_type=MESH)

    signal("x")
    signal("y")
    signal("own")
    pl.when(z < count_z - 1)(lambda: signal("up"))
    pl.when(z > 0)(lambda: signal("down"))
    ends = jnp.where(z < count_z - 1, 1, 0) + jnp.where(z > 0, 1, 0)
    pl.semaphore_wait(barrier, 3 + ends)


def turned(tensor, cosine, sine_part):
    return tensor * cosine + pltpu.roll(tensor, tensor.shape[-1] // 2, 1) * sine_part


def thirds(tensor):
    parts = []
    for _ in range(3):
        part = tensor.astype(jnp.bfloat16)
        parts.append(part)
        tensor = tensor - part.astype(jnp.float32)
    return parts


def exact_scores(queries, keys):
    q1, q2, q3 = thirds(queries)
    k1, k2, k3 = thirds(keys)
    left = jnp.concatenate([q1, q2, q1, q2, q1, q3], axis=1)
    right = jnp.concatenate([k1, k1, k2, k2, k3, k1], axis=1)
    return lax.dot_general(
        left, right, (((1,), (1,)), ((), ())), preferred_element_type=jnp.float32
    )


def layer_pieces(depth, source, length, held, gains, biases, angles, scratch, store):
    normed, projected, context = scratch
    rows, width = normed.shape
    depth_rows = held.shape[1] * held.shape[2] * held.shape[3] * held.shape[4]
    group_size = HEADS // KV_HEADS
    kv_width = KV_HEADS * HEAD_DIM
    tile = 2 * LANES

    def weight(column):
        return held[depth, :, :, :, :, pl.ds(column, tile)].reshape(depth_rows, tile)

    def project():
        wide = source[...].astype(jnp.float32)
        inv_rms = lax.rsqrt(jnp.mean(wide * wide, axis=-1, keepdims=True) + EPS)
        normed[...] = (wide * inv_rms * gains[depth, 0]).astype(jnp.bfloat16)

        @pl.loop(0, projected.shape[1] // tile)
        def _(j):
            column = pl.multiple_of(j * tile, tile)
            block = jnp.dot(normed[...], weight(column), preferred_element_type=jnp.float32)
            projected[:, pl.ds(column, tile)] = block + biases[depth, 0, :, pl.ds(column, tile)]

    def attend():
        cosine, sine_part = angles[0], angles[1]
        shape = (group_size * length, length)
        query_at = lax.rem(lax.broadcasted_iota(jnp.int32, shape, 0), length)
        causal = query_at >= lax.broadcasted_iota(jnp.int32, shape, 1)

        @pl.loop(0, rows // length)
        def _(unit):
            there = pl.ds(pl.multiple_of(unit * length, length), length)
            for head in range(KV_HEADS):
                first = head * group_size * HEAD_DIM

                def columns(start):
                    return projected[there, start : start + HEAD_DIM]

                queries = jnp.concatenate(
                    [
                        turned(columns(first + h * HEAD_DIM), cosine, sine_part)
                        for h in range(group_size)
                    ],
                    axis=0,
                )
                keys = turned(columns(width + head * HEAD_DIM), cosine, sine_part)
                values = columns(width + kv_width + head * HEAD_DIM).astype(jnp.bfloat16)
                scores = exact_scores(queries, keys) * (1.0 / math.sqrt(HEAD_DIM))
                scores = jnp.where(causal, scores, -1e30)
                weights = jnp.exp(scores - jnp.max(scores, axis=-1, keepdims=True))
                total = jnp.sum(weights, axis=-1, keepdims=True)
                probability = (weights / total).astype(jnp.bfloat16)
                block = jnp.dot(probability, values, preferred_element_type=jnp.float32)
                block = block.astype(jnp.bfloat16)
                for h in range(group_size):
                    to = slice(first + h * HEAD_DIM, first + (h + 1) * HEAD_DIM)
                    context[there, to] = block[h * length : (h + 1) * length]

    def update():
        @pl.loop(0, width // tile)
        def _(j):
            column = pl.multiple_of(j * tile, tile)
            to = pl.ds(column, tile)
            block = jnp.dot(
                context[...], weight(projected.shape[1] + column), preferred_element_type=jnp.float32
            )
            wide = source[:, to].astype(jnp.float32)
            store[:, to] = (wide + block).astype(jnp.bfloat16)

    return project, attend, update


def section_kernel(
    count_z,
    length,
    chunks,
    hidden_ref,
    gain_ref,
    qkv_ref,
    bias_ref,
    out_ref,
    angles,
    result,
    held,
    gains,
    biases,
    before,
    after,
    normed,
    projected,
    context,
    send_sems,
    recv_sems,
    act_sems,
    local_sems,
):
    place = Place(count_z)
    x, y, z, p = place.x, place.y, place.z, place.p
    qkv = qkv_ref.shape[-1]
    width = out_ref.shape[-1]
    rows = before.shape[1] // chunks
    half = chunks // 2
    on = [x == 0, x == 1]

    loads = [
        (None, pltpu.make_async_copy(gain_ref, gains, local_sems.at[0])),
        (None, pltpu.make_async_copy(bias_ref, biases, local_sems.at[1])),
        (on[0], pltpu.make_async_copy(hidden_ref, before.at[0], local_sems.at[2])),
    ]
    for depth in range(2):
        home = held.at[depth, z, y, p]
        parts = ((qkv_ref, pl.ds(0, qkv)), (out_ref, pl.ds(qkv, width)))
        for number, (ref, columns) in enumerate(parts):
            sem = local_sems.at[3 + 2 * depth + number]
            load = pltpu.make_async_copy(ref.at[depth, 0], home.at[:, columns], sem)
            loads.append((None, load))
    for when, load in loads:
        under(when, load.start)
    greet(place)
    for when, load in loads:
        under(when, load.wait)

    sent = []
    streams = make_streams(qkv, qkv + width)
    pace = 2 * rows * width / LINK
    _, program = make_plan(count_z, held.shape[4], streams, chunks, pace)

    seen, met = {}, set()
    for _, section, what in program:
        if what[0] not in COSTS and (section, what[1]) not in seen:
            stream = streams[what[1]]
            slot = 1 if section == 0 and stream.mode else stream.slot
            seen[section, what[1]] = Gather(
                stream, section, slot, held, place, send_sems, recv_sems, sent
            )

    def partners(section, slot, groups):
        for (owner, number), part in seen.items():
            known = part.slot != slot or owner != section or (owner, number) in met
            if not known and (part.stream.group in groups or slot == 0):
                met.add((owner, number))
                part.from_partner()

    def crossing(slot, chunk, depth):
        here = pl.ds(chunk * rows, rows)
        return pltpu.make_async_remote_copy(
            src_ref=after.at[depth, here],
            dst_ref=before.at[slot, here],
            send_sem=act_sems.at[0, depth, chunk],
            recv_sem=act_sems.at[1, slot, chunk],
            device_id=place.target("x"),
            device_id_type=MESH,
        )

    def item(section, depth, chunk):
        here = pl.ds(chunk * rows, rows)
        final = section == 1 and depth == 1 and chunk >= half
        store = after.at[depth, here]
        if final:
            store = result.at[pl.ds((chunk - half) * rows, rows)]
        pieces = layer_pieces(
            depth,
            before.at[depth, here],
            length,
            held,
            gains,
            biases,
            angles,
            (normed, projected, context.at[here]),
            store,
        )

        def project():
            if section or depth:
                crossing(depth, chunk, 0).wait_recv()
            pieces[0]()

        def update():
            pieces[2]()
            if not final:
                crossing(depth + section, chunk, depth).start()

        if not final:
            sent.append(
                lambda: pl.when(on[section])(
                    lambda: crossing(depth + section, chunk, depth).wait_send()
                )
            )
        return {"project": project, "attend": pieces[1], "update": update}

    items = {}
    for _, section, what in program:
        kind, number = what[:2]
        if kind in COSTS:
            key = (section, *what[1:])
            if key not in items:
                items[key] = item(*key)
            partners(section, number, "qo" if kind == "update" else "q")
            pl.when(on[section])(items[key][kind])
            continue
        part = seen[section, number]
        if kind in ("arrive", "mirror"):
            getattr(part, kind)(*what[2:])
        else:
            getattr(part, kind)()

    @pl.when(on[0])
    def _():
        for chunk in range(half):
            here = pl.ds(chunk * rows, rows)
            crossing(2, chunk, 0).wait_recv()
            result[here] = before[2, here]

    for finish in sent:
        finish()


def own_micros(sections, fsdp, hidden_in, norm_gain, qkv_weight, qkv_bias, out_weight):
    depths, _, shard, qkv = qkv_weight.shape
    micros, seqs, length, width = hidden_in.shape
    rows = micros * seqs * length
    owned = rows // sections
    count_z = fsdp // 4
    half_dim = HEAD_DIM // 2
    frequency = np.exp(np.arange(half_dim) * (-2.0 * math.log(THETA) / HEAD_DIM))
    turn = np.arange(length)[:, None] * frequency[None, :]
    cosine, sine_part = np.cos(turn), np.sin(turn)
    angles = np.stack(
        [
            np.concatenate([cosine, cosine], axis=-1),
            np.concatenate([-sine_part, sine_part], axis=-1),
        ]
    ).astype(np.float32)
    count = len(make_streams(qkv, qkv + width))
    sems = (count, len(KINDS), count_z)
    anywhere = pl.BlockSpec(memory_space=pl.ANY)
    in_vmem = pl.BlockSpec(memory_space=pltpu.VMEM)
    result = pl.pallas_call(
        partial(section_kernel, count_z, length, CHUNKS),
        out_shape=jax.ShapeDtypeStruct((owned, width), hidden_in.dtype),
        in_specs=[anywhere] * 5 + [in_vmem],
        out_specs=in_vmem,
        scratch_shapes=[
            pltpu.VMEM((3, count_z, 2, 2, shard, qkv + width), qkv_weight.dtype),
            pltpu.VMEM((depths, 1, 1, width), jnp.float32),
            pltpu.VMEM((depths, 1, 1, qkv), jnp.float32),
            pltpu.VMEM((3, rows, width), jnp.bfloat16),
            pltpu.VMEM((2, rows, width), jnp.bfloat16),
            pltpu.VMEM((rows // CHUNKS, width), jnp.bfloat16),
            pltpu.VMEM((rows // CHUNKS, qkv), jnp.float32),
            pltpu.VMEM((rows, width), jnp.bfloat16),
            pltpu.SemaphoreType.DMA(sems),
            pltpu.SemaphoreType.DMA(sems),
            pltpu.SemaphoreType.DMA((2, 3, CHUNKS)),
            pltpu.SemaphoreType.DMA((7,)),
        ],
        compiler_params=pltpu.CompilerParams(
            collective_id=0, has_side_effects=True, vmem_limit_bytes=62 * 1024 * 1024
        ),
    )(
        hidden_in.reshape(rows, width),
        norm_gain.reshape(depths, 1, 1, width),
        qkv_weight,
        qkv_bias.reshape(depths, 1, 1, qkv),
        out_weight,
        jnp.asarray(angles),
    )
    return result.reshape(micros // sections, seqs, length, width)


def solution(mesh):
    in_specs = (
        P(None, "fsdp", None, None),
        P(None, "section", None),
        P(None, "section", "fsdp", None),
        P(None, "section", None),
        P(None, "section", "fsdp", None),
    )
    out_specs = P("section", "fsdp", None, None)
    whole_fits = mesh.shape["section"] == 2 and mesh.shape["fsdp"] % 4 == 0
    body = partial(own_micros, mesh.shape["section"], mesh.shape["fsdp"]) if whole_fits else per_device
    return jax.shard_map(
        body, mesh=mesh, in_specs=in_specs, out_specs=out_specs, check_vma=False
    )
```

```python
import heapq
from functools import partial
import math

import jax
import jax.numpy as jnp
import numpy as np
from jax import lax
from jax.experimental import pallas as pl
from jax.experimental.pallas import tpu as pltpu
from jax.sharding import PartitionSpec as P

HEADS = 12
KV_HEADS = 2
HEAD_DIM = 128


THETA = 1000000.0
EPS = 1.0


def as_sent(array):

    def short(part):
        return part.astype(jnp.bfloat16) if part.dtype == jnp.float32 else part

    return jax.tree.map(short, array)


def passed_along(block, axis, distance):
    devices = range(lax.axis_size(axis))
    route = [((i - distance) % len(devices), i) for i in devices]
    return lax.ppermute(block, axis, route)


def from_root(value, axis, source):
    kept = jnp.where(lax.axis_index(axis) == source, value, 0).astype(value.dtype)
    return lax.psum(kept, axis)


def rotate(tensor, cosine, sine_part):
    half_dim = tensor.shape[-1] // 2
    leading = tensor[..., :half_dim]
    second = tensor[..., half_dim:]
    return jnp.concatenate(
        [leading * cosine - second * sine_part, second * cosine + leading * sine_part], axis=-1
    )


def attend_layer(hidden, gain, w_qkv, bias, w_out):
    rows, length, width = hidden.shape
    group_size = HEADS // KV_HEADS
    kv_width = KV_HEADS * HEAD_DIM
    wide = hidden.astype(jnp.float32)
    inv_rms = lax.rsqrt(jnp.mean(wide * wide, axis=-1, keepdims=True) + EPS)
    normed = (wide * inv_rms * gain).astype(jnp.bfloat16)
    projected = (
        jnp.dot(normed.reshape(rows * length, width), w_qkv, preferred_element_type=jnp.float32)
        + bias
    )
    projected = projected.reshape(rows, length, width + 2 * kv_width)
    queries = projected[..., :width].reshape(rows, length, KV_HEADS, group_size, HEAD_DIM)
    key_rows = projected[..., width : width + kv_width].reshape(rows, length, KV_HEADS, HEAD_DIM)
    value_rows = (
        projected[..., width + kv_width :]
        .astype(jnp.bfloat16)
        .reshape(rows, length, KV_HEADS, HEAD_DIM)
    )
    half_dim = HEAD_DIM // 2
    frequency = jnp.exp(
        jnp.arange(half_dim, dtype=jnp.float32) * (-2.0 * math.log(THETA) / HEAD_DIM)
    )
    angles = jnp.arange(length, dtype=jnp.float32)[:, None] * frequency[None, :]
    cosine = jnp.cos(angles)
    sine_part = jnp.sin(angles)
    queries = rotate(queries, cosine[None, :, None, None, :], sine_part[None, :, None, None, :])
    key_rows = rotate(key_rows, cosine[None, :, None, :], sine_part[None, :, None, :])
    scores = jnp.einsum(
        "rqkgd,rpkd->rkgqp", queries, key_rows, precision=lax.Precision.HIGHEST
    ) / math.sqrt(HEAD_DIM)
    causal = jnp.arange(length)[:, None] >= jnp.arange(length)[None, :]
    scores = jnp.where(causal, scores, -1e30)
    row_max = jnp.max(scores, axis=-1, keepdims=True)
    weights = jnp.exp(scores - row_max)
    probability = (weights / jnp.sum(weights, axis=-1, keepdims=True)).astype(jnp.bfloat16)
    context = jnp.einsum(
        "rkgqp,rpkd->rqkgd", probability, value_rows, preferred_element_type=jnp.float32
    )
    context = context.reshape(rows, length, width).astype(jnp.bfloat16)
    update = jnp.dot(
        context.reshape(rows * length, width), w_out, preferred_element_type=jnp.float32
    )
    return (wide + update.reshape(rows, length, width)).astype(jnp.bfloat16)


def run_span(weight_pair, gain, bias, block_rows):
    return attend_layer(block_rows, gain, weight_pair[0], bias, weight_pair[1])


def vanish(block_rows):
    return jnp.zeros_like(block_rows)


def per_device(hidden_in, norm_gain, qkv_weight, qkv_bias, out_weight):
    sections = lax.axis_size("section")
    my_section = lax.axis_index("section")
    micro_count = hidden_in.shape[0]
    owned_count = micro_count // sections
    tick_count = 2 * micro_count + sections - 1
    span_gains = norm_gain[:, 0]
    biases = qkv_bias[:, 0]
    waiting = jnp.zeros_like(hidden_in)
    result = jnp.zeros_like(hidden_in)

    def make_tick(layers):
        branches = [vanish]
        for span_no in range(2):
            branches.append(
                partial(run_span, layers[span_no], span_gains[span_no], biases[span_no])
            )

        def advance(moment, state_pair):
            waiting, result = state_pair
            work_item = moment - my_section
            active = (work_item >= 0) & (work_item < 2 * micro_count)
            span_id = jnp.clip(work_item // micro_count, 0, 1)
            slot_id = jnp.mod(work_item, micro_count)
            entering = lax.dynamic_index_in_dim(hidden_in, slot_id, 0, keepdims=False)
            stored = lax.dynamic_index_in_dim(waiting, slot_id, 0, keepdims=False)
            block_in = jnp.where((span_id == 0) & (my_section == 0), entering, stored)
            selector = jnp.where(active, span_id + 1, 0)
            block_out = lax.switch(selector, branches, block_in)
            arrived = jax.tree.map(
                lambda part, own: part.astype(own.dtype),
                passed_along(as_sent(block_out), "section", 1),
                block_out,
            )
            sender = jnp.mod(my_section - 1, sections)
            sent_item = moment - sender
            accept = (
                (sent_item >= 0)
                & (sent_item < 2 * micro_count)
                & jnp.logical_not((sender == sections - 1) & (sent_item >= micro_count))
            )
            got_slot = jnp.mod(sent_item, micro_count)
            before = lax.dynamic_index_in_dim(waiting, got_slot, 0, keepdims=False)
            waiting = lax.dynamic_update_index_in_dim(
                waiting, jnp.where(accept, arrived, before), got_slot, 0
            )
            finish = moment - (sections - 1) - micro_count
            completed = (finish >= 0) & (finish < micro_count)
            final_slot = jnp.clip(finish, 0, micro_count - 1)
            previous = lax.dynamic_index_in_dim(result, final_slot, 0, keepdims=False)
            owned = completed & (my_section == sections - 1)
            result = lax.dynamic_update_index_in_dim(
                result, jnp.where(owned, block_out, previous), final_slot, 0
            )
            return (waiting, result)

        return advance

    first_pair = (
        lax.all_gather(qkv_weight[0, 0], "fsdp", axis=0, tiled=True),
        lax.all_gather(out_weight[0, 0], "fsdp", axis=0, tiled=True),
    )
    state_pair = lax.fori_loop(
        0, micro_count, make_tick((first_pair, first_pair)), (waiting, result)
    )
    second_pair = (
        lax.all_gather(qkv_weight[1, 0], "fsdp", axis=0, tiled=True),
        lax.all_gather(out_weight[1, 0], "fsdp", axis=0, tiled=True),
    )
    state_pair = lax.fori_loop(
        micro_count, tick_count, make_tick((first_pair, second_pair)), state_pair
    )
    waiting, result = state_pair
    result = from_root(result, "section", sections - 1)
    return lax.dynamic_slice_in_dim(result, my_section * owned_count, owned_count, 0)


MESH = pl.DeviceIdType.MESH
LANES = 128
KINDS = ("y", "up", "down", "own", "core_y", "core_z", "x_y", "x_z", "x_own")
LINK = 46650.0
SLOWER = 1.03
LAG = 1.9
CHUNKS = 4
COSTS = {"project": 1.9, "attend": 2.9, "update": 1.0}
PIECES = tuple(COSTS)
BEHIND = 2
FIRST = (
    (0.0, "zy", 12, "q"),
    (0.0, "zy", 12, "q"),
    (20.0, "yz", 1, "q"),
    (0.0, "yz", 3, "q"),
)
OTHER = (
    (0.0, "zy", 11, "q"),
    (0.0, "zy", 12, "q"),
    (0.0, "yz", 5, "q"),
)
SECOND = (
    (47.0, "zy", 13, "q"),
    (47.0, "yz", 3, "q"),
    (55.0, "zy", 6, "o"),
    (0.0, "zy", 6, "o", "relay"),
)
LAST = (
    (60.0, "zy", 13, "q"),
    (55.0, "zy", 3, "q"),
    (65.0, "zy", 8, "o"),
    (65.0, "yz", 4, "o"),
)
SHIFTS = {(0, 1): -2, (0, 0): 2}
BLEND = 0.4
EARLY = -2.0
ROUNDS = 4


class Stream:
    def __init__(self, number, slot, section, order, low, high, group, release, mode=None):
        self.number, self.slot, self.section, self.order = number, slot, section, order
        self.low, self.tiles, self.group = low, high - low, group
        self.release, self.mode = release, mode


def make_streams(projected, columns):
    split, total = projected // LANES, columns // LANES
    streams = []

    def add(table, slot, section):
        single = len({row[3] for row in table}) == 1
        for group, low, high in (("q", 0, split), ("o", split, total)):
            rows = [row for row in table if row[3] == group]
            if single:
                low, high = 0, total
            whole, done = sum(row[2] for row in rows), 0
            for row in rows:
                start = low + done * (high - low) // whole
                done += row[2]
                end = low + done * (high - low) // whole
                place = (2, 1) if len(row) > 4 else (slot, section)
                mode = row[4] if len(row) > 4 else None
                streams.append(
                    Stream(len(streams), *place, row[1], start, end, group, row[0], mode)
                )

    add(FIRST, 0, 0)
    add(OTHER, 0, 1)
    add(SECOND, 1, 0)
    add(LAST, 1, 1)
    return streams


def arrivals(count_z, shard, streams):
    free, heard, events, pushed = {}, {}, [], []
    unit = shard * LANES * 2 / LINK * SLOWER

    def push(now, *rest):
        heapq.heappush(events, (now, len(pushed), rest))
        pushed.append(now)

    def issue(now, x, z, kind, size, rest):
        done = max(now, free.get((x, z, kind), 0.0)) + size
        free[x, z, kind] = done
        push(done + LAG, *rest)

    def size_of(stream, stage):
        return stream.tiles * unit * (2 if "y" in stream.order[: max(stage, 0)] else 1)

    def have(now, x, stream, stage, source, z):
        if stage == len(stream.order):
            return
        size = size_of(stream, stage)
        if stream.order[stage] == "y":
            issue(now, x, z, "y", size, ("arrive", x, stream, stage, source, z))
            return
        if z < count_z - 1:
            issue(now, x, z, "up", size, ("arrive", x, stream, stage, source, z + 1))
        if z > 0:
            issue(now, x, z, "down", size, ("arrive", x, stream, stage, source, z - 1))
        have(now, x, stream, stage + 1, source, z)

    def note(now, x, kind, stream, stage, shift):
        heard.setdefault((x, kind, stream.number, stage, shift), []).append(now)

    for stream in streams:
        for z in range(count_z):
            push(stream.release, "start", stream.section, stream, -1, z, z)
    while events:
        now, _, (kind, x, stream, stage, source, z) = heapq.heappop(events)
        if kind == "start" and stream.mode == "relay":
            note(now, 1 - x, "give", stream, -1, 0)
            issue(now, 1 - x, z, "x", size_of(stream, -1), ("given", x, stream, -1, z, z))
            continue
        note(now, x, kind, stream, stage, source - z)
        if kind in ("start", "given"):
            have(now, x, stream, 0, source, z)
        if kind == "arrive":
            size = size_of(stream, stage)
            if stream.order[stage] == "z" and 0 < z < count_z - 1:
                way, to = ("up", z + 1) if source < z else ("down", z - 1)
                issue(now, x, z, way, size, ("arrive", x, stream, stage, source, to))
            have(now, x, stream, stage + 1, source, z)
            if stream.mode == "relay":
                issue(now, x, z, "x", size, ("mirror", 1 - x, stream, stage, source, z))
    return heard


def slot_of(kind, stream):
    return 1 if kind == "mirror" else stream.slot


def needs(streams, program):
    last = {}
    for time, x, what in program:
        if what[0] in ("arrive", "mirror"):
            stream = streams[what[1]]
            for group in (stream.group, "all"):
                key = (x, slot_of(what[0], stream), group)
                last[key] = max(last.get(key, 0.0), time)
    return last


def time_line(chunks, last, pace):
    spots, link = [], [0.0, 0.0]
    ready = {key: time + 1.0 for key, time in last.items()}

    def cross(now, x):
        link[x] = max(link[x], now) + pace
        return link[x] + LAG

    ends, got = [0.0, 0.0], {}
    for x, depth in ((0, 0), (1, 0), (0, 1), (1, 1)):
        now, sent = ends[x], {}
        whole = ready[x, depth, "all"]
        first = ready.get((x, depth, "q"), whole)
        for chunk in range(chunks):
            now = max(now, first, got.get(chunk, 0.0))
            for kind in PIECES:
                now = max(now, whole) if kind == "update" else now
                spots.append((now, x, (kind, depth, chunk)))
                now += COSTS[kind]
            sent[chunk] = cross(now, x)
        ends[x], got = now, sent
    return spots


def run(count_z, shard, streams, program, chunks, pace):
    unit = shard * LANES * 2 / LINK * SLOWER
    devices = [(x, z) for x in (0, 1) for z in range(count_z)]
    lists = [[what for _, x, what in program if x == section] for section in (0, 1)]
    now = {d: 0.0 for d in devices}
    at = {d: 0 for d in devices}
    free, arrived, record = {}, {}, {}

    def size_of(stream, stage):
        return stream.tiles * unit * (2 if "y" in stream.order[: max(stage, 0)] else 1)

    def send(d, kind, size, to, *key):
        done = max(now[d], free.get((d, kind), 0.0)) + size
        free[d, kind] = done
        arrived[(to, *key)] = done + LAG

    def have(d, stream, stage, source):
        x, z = d
        if stage == len(stream.order):
            return
        size = size_of(stream, stage)
        if stream.order[stage] == "y":
            send(d, "y", size, d, "arrive", stream.number, stage, source)
            return
        if z < count_z - 1:
            send(d, "up", size, (x, z + 1), "arrive", stream.number, stage, source)
        if z > 0:
            send(d, "down", size, (x, z - 1), "arrive", stream.number, stage, source)
        have(d, stream, stage + 1, source)

    def wait(d, what, *key):
        if (d, *key) not in arrived:
            return False
        now[d] = max(now[d], arrived[(d, *key)])
        record.setdefault((d[0], what), []).append(arrived[(d, *key)])
        return True

    def piece(d, what):
        x, z = d
        kind, depth, chunk = what
        if kind == "project" and (x or depth):
            if not wait(d, what, "act", depth, chunk):
                return False
        else:
            record.setdefault((x, what), []).append(now[d])
        now[d] += COSTS[kind]
        if kind == "update":
            to = (0, depth + 1) if x else (1, depth)
            if depth + x < 2 or chunk < chunks // 2:
                send(d, "x", pace * SLOWER, (to[0], z), "act", to[1], chunk)
        return True

    def step(d, what):
        if what[0] in COSTS:
            return piece(d, what)
        x, z = d
        kind, number, stage, shift = what
        stream, source = streams[number], z + shift
        if not 0 <= source < count_z:
            return True
        if kind == "start":
            have(d, stream, 0, z)
            return True
        if kind == "give":
            send(d, "x", size_of(stream, -1), (1 - x, z), "given", number, -1, z)
            return True
        if not wait(d, what, kind, number, stage, source):
            return False
        size = size_of(stream, stage)
        if kind == "given":
            have(d, stream, 0, z)
        if kind == "arrive":
            if stream.order[stage] == "z":
                if source < z < count_z - 1:
                    send(d, "up", size, (x, z + 1), "arrive", number, stage, source)
                if 0 < z < source:
                    send(d, "down", size, (x, z - 1), "arrive", number, stage, source)
            have(d, stream, stage + 1, source)
            if stream.mode == "relay":
                send(d, "x", size, (1 - x, z), "mirror", number, stage, source)
        return True

    moved = True
    while moved:
        moved = False
        for d in devices:
            while at[d] < len(lists[d[0]]) and step(d, lists[d[0]][at[d]]):
                at[d] += 1
                moved = True
    if any(at[d] < len(lists[d[0]]) for d in devices):
        return 1e9, record
    tail = [t for key, t in arrived.items() if key[1:3] == ("act", 2)]
    return max(list(now.values()) + tail), record


def in_order(streams, moves, spots):
    last, ends, pieces = needs(streams, moves), {}, []
    for time, x, what in sorted(spots, key=lambda e: (e[2][1], e[2][2], PIECES.index(e[2][0]))):
        kind, depth, _ = what
        group = "all" if kind == "update" else "q"
        time = max(time, last.get((x, depth, group), last[x, depth, "all"]) + 0.01)
        time = ends[x] = max(time, ends.get(x, 0.0) + 0.001)
        pieces.append((time, x, what))
    entries = [(time, 0, x, what) for time, x, what in moves]
    entries += [(time, 1, x, what) for time, x, what in pieces]
    return [(time, x, what) for time, _, x, what in sorted(entries, key=lambda e: e[:2])]


def make_plan(count_z, shard, streams, chunks, pace):
    heard = arrivals(count_z, shard, streams)
    moves = [(sum(t) / len(t), key[0], key[1:]) for key, t in heard.items()]
    spots = time_line(chunks, needs(streams, moves), pace)
    spots = [(t + SHIFTS.get((x, what[1]), 0.0), x, what) for t, x, what in spots]
    best, kept = 1e10, None
    for _ in range(ROUNDS):
        program = in_order(streams, moves, spots)
        end, record = run(count_z, shard, streams, program, chunks, pace)
        if end < best:
            best, kept = end, program

        def again(entry):
            time, x, what = entry
            seen = record.get((x, what))
            if not seen:
                return entry
            if what[0] in COSTS:
                return (min(seen) + EARLY, x, what)
            return ((1 - BLEND) * sum(seen) / len(seen) + BLEND * max(seen), x, what)

        moves = sorted(map(again, moves), key=lambda entry: entry[0])
        spots = list(map(again, spots))
    return best, kept


def both(first, second):
    if first is None or second is None:
        return second if first is None else first
    return first & second


def under(when, action):
    if when is None:
        action()
    else:
        pl.when(when)(action)


class Place:
    def __init__(self, count_z):
        self.x = lax.axis_index("section")
        self.f = lax.axis_index("fsdp")
        self.p, self.y, self.z = self.f % 2, (self.f // 2) % 2, self.f // 4
        self.count_z = count_z

    def target(self, kind):
        if kind.startswith("x"):
            return {"section": 1 - self.x, "fsdp": self.f}
        step = {"y": 2 - 4 * self.y, "up": 4, "down": -4}.get(kind, 1 - 2 * self.p)
        return {"section": self.x, "fsdp": self.f + step}


class Gather:
    def __init__(self, stream, section, slot, held, place, send_sems, recv_sems):
        self.stream, self.slot, self.held, self.place = stream, slot, held, place
        self.send_sems, self.recv_sems, self.finishing = send_sems, recv_sems, False
        self.here = place.x == section

    def valid(self, d):
        z = self.place.z + d
        return (z >= 0) & (z < self.place.count_z)

    def region(self, shift, rows, p, slot=None):
        columns = pl.ds(self.stream.low * LANES, self.stream.tiles * LANES)
        slot = self.slot if slot is None else slot
        return self.held.at[slot, self.place.z + shift, rows, p, :, columns]

    def copy(self, kind, ref, shift, to=None):
        slot = self.place.z + shift
        kind_no = KINDS.index(kind)
        recv_no = KINDS.index("up") if kind == "down" else kind_no
        number = self.stream.number
        return pltpu.make_async_remote_copy(
            src_ref=ref,
            dst_ref=ref if to is None else to,
            send_sem=self.send_sems.at[number, kind_no, slot],
            recv_sem=self.recv_sems.at[number, recv_no, slot],
            device_id=self.place.target(kind),
            device_id_type=MESH,
        )

    def rows(self, got, other=False):
        if got:
            return pl.ds(0, 2)
        return 1 - self.place.y if other else self.place.y

    def send(self, kind, ref, shift, when=None, to=None):
        copy = self.copy(kind, ref, shift, to)
        under(both(self.here, when), copy.wait_send if self.finishing else copy.start)

    def wait(self, kind, ref, shift, when=None):
        if not self.finishing:
            copy = self.copy(kind, ref, shift)
            under(both(self.here, when), copy.wait_recv)

    def have(self, stage, shift, when=None):
        order, place = self.stream.order, self.place
        if stage == len(order):
            return
        ref = self.region(shift, self.rows("y" in order[:stage]), place.p)
        if order[stage] == "y":
            self.send("y", ref, shift, when)
            return
        self.send("up", ref, shift, place.z < place.count_z - 1)
        self.send("down", ref, shift, place.z > 0)
        self.have(stage + 1, shift)

    def shifts(self):
        pairs = [(-r, r) for r in range(1, self.place.count_z)]
        return [d for pair in pairs for d in pair]

    def rows_at(self, stage):
        order = self.stream.order
        if stage < 0:
            return self.rows(False)
        return self.rows("y" in order[:stage], other=order[stage] == "y")

    def start(self):
        self.have(0, 0)
        self.send("own", self.region(0, self.rows(False), self.place.p), 0)

    def give(self):
        ref = self.region(0, self.rows(False), self.place.p)
        self.send("x_own", ref, 0, None, self.region(0, self.rows(False), self.place.p, 2))
        self.send("own", ref, 0)

    def given(self):
        self.wait("x_own", self.region(0, self.rows(False), self.place.p), 0)
        self.have(0, 0)

    def arrive(self, stage, shift):
        place = self.place
        dim = self.stream.order[stage]
        when = self.valid(shift) if shift else None
        kind = ("up" if shift < 0 else "down") if dim == "z" else dim
        ref = self.region(shift, self.rows_at(stage), place.p)
        self.wait(kind, ref, shift, when)
        if dim == "z":
            onward = place.z < place.count_z - 1 if shift < 0 else place.z > 0
            self.send(kind, ref, shift, both(when, onward))
        self.have(stage + 1, shift, when)
        if self.stream.mode == "relay":
            to = self.region(shift, self.rows_at(stage), place.p, 1)
            self.send("x_" + dim, ref, shift, when, to)
        else:
            self.send("core_" + dim, ref, shift, when)

    def mirror(self, stage, shift):
        dim = self.stream.order[stage]
        when = self.valid(shift) if shift else None
        ref = self.region(shift, self.rows_at(stage), self.place.p)
        self.wait("x_" + dim, ref, shift, when)
        self.send("core_" + dim, ref, shift, when)

    def from_partner(self):
        order, place = self.stream.order, self.place
        self.wait("own", self.region(0, self.rows(False), 1 - place.p), 0)
        for stage, dim in enumerate(order):
            spread = "z" in order[:stage]
            shifts = self.shifts() if dim == "z" else [0] + (self.shifts() if spread else [])
            for shift in shifts:
                ref = self.region(shift, self.rows_at(stage), 1 - place.p)
                self.wait("core_" + dim, ref, shift, self.valid(shift) if shift else None)


def greet(place):
    barrier = pltpu.get_barrier_semaphore()
    z, count_z = place.z, place.count_z

    def signal(kind):
        pl.semaphore_signal(barrier, inc=1, device_id=place.target(kind), device_id_type=MESH)

    signal("x")
    signal("y")
    signal("own")
    pl.when(z < count_z - 1)(lambda: signal("up"))
    pl.when(z > 0)(lambda: signal("down"))
    ends = jnp.where(z < count_z - 1, 1, 0) + jnp.where(z > 0, 1, 0)
    pl.semaphore_wait(barrier, 3 + ends)


def turned(tensor, cosine, sine_part):
    return tensor * cosine + pltpu.roll(tensor, tensor.shape[-1] // 2, 1) * sine_part


def thirds(tensor):
    parts = []
    for _ in range(3):
        part = tensor.astype(jnp.bfloat16)
        parts.append(part)
        tensor = tensor - part.astype(jnp.float32)
    return parts


def exact_scores(queries, keys):
    q1, q2, q3 = thirds(queries)
    k1, k2, k3 = thirds(keys)
    left = jnp.concatenate([q1, q2, q1, q2, q1, q3], axis=1)
    right = jnp.concatenate([k1, k1, k2, k2, k3, k1], axis=1)
    return lax.dot_general(
        left, right, (((1,), (1,)), ((), ())), preferred_element_type=jnp.float32
    )


def layer_pieces(depth, source, length, held, gains, biases, angles, scratch, store):
    normed, projected, context = scratch
    rows, width = normed.shape
    depth_rows = held.shape[1] * held.shape[2] * held.shape[3] * held.shape[4]
    group_size = HEADS // KV_HEADS
    kv_width = KV_HEADS * HEAD_DIM
    tile = 2 * LANES

    def weight(column):
        return held[depth, :, :, :, :, pl.ds(column, tile)].reshape(depth_rows, tile)

    def project():
        wide = source[...].astype(jnp.float32)
        inv_rms = lax.rsqrt(jnp.mean(wide * wide, axis=-1, keepdims=True) + EPS)
        normed[...] = (wide * inv_rms * gains[depth, 0]).astype(jnp.bfloat16)

        @pl.loop(0, projected.shape[1] // tile)
        def _(j):
            column = pl.multiple_of(j * tile, tile)
            block = jnp.dot(normed[...], weight(column), preferred_element_type=jnp.float32)
            projected[:, pl.ds(column, tile)] = block + biases[depth, 0, :, pl.ds(column, tile)]

    def attend():
        cosine, sine_part = angles[0], angles[1]
        shape = (group_size * length, length)
        query_at = lax.rem(lax.broadcasted_iota(jnp.int32, shape, 0), length)
        causal = query_at >= lax.broadcasted_iota(jnp.int32, shape, 1)

        @pl.loop(0, rows // length)
        def _(unit):
            there = pl.ds(pl.multiple_of(unit * length, length), length)
            for head in range(KV_HEADS):
                first = head * group_size * HEAD_DIM

                def columns(start):
                    return projected[there, start : start + HEAD_DIM]

                queries = jnp.concatenate(
                    [
                        turned(columns(first + h * HEAD_DIM), cosine, sine_part)
                        for h in range(group_size)
                    ],
                    axis=0,
                )
                keys = turned(columns(width + head * HEAD_DIM), cosine, sine_part)
                values = columns(width + kv_width + head * HEAD_DIM).astype(jnp.bfloat16)
                scores = exact_scores(queries, keys) * (1.0 / math.sqrt(HEAD_DIM))
                scores = jnp.where(causal, scores, -1e30)
                weights = jnp.exp(scores - jnp.max(scores, axis=-1, keepdims=True))
                total = jnp.sum(weights, axis=-1, keepdims=True)
                probability = (weights / total).astype(jnp.bfloat16)
                block = jnp.dot(probability, values, preferred_element_type=jnp.float32)
                block = block.astype(jnp.bfloat16)
                for h in range(group_size):
                    to = slice(first + h * HEAD_DIM, first + (h + 1) * HEAD_DIM)
                    context[there, to] = block[h * length : (h + 1) * length]

    def update():
        @pl.loop(0, width // tile)
        def _(j):
            column = pl.multiple_of(j * tile, tile)
            to = pl.ds(column, tile)
            block = jnp.dot(
                context[...], weight(projected.shape[1] + column), preferred_element_type=jnp.float32
            )
            wide = source[:, to].astype(jnp.float32)
            store[:, to] = (wide + block).astype(jnp.bfloat16)

    return project, attend, update


def section_kernel(
    count_z,
    length,
    chunks,
    hidden_ref,
    gain_ref,
    qkv_ref,
    bias_ref,
    out_ref,
    angles,
    result,
    held,
    gains,
    biases,
    before,
    after,
    normed,
    projected,
    context,
    send_sems,
    recv_sems,
    act_sems,
    local_sems,
):
    place = Place(count_z)
    x, y, z, p = place.x, place.y, place.z, place.p
    qkv = qkv_ref.shape[-1]
    width = out_ref.shape[-1]
    rows = before.shape[1] // chunks
    half = chunks // 2
    on = [x == 0, x == 1]

    loads = [
        (None, pltpu.make_async_copy(gain_ref, gains, local_sems.at[0])),
        (None, pltpu.make_async_copy(bias_ref, biases, local_sems.at[1])),
        (on[0], pltpu.make_async_copy(hidden_ref, before.at[0], local_sems.at[2])),
    ]
    for depth in range(2):
        home = held.at[depth, z, y, p]
        parts = ((qkv_ref, pl.ds(0, qkv)), (out_ref, pl.ds(qkv, width)))
        for number, (ref, columns) in enumerate(parts):
            sem = local_sems.at[3 + 2 * depth + number]
            load = pltpu.make_async_copy(ref.at[depth, 0], home.at[:, columns], sem)
            loads.append((None, load))
    for when, load in loads:
        under(when, load.start)
    greet(place)
    for when, load in loads:
        under(when, load.wait)

    streams = make_streams(qkv, qkv + width)
    pace = 2 * rows * width / LINK
    _, program = make_plan(count_z, held.shape[4], streams, chunks, pace)

    seen, met, moves = {}, set(), {}
    for _, section, what in program:
        if what[0] not in COSTS and (section, what[1]) not in seen:
            stream = streams[what[1]]
            slot = 1 if section == 0 and stream.mode else stream.slot
            seen[section, what[1]] = Gather(
                stream, section, slot, held, place, send_sems, recv_sems
            )

    def partners(section, slot, groups):
        found = []
        for (owner, number), part in seen.items():
            known = part.slot != slot or owner != section or (owner, number) in met
            if not known and (part.stream.group in groups or slot == 0):
                met.add((owner, number))
                found.append(part.from_partner)
        return found

    def move(section, what):
        part = seen[section, what[1]]
        rest = what[2:] if what[0] in ("arrive", "mirror") else ()
        return partial(getattr(part, what[0]), *rest)

    everything, segments, loose = [], {}, {0: [], 1: []}
    for _, section, what in program:
        kind, number = what[:2]
        if kind not in COSTS:
            everything.append(move(section, what))
            loose[section].append(everything[-1])
            continue
        spot = number * chunks + what[2] + BEHIND * section, PIECES.index(kind)
        loose[section] += partners(section, number, "qo" if kind == "update" else "q")
        segments.setdefault(spot, []).extend(loose[section])
        loose[section] = []

    def crossing(slot, chunk, depth):
        here = pl.ds(pl.multiple_of(chunk * rows, rows), rows)
        return pltpu.make_async_remote_copy(
            src_ref=after.at[depth, here],
            dst_ref=before.at[slot, here],
            send_sem=act_sems.at[0, depth, chunk],
            recv_sem=act_sems.at[1, slot, chunk],
            device_id=place.target("x"),
            device_id_type=MESH,
        )

    @pl.loop(0, 2 * chunks + BEHIND)
    def _(step):
        item = step - BEHIND * x
        present = (item >= 0) & (item < 2 * chunks)
        depth, chunk = item // chunks, item % chunks
        here = pl.ds(pl.multiple_of(chunk * rows, rows), rows)
        pieces = layer_pieces(
            depth,
            before.at[depth, here],
            length,
            held,
            gains,
            biases,
            angles,
            (normed, projected, context),
            after.at[depth, here],
        )
        for number, piece in enumerate(pieces):
            for (spot, place_in), actions in segments.items():
                if place_in == number and actions:
                    pl.when(step == spot)(lambda actions=actions: [f() for f in actions] and None)
            if number == 0:
                pl.when(present & (item + x > 0) & (item + chunks * x >= chunks))(
                    lambda: crossing(depth, chunk, 0).wait_recv()
                )
            pl.when(present)(piece)
        last = chunks + half + 2 * chunks * (1 - x)
        pl.when(present & (item < last))(lambda: crossing(depth + x, chunk, depth).start())

    for actions in loose.values():
        for action in actions:
            action()

    def pass_on(section, depth, chunk):
        return pl.when(on[section])(
            lambda: crossing(depth + section, chunk, depth).wait_send()
        )

    @pl.when(on[0])
    def _():
        for chunk in range(half):
            crossing(2, chunk, 0).wait_recv()
        result[...] = before[2, pl.ds(0, half * rows)]

    @pl.when(on[1])
    def _():
        result[...] = after[1, pl.ds(half * rows, half * rows)]

    for section in (0, 1):
        for number in range(2 * chunks if section == 0 else chunks + half):
            pass_on(section, number // chunks, number % chunks)
    for part in seen.values():
        part.finishing = True
    for action in everything:
        action()


def own_micros(sections, fsdp, hidden_in, norm_gain, qkv_weight, qkv_bias, out_weight):
    depths, _, shard, qkv = qkv_weight.shape
    micros, seqs, length, width = hidden_in.shape
    rows = micros * seqs * length
    owned = rows // sections
    count_z = fsdp // 4
    half_dim = HEAD_DIM // 2
    frequency = np.exp(np.arange(half_dim) * (-2.0 * math.log(THETA) / HEAD_DIM))
    turn = np.arange(length)[:, None] * frequency[None, :]
    cosine, sine_part = np.cos(turn), np.sin(turn)
    angles = np.stack(
        [
            np.concatenate([cosine, cosine], axis=-1),
            np.concatenate([-sine_part, sine_part], axis=-1),
        ]
    ).astype(np.float32)
    count = len(make_streams(qkv, qkv + width))
    sems = (count, len(KINDS), count_z)
    anywhere = pl.BlockSpec(memory_space=pl.ANY)
    in_vmem = pl.BlockSpec(memory_space=pltpu.VMEM)
    result = pl.pallas_call(
        partial(section_kernel, count_z, length, CHUNKS),
        out_shape=jax.ShapeDtypeStruct((owned, width), hidden_in.dtype),
        in_specs=[anywhere] * 5 + [in_vmem],
        out_specs=in_vmem,
        scratch_shapes=[
            pltpu.VMEM((3, count_z, 2, 2, shard, qkv + width), qkv_weight.dtype),
            pltpu.VMEM((depths, 1, 1, width), jnp.float32),
            pltpu.VMEM((depths, 1, 1, qkv), jnp.float32),
            pltpu.VMEM((3, rows, width), jnp.bfloat16),
            pltpu.VMEM((2, rows, width), jnp.bfloat16),
            pltpu.VMEM((rows // CHUNKS, width), jnp.bfloat16),
            pltpu.VMEM((rows // CHUNKS, qkv), jnp.float32),
            pltpu.VMEM((rows // CHUNKS, width), jnp.bfloat16),
            pltpu.SemaphoreType.DMA(sems),
            pltpu.SemaphoreType.DMA(sems),
            pltpu.SemaphoreType.DMA((2, 3, CHUNKS)),
            pltpu.SemaphoreType.DMA((7,)),
        ],
        compiler_params=pltpu.CompilerParams(
            collective_id=0, has_side_effects=True, vmem_limit_bytes=62 * 1024 * 1024
        ),
    )(
        hidden_in.reshape(rows, width),
        norm_gain.reshape(depths, 1, 1, width),
        qkv_weight,
        qkv_bias.reshape(depths, 1, 1, qkv),
        out_weight,
        jnp.asarray(angles),
    )
    return result.reshape(micros // sections, seqs, length, width)


def solution(mesh):
    in_specs = (
        P(None, "fsdp", None, None),
        P(None, "section", None),
        P(None, "section", "fsdp", None),
        P(None, "section", None),
        P(None, "section", "fsdp", None),
    )
    out_specs = P("section", "fsdp", None, None)
    whole_fits = mesh.shape["section"] == 2 and mesh.shape["fsdp"] % 4 == 0
    body = partial(own_micros, mesh.shape["section"], mesh.shape["fsdp"]) if whole_fits else per_device
    return jax.shard_map(
        body, mesh=mesh, in_specs=in_specs, out_specs=out_specs, check_vma=False
    )
```

```python
import heapq
from functools import partial
import math

import jax
import jax.numpy as jnp
import numpy as np
from jax import lax
from jax.experimental import pallas as pl
from jax.experimental.pallas import tpu as pltpu
from jax.sharding import PartitionSpec as P

HEADS = 12
KV_HEADS = 2
HEAD_DIM = 128


THETA = 1000000.0
EPS = 1.0


def as_sent(array):

    def short(part):
        return part.astype(jnp.bfloat16) if part.dtype == jnp.float32 else part

    return jax.tree.map(short, array)


def passed_along(block, axis, distance):
    devices = range(lax.axis_size(axis))
    route = [((i - distance) % len(devices), i) for i in devices]
    return lax.ppermute(block, axis, route)


def from_root(value, axis, source):
    kept = jnp.where(lax.axis_index(axis) == source, value, 0).astype(value.dtype)
    return lax.psum(kept, axis)


def rotate(tensor, cosine, sine_part):
    half_dim = tensor.shape[-1] // 2
    leading = tensor[..., :half_dim]
    second = tensor[..., half_dim:]
    return jnp.concatenate(
        [leading * cosine - second * sine_part, second * cosine + leading * sine_part], axis=-1
    )


def attend_layer(hidden, gain, w_qkv, bias, w_out):
    rows, length, width = hidden.shape
    group_size = HEADS // KV_HEADS
    kv_width = KV_HEADS * HEAD_DIM
    wide = hidden.astype(jnp.float32)
    inv_rms = lax.rsqrt(jnp.mean(wide * wide, axis=-1, keepdims=True) + EPS)
    normed = (wide * inv_rms * gain).astype(jnp.bfloat16)
    projected = (
        jnp.dot(normed.reshape(rows * length, width), w_qkv, preferred_element_type=jnp.float32)
        + bias
    )
    projected = projected.reshape(rows, length, width + 2 * kv_width)
    queries = projected[..., :width].reshape(rows, length, KV_HEADS, group_size, HEAD_DIM)
    key_rows = projected[..., width : width + kv_width].reshape(rows, length, KV_HEADS, HEAD_DIM)
    value_rows = (
        projected[..., width + kv_width :]
        .astype(jnp.bfloat16)
        .reshape(rows, length, KV_HEADS, HEAD_DIM)
    )
    half_dim = HEAD_DIM // 2
    frequency = jnp.exp(
        jnp.arange(half_dim, dtype=jnp.float32) * (-2.0 * math.log(THETA) / HEAD_DIM)
    )
    angles = jnp.arange(length, dtype=jnp.float32)[:, None] * frequency[None, :]
    cosine = jnp.cos(angles)
    sine_part = jnp.sin(angles)
    queries = rotate(queries, cosine[None, :, None, None, :], sine_part[None, :, None, None, :])
    key_rows = rotate(key_rows, cosine[None, :, None, :], sine_part[None, :, None, :])
    scores = jnp.einsum(
        "rqkgd,rpkd->rkgqp", queries, key_rows, precision=lax.Precision.HIGHEST
    ) / math.sqrt(HEAD_DIM)
    causal = jnp.arange(length)[:, None] >= jnp.arange(length)[None, :]
    scores = jnp.where(causal, scores, -1e30)
    row_max = jnp.max(scores, axis=-1, keepdims=True)
    weights = jnp.exp(scores - row_max)
    probability = (weights / jnp.sum(weights, axis=-1, keepdims=True)).astype(jnp.bfloat16)
    context = jnp.einsum(
        "rkgqp,rpkd->rqkgd", probability, value_rows, preferred_element_type=jnp.float32
    )
    context = context.reshape(rows, length, width).astype(jnp.bfloat16)
    update = jnp.dot(
        context.reshape(rows * length, width), w_out, preferred_element_type=jnp.float32
    )
    return (wide + update.reshape(rows, length, width)).astype(jnp.bfloat16)


def run_span(weight_pair, gain, bias, block_rows):
    return attend_layer(block_rows, gain, weight_pair[0], bias, weight_pair[1])


def vanish(block_rows):
    return jnp.zeros_like(block_rows)


def per_device(hidden_in, norm_gain, qkv_weight, qkv_bias, out_weight):
    sections = lax.axis_size("section")
    my_section = lax.axis_index("section")
    micro_count = hidden_in.shape[0]
    owned_count = micro_count // sections
    tick_count = 2 * micro_count + sections - 1
    span_gains = norm_gain[:, 0]
    biases = qkv_bias[:, 0]
    waiting = jnp.zeros_like(hidden_in)
    result = jnp.zeros_like(hidden_in)

    def make_tick(layers):
        branches = [vanish]
        for span_no in range(2):
            branches.append(
                partial(run_span, layers[span_no], span_gains[span_no], biases[span_no])
            )

        def advance(moment, state_pair):
            waiting, result = state_pair
            work_item = moment - my_section
            active = (work_item >= 0) & (work_item < 2 * micro_count)
            span_id = jnp.clip(work_item // micro_count, 0, 1)
            slot_id = jnp.mod(work_item, micro_count)
            entering = lax.dynamic_index_in_dim(hidden_in, slot_id, 0, keepdims=False)
            stored = lax.dynamic_index_in_dim(waiting, slot_id, 0, keepdims=False)
            block_in = jnp.where((span_id == 0) & (my_section == 0), entering, stored)
            selector = jnp.where(active, span_id + 1, 0)
            block_out = lax.switch(selector, branches, block_in)
            arrived = jax.tree.map(
                lambda part, own: part.astype(own.dtype),
                passed_along(as_sent(block_out), "section", 1),
                block_out,
            )
            sender = jnp.mod(my_section - 1, sections)
            sent_item = moment - sender
            accept = (
                (sent_item >= 0)
                & (sent_item < 2 * micro_count)
                & jnp.logical_not((sender == sections - 1) & (sent_item >= micro_count))
            )
            got_slot = jnp.mod(sent_item, micro_count)
            before = lax.dynamic_index_in_dim(waiting, got_slot, 0, keepdims=False)
            waiting = lax.dynamic_update_index_in_dim(
                waiting, jnp.where(accept, arrived, before), got_slot, 0
            )
            finish = moment - (sections - 1) - micro_count
            completed = (finish >= 0) & (finish < micro_count)
            final_slot = jnp.clip(finish, 0, micro_count - 1)
            previous = lax.dynamic_index_in_dim(result, final_slot, 0, keepdims=False)
            owned = completed & (my_section == sections - 1)
            result = lax.dynamic_update_index_in_dim(
                result, jnp.where(owned, block_out, previous), final_slot, 0
            )
            return (waiting, result)

        return advance

    first_pair = (
        lax.all_gather(qkv_weight[0, 0], "fsdp", axis=0, tiled=True),
        lax.all_gather(out_weight[0, 0], "fsdp", axis=0, tiled=True),
    )
    state_pair = lax.fori_loop(
        0, micro_count, make_tick((first_pair, first_pair)), (waiting, result)
    )
    second_pair = (
        lax.all_gather(qkv_weight[1, 0], "fsdp", axis=0, tiled=True),
        lax.all_gather(out_weight[1, 0], "fsdp", axis=0, tiled=True),
    )
    state_pair = lax.fori_loop(
        micro_count, tick_count, make_tick((first_pair, second_pair)), state_pair
    )
    waiting, result = state_pair
    result = from_root(result, "section", sections - 1)
    return lax.dynamic_slice_in_dim(result, my_section * owned_count, owned_count, 0)


MESH = pl.DeviceIdType.MESH
LANES = 128
KINDS = ("y", "up", "down", "own", "core_y", "core_z", "x_y", "x_z", "x_own")
LINK = 46650.0
SLOWER = 1.03
LAG = 1.9
CHUNKS = 4
COSTS = {"project": 1.9, "attend": 3.1, "update": 1.1}
PIECES = tuple(COSTS)
BEHIND = 0
FIRST = (
    (0.0, "zy", 13, "q"),
    (0.0, "yz", 3, "q"),
    (0.0, "zy", 10, "o"),
    (0.0, "yz", 2, "o"),
)
OTHER = (
    (0.0, "zy", 12, "q"),
    (0.0, "yz", 4, "q"),
    (0.0, "zy", 11, "o"),
    (0.0, "yz", 1, "o"),
)
SECOND = (
    (47.0, "zy", 13, "q"),
    (47.0, "yz", 3, "q"),
    (55.0, "zy", 5, "o"),
    (0.0, "zy", 7, "o", "relay"),
)
LAST = (
    (60.0, "zy", 15, "q"),
    (55.0, "yz", 1, "q"),
    (65.0, "zy", 4, "o"),
    (65.0, "zy", 4, "o"),
    (65.0, "yz", 4, "o"),
)
SHIFTS = {(0, 1): 0, (0, 0): 2, (1, 1): -4, (1, 0): 4}
BLEND = 1.0
EARLY = -2.0
ROUNDS = 4


class Stream:
    def __init__(self, number, slot, section, order, low, high, group, release, mode=None):
        self.number, self.slot, self.section, self.order = number, slot, section, order
        self.low, self.tiles, self.group = low, high - low, group
        self.release, self.mode = release, mode


def make_streams(projected, columns):
    split, total = projected // LANES, columns // LANES
    streams = []

    def add(table, slot, section):
        single = len({row[3] for row in table}) == 1
        for group, low, high in (("q", 0, split), ("o", split, total)):
            rows = [row for row in table if row[3] == group]
            if single:
                low, high = 0, total
            whole, done = sum(row[2] for row in rows), 0
            for row in rows:
                start = low + done * (high - low) // whole
                done += row[2]
                end = low + done * (high - low) // whole
                place = (2, 1) if len(row) > 4 else (slot, section)
                mode = row[4] if len(row) > 4 else None
                streams.append(
                    Stream(len(streams), *place, row[1], start, end, group, row[0], mode)
                )

    add(FIRST, 0, 0)
    add(OTHER, 0, 1)
    add(SECOND, 1, 0)
    add(LAST, 1, 1)
    return streams


def arrivals(count_z, shard, streams):
    free, heard, events, pushed = {}, {}, [], []
    unit = shard * LANES * 2 / LINK * SLOWER

    def push(now, *rest):
        heapq.heappush(events, (now, len(pushed), rest))
        pushed.append(now)

    def issue(now, x, z, kind, size, rest):
        done = max(now, free.get((x, z, kind), 0.0)) + size
        free[x, z, kind] = done
        push(done + LAG, *rest)

    def size_of(stream, stage):
        return stream.tiles * unit * (2 if "y" in stream.order[: max(stage, 0)] else 1)

    def have(now, x, stream, stage, source, z):
        if stage == len(stream.order):
            return
        size = size_of(stream, stage)
        if stream.order[stage] == "y":
            issue(now, x, z, "y", size, ("arrive", x, stream, stage, source, z))
            return
        if z < count_z - 1:
            issue(now, x, z, "up", size, ("arrive", x, stream, stage, source, z + 1))
        if z > 0:
            issue(now, x, z, "down", size, ("arrive", x, stream, stage, source, z - 1))
        have(now, x, stream, stage + 1, source, z)

    def note(now, x, kind, stream, stage, shift):
        heard.setdefault((x, kind, stream.number, stage, shift), []).append(now)

    for stream in streams:
        for z in range(count_z):
            push(stream.release, "start", stream.section, stream, -1, z, z)
    while events:
        now, _, (kind, x, stream, stage, source, z) = heapq.heappop(events)
        if kind == "start" and stream.mode == "relay":
            note(now, 1 - x, "give", stream, -1, 0)
            issue(now, 1 - x, z, "x", size_of(stream, -1), ("given", x, stream, -1, z, z))
            continue
        note(now, x, kind, stream, stage, source - z)
        if kind in ("start", "given"):
            have(now, x, stream, 0, source, z)
        if kind == "arrive":
            size = size_of(stream, stage)
            if stream.order[stage] == "z" and 0 < z < count_z - 1:
                way, to = ("up", z + 1) if source < z else ("down", z - 1)
                issue(now, x, z, way, size, ("arrive", x, stream, stage, source, to))
            have(now, x, stream, stage + 1, source, z)
            if stream.mode == "relay":
                issue(now, x, z, "x", size, ("mirror", 1 - x, stream, stage, source, z))
    return heard


def slot_of(kind, stream):
    return 1 if kind == "mirror" else stream.slot


def needs(streams, program):
    last = {}
    for time, x, what in program:
        if what[0] in ("arrive", "mirror"):
            stream = streams[what[1]]
            for group in (stream.group, "all"):
                key = (x, slot_of(what[0], stream), group)
                last[key] = max(last.get(key, 0.0), time)
    return last


def time_line(chunks, last, pace):
    spots, link = [], [0.0, 0.0]
    ready = {key: time + 1.0 for key, time in last.items()}

    def cross(now, x):
        link[x] = max(link[x], now) + pace
        return link[x] + LAG

    ends, got = [0.0, 0.0], {}
    for x, depth in ((0, 0), (1, 0), (0, 1), (1, 1)):
        now, sent = ends[x], {}
        whole = ready[x, depth, "all"]
        first = ready.get((x, depth, "q"), whole)
        for chunk in range(chunks):
            now = max(now, first, got.get(chunk, 0.0))
            for kind in PIECES:
                now = max(now, whole) if kind == "update" else now
                spots.append((now, x, (kind, depth, chunk)))
                now += COSTS[kind]
            sent[chunk] = cross(now, x)
        ends[x], got = now, sent
    return spots


def run(count_z, shard, streams, program, chunks, pace):
    unit = shard * LANES * 2 / LINK * SLOWER
    devices = [(x, z) for x in (0, 1) for z in range(count_z)]
    lists = [[what for _, x, what in program if x == section] for section in (0, 1)]
    now = {d: 0.0 for d in devices}
    at = {d: 0 for d in devices}
    free, arrived, record = {}, {}, {}

    def size_of(stream, stage):
        return stream.tiles * unit * (2 if "y" in stream.order[: max(stage, 0)] else 1)

    def send(d, kind, size, to, *key):
        done = max(now[d], free.get((d, kind), 0.0)) + size
        free[d, kind] = done
        arrived[(to, *key)] = done + LAG

    def have(d, stream, stage, source):
        x, z = d
        if stage == len(stream.order):
            return
        size = size_of(stream, stage)
        if stream.order[stage] == "y":
            send(d, "y", size, d, "arrive", stream.number, stage, source)
            return
        if z < count_z - 1:
            send(d, "up", size, (x, z + 1), "arrive", stream.number, stage, source)
        if z > 0:
            send(d, "down", size, (x, z - 1), "arrive", stream.number, stage, source)
        have(d, stream, stage + 1, source)

    def wait(d, what, *key):
        if (d, *key) not in arrived:
            return False
        now[d] = max(now[d], arrived[(d, *key)])
        record.setdefault((d[0], what), []).append(arrived[(d, *key)])
        return True

    def piece(d, what):
        x, z = d
        kind, depth, chunk = what
        if kind == "project" and (x or depth):
            if not wait(d, what, "act", depth, chunk):
                return False
        else:
            record.setdefault((x, what), []).append(now[d])
        now[d] += COSTS[kind]
        if kind == "update":
            to = (0, depth + 1) if x else (1, depth)
            if depth + x < 2 or chunk < chunks // 2:
                send(d, "x", pace * SLOWER, (to[0], z), "act", to[1], chunk)
        return True

    def step(d, what):
        if what[0] in COSTS:
            return piece(d, what)
        x, z = d
        kind, number, stage, shift = what
        stream, source = streams[number], z + shift
        if not 0 <= source < count_z:
            return True
        if kind == "start":
            have(d, stream, 0, z)
            return True
        if kind == "give":
            send(d, "x", size_of(stream, -1), (1 - x, z), "given", number, -1, z)
            return True
        if not wait(d, what, kind, number, stage, source):
            return False
        size = size_of(stream, stage)
        if kind == "given":
            have(d, stream, 0, z)
        if kind == "arrive":
            if stream.order[stage] == "z":
                if source < z < count_z - 1:
                    send(d, "up", size, (x, z + 1), "arrive", number, stage, source)
                if 0 < z < source:
                    send(d, "down", size, (x, z - 1), "arrive", number, stage, source)
            have(d, stream, stage + 1, source)
            if stream.mode == "relay":
                send(d, "x", size, (1 - x, z), "mirror", number, stage, source)
        return True

    moved = True
    while moved:
        moved = False
        for d in devices:
            while at[d] < len(lists[d[0]]) and step(d, lists[d[0]][at[d]]):
                at[d] += 1
                moved = True
    if any(at[d] < len(lists[d[0]]) for d in devices):
        return 1e9, record
    tail = [t for key, t in arrived.items() if key[1:3] == ("act", 2)]
    return max(list(now.values()) + tail), record


def in_order(streams, moves, spots):
    last, ends, pieces = needs(streams, moves), {}, []
    for time, x, what in sorted(spots, key=lambda e: (e[2][1], e[2][2], PIECES.index(e[2][0]))):
        kind, depth, _ = what
        group = "all" if kind == "update" else "q"
        time = max(time, last.get((x, depth, group), last[x, depth, "all"]) + 0.01)
        time = ends[x] = max(time, ends.get(x, 0.0) + 0.001)
        pieces.append((time, x, what))
    entries = [(time, 0, x, what) for time, x, what in moves]
    entries += [(time, 1, x, what) for time, x, what in pieces]
    return [(time, x, what) for time, _, x, what in sorted(entries, key=lambda e: e[:2])]


def make_plan(count_z, shard, streams, chunks, pace):
    heard = arrivals(count_z, shard, streams)
    moves = [(sum(t) / len(t), key[0], key[1:]) for key, t in heard.items()]
    spots = time_line(chunks, needs(streams, moves), pace)
    spots = [(t + SHIFTS.get((x, what[1]), 0.0), x, what) for t, x, what in spots]
    best, kept = 1e10, None
    for _ in range(ROUNDS):
        program = in_order(streams, moves, spots)
        end, record = run(count_z, shard, streams, program, chunks, pace)
        if end < best:
            best, kept = end, program

        def again(entry):
            time, x, what = entry
            seen = record.get((x, what))
            if not seen:
                return entry
            if what[0] in COSTS:
                return (min(seen) + EARLY, x, what)
            return ((1 - BLEND) * sum(seen) / len(seen) + BLEND * max(seen), x, what)

        moves = sorted(map(again, moves), key=lambda entry: entry[0])
        spots = list(map(again, spots))
    return best, kept


def both(first, second):
    if first is None or second is None:
        return second if first is None else first
    return first & second


def under(when, action):
    if when is None:
        action()
    else:
        pl.when(when)(action)


class Place:
    def __init__(self, count_z):
        self.x = lax.axis_index("section")
        self.f = lax.axis_index("fsdp")
        self.p, self.y, self.z = self.f % 2, (self.f // 2) % 2, self.f // 4
        self.count_z = count_z

    def target(self, kind):
        if kind.startswith("x"):
            return {"section": 1 - self.x, "fsdp": self.f}
        step = {"y": 2 - 4 * self.y, "up": 4, "down": -4}.get(kind, 1 - 2 * self.p)
        return {"section": self.x, "fsdp": self.f + step}


class Gather:
    def __init__(self, stream, section, slot, held, place, send_sems, recv_sems):
        self.stream, self.slot, self.held, self.place = stream, slot, held, place
        self.send_sems, self.recv_sems, self.finishing = send_sems, recv_sems, False
        self.here = place.x == section

    def valid(self, d):
        z = self.place.z + d
        return (z >= 0) & (z < self.place.count_z)

    def region(self, shift, rows, p, slot=None):
        columns = pl.ds(self.stream.low * LANES, self.stream.tiles * LANES)
        slot = self.slot if slot is None else slot
        return self.held.at[slot, self.place.z + shift, rows, p, :, columns]

    def copy(self, kind, ref, shift, to=None):
        slot = self.place.z + shift
        kind_no = KINDS.index(kind)
        recv_no = KINDS.index("up") if kind == "down" else kind_no
        number = self.stream.number
        return pltpu.make_async_remote_copy(
            src_ref=ref,
            dst_ref=ref if to is None else to,
            send_sem=self.send_sems.at[number, kind_no, slot],
            recv_sem=self.recv_sems.at[number, recv_no, slot],
            device_id=self.place.target(kind),
            device_id_type=MESH,
        )

    def rows(self, got, other=False):
        if got:
            return pl.ds(0, 2)
        return 1 - self.place.y if other else self.place.y

    def send(self, kind, ref, shift, when=None, to=None):
        copy = self.copy(kind, ref, shift, to)
        under(both(self.here, when), copy.wait_send if self.finishing else copy.start)

    def wait(self, kind, ref, shift, when=None):
        if not self.finishing:
            copy = self.copy(kind, ref, shift)
            under(both(self.here, when), copy.wait_recv)

    def have(self, stage, shift, when=None):
        order, place = self.stream.order, self.place
        if stage == len(order):
            return
        ref = self.region(shift, self.rows("y" in order[:stage]), place.p)
        if order[stage] == "y":
            self.send("y", ref, shift, when)
            return
        self.send("up", ref, shift, place.z < place.count_z - 1)
        self.send("down", ref, shift, place.z > 0)
        self.have(stage + 1, shift)

    def shifts(self):
        pairs = [(-r, r) for r in range(1, self.place.count_z)]
        return [d for pair in pairs for d in pair]

    def rows_at(self, stage):
        order = self.stream.order
        if stage < 0:
            return self.rows(False)
        return self.rows("y" in order[:stage], other=order[stage] == "y")

    def start(self):
        self.have(0, 0)
        self.send("own", self.region(0, self.rows(False), self.place.p), 0)

    def give(self):
        ref = self.region(0, self.rows(False), self.place.p)
        self.send("x_own", ref, 0, None, self.region(0, self.rows(False), self.place.p, 2))
        self.send("own", ref, 0)

    def given(self):
        self.wait("x_own", self.region(0, self.rows(False), self.place.p), 0)
        self.have(0, 0)

    def arrive(self, stage, shift):
        place = self.place
        dim = self.stream.order[stage]
        when = self.valid(shift) if shift else None
        kind = ("up" if shift < 0 else "down") if dim == "z" else dim
        ref = self.region(shift, self.rows_at(stage), place.p)
        self.wait(kind, ref, shift, when)
        if dim == "z":
            onward = place.z < place.count_z - 1 if shift < 0 else place.z > 0
            self.send(kind, ref, shift, both(when, onward))
        self.have(stage + 1, shift, when)
        if self.stream.mode == "relay":
            to = self.region(shift, self.rows_at(stage), place.p, 1)
            self.send("x_" + dim, ref, shift, when, to)
        else:
            self.send("core_" + dim, ref, shift, when)

    def mirror(self, stage, shift):
        dim = self.stream.order[stage]
        when = self.valid(shift) if shift else None
        ref = self.region(shift, self.rows_at(stage), self.place.p)
        self.wait("x_" + dim, ref, shift, when)
        self.send("core_" + dim, ref, shift, when)

    def from_partner(self):
        order, place = self.stream.order, self.place
        self.wait("own", self.region(0, self.rows(False), 1 - place.p), 0)
        for stage, dim in enumerate(order):
            spread = "z" in order[:stage]
            shifts = self.shifts() if dim == "z" else [0] + (self.shifts() if spread else [])
            for shift in shifts:
                ref = self.region(shift, self.rows_at(stage), 1 - place.p)
                self.wait("core_" + dim, ref, shift, self.valid(shift) if shift else None)


def greet(place):
    barrier = pltpu.get_barrier_semaphore()
    z, count_z = place.z, place.count_z

    def signal(kind):
        pl.semaphore_signal(barrier, inc=1, device_id=place.target(kind), device_id_type=MESH)

    signal("x")
    signal("y")
    signal("own")
    pl.when(z < count_z - 1)(lambda: signal("up"))
    pl.when(z > 0)(lambda: signal("down"))
    ends = jnp.where(z < count_z - 1, 1, 0) + jnp.where(z > 0, 1, 0)
    pl.semaphore_wait(barrier, 3 + ends)


def turned(tensor, cosine, sine_part):
    return tensor * cosine + pltpu.roll(tensor, tensor.shape[-1] // 2, 1) * sine_part


def thirds(tensor):
    parts = []
    for _ in range(3):
        part = tensor.astype(jnp.bfloat16)
        parts.append(part)
        tensor = tensor - part.astype(jnp.float32)
    return parts


def exact_scores(queries, keys):
    q1, q2, q3 = thirds(queries)
    k1, k2, k3 = thirds(keys)
    left = jnp.concatenate([q1, q2, q1, q2, q1, q3], axis=1)
    right = jnp.concatenate([k1, k1, k2, k2, k3, k1], axis=1)
    return lax.dot_general(
        left, right, (((1,), (1,)), ((), ())), preferred_element_type=jnp.float32
    )


def layer_pieces(depth, source, length, held, gains, biases, angles, scratch, store):
    normed, projected, context = scratch
    rows, width = normed.shape
    depth_rows = held.shape[1] * held.shape[2] * held.shape[3] * held.shape[4]
    group_size = HEADS // KV_HEADS
    kv_width = KV_HEADS * HEAD_DIM

    def halved(columns):
        return columns // 2 if columns % (2 * LANES) == 0 else LANES

    def weight(column, tile):
        return held[depth, :, :, :, :, pl.ds(column, tile)].reshape(depth_rows, tile)

    def project():
        wide = source[...].astype(jnp.float32)
        inv_rms = lax.rsqrt(jnp.mean(wide * wide, axis=-1, keepdims=True) + EPS)
        normed[...] = (wide * inv_rms * gains[depth, 0]).astype(jnp.bfloat16)

        tile = halved(projected.shape[1])

        @pl.loop(0, projected.shape[1] // tile)
        def _(j):
            column = pl.multiple_of(j * tile, tile)
            block = jnp.dot(normed[...], weight(column, tile), preferred_element_type=jnp.float32)
            projected[:, pl.ds(column, tile)] = block + biases[depth, 0, :, pl.ds(column, tile)]

    def attend():
        cosine, sine_part = angles[0], angles[1]
        shape = (group_size * length, length)
        query_at = lax.rem(lax.broadcasted_iota(jnp.int32, shape, 0), length)
        causal = query_at >= lax.broadcasted_iota(jnp.int32, shape, 1)

        @pl.loop(0, rows // length)
        def _(unit):
            there = pl.ds(pl.multiple_of(unit * length, length), length)
            for head in range(KV_HEADS):
                first = head * group_size * HEAD_DIM

                def columns(start):
                    return projected[there, start : start + HEAD_DIM]

                queries = jnp.concatenate(
                    [
                        turned(columns(first + h * HEAD_DIM), cosine, sine_part)
                        for h in range(group_size)
                    ],
                    axis=0,
                )
                keys = turned(columns(width + head * HEAD_DIM), cosine, sine_part)
                values = columns(width + kv_width + head * HEAD_DIM).astype(jnp.bfloat16)
                scores = exact_scores(queries, keys) * (1.0 / math.sqrt(HEAD_DIM))
                scores = jnp.where(causal, scores, -1e30)
                weights = jnp.exp(scores - jnp.max(scores, axis=-1, keepdims=True))
                total = jnp.sum(weights, axis=-1, keepdims=True)
                probability = (weights / total).astype(jnp.bfloat16)
                block = jnp.dot(probability, values, preferred_element_type=jnp.float32)
                block = block.astype(jnp.bfloat16)
                for h in range(group_size):
                    to = slice(first + h * HEAD_DIM, first + (h + 1) * HEAD_DIM)
                    context[there, to] = block[h * length : (h + 1) * length]

    def update():
        tile = halved(width)

        @pl.loop(0, width // tile)
        def _(j):
            column = pl.multiple_of(j * tile, tile)
            to = pl.ds(column, tile)
            block = jnp.dot(
                context[...], weight(projected.shape[1] + column, tile), preferred_element_type=jnp.float32
            )
            wide = source[:, to].astype(jnp.float32)
            store[:, to] = (wide + block).astype(jnp.bfloat16)

    return project, attend, update


def section_kernel(
    count_z,
    length,
    chunks,
    hidden_ref,
    gain_ref,
    qkv_ref,
    bias_ref,
    out_ref,
    angles,
    result,
    held,
    gains,
    biases,
    before,
    after,
    normed,
    projected,
    context,
    send_sems,
    recv_sems,
    act_sems,
    local_sems,
):
    place = Place(count_z)
    x, y, z, p = place.x, place.y, place.z, place.p
    qkv = qkv_ref.shape[-1]
    width = out_ref.shape[-1]
    rows = before.shape[1] // chunks
    half = chunks // 2
    on = [x == 0, x == 1]

    loads = [
        (None, pltpu.make_async_copy(gain_ref, gains, local_sems.at[0])),
        (None, pltpu.make_async_copy(bias_ref, biases, local_sems.at[1])),
        (on[0], pltpu.make_async_copy(hidden_ref, before.at[0], local_sems.at[2])),
    ]
    for depth in range(2):
        home = held.at[depth, z, y, p]
        parts = ((qkv_ref, pl.ds(0, qkv)), (out_ref, pl.ds(qkv, width)))
        for number, (ref, columns) in enumerate(parts):
            sem = local_sems.at[3 + 2 * depth + number]
            load = pltpu.make_async_copy(ref.at[depth, 0], home.at[:, columns], sem)
            loads.append((None, load))
    for when, load in loads:
        under(when, load.start)
    greet(place)
    for when, load in loads:
        under(when, load.wait)

    streams = make_streams(qkv, qkv + width)
    pace = 2 * rows * width / LINK
    _, program = make_plan(count_z, held.shape[4], streams, chunks, pace)

    seen, met, moves = {}, set(), {}
    for _, section, what in program:
        if what[0] not in COSTS and (section, what[1]) not in seen:
            stream = streams[what[1]]
            slot = 1 if section == 0 and stream.mode else stream.slot
            seen[section, what[1]] = Gather(
                stream, section, slot, held, place, send_sems, recv_sems
            )

    def partners(section, slot, groups):
        found = []
        for (owner, number), part in seen.items():
            known = part.slot != slot or owner != section or (owner, number) in met
            if not known and part.stream.group in groups:
                met.add((owner, number))
                found.append(part.from_partner)
        return found

    def move(section, what):
        part = seen[section, what[1]]
        rest = what[2:] if what[0] in ("arrive", "mirror") else ()
        return partial(getattr(part, what[0]), *rest)

    everything, segments, loose = [], {}, {0: [], 1: []}
    for _, section, what in program:
        kind, number = what[:2]
        if kind not in COSTS:
            everything.append(move(section, what))
            loose[section].append(everything[-1])
            continue
        spot = number * chunks + what[2] + BEHIND * section, PIECES.index(kind)
        loose[section] += partners(section, number, "qo" if kind == "update" else "q")
        segments.setdefault(spot, []).extend(loose[section])
        loose[section] = []

    def crossing(slot, chunk, depth):
        here = pl.ds(pl.multiple_of(chunk * rows, rows), rows)
        return pltpu.make_async_remote_copy(
            src_ref=after.at[depth, here],
            dst_ref=before.at[slot, here],
            send_sem=act_sems.at[0, depth, chunk],
            recv_sem=act_sems.at[1, slot, chunk],
            device_id=place.target("x"),
            device_id_type=MESH,
        )

    @pl.loop(0, 2 * chunks + BEHIND)
    def _(step):
        item = step - BEHIND * x
        present = (item >= 0) & (item < 2 * chunks)
        depth, chunk = item // chunks, item % chunks
        here = pl.ds(pl.multiple_of(chunk * rows, rows), rows)
        pieces = layer_pieces(
            depth,
            before.at[depth, here],
            length,
            held,
            gains,
            biases,
            angles,
            (normed, projected, context),
            after.at[depth, here],
        )
        for number, piece in enumerate(pieces):
            for (spot, place_in), actions in segments.items():
                if place_in == number and actions:
                    pl.when(step == spot)(lambda actions=actions: [f() for f in actions] and None)
            if number == 0:
                pl.when(present & (item + x > 0) & (item + chunks * x >= chunks))(
                    lambda: crossing(depth, chunk, 0).wait_recv()
                )
            pl.when(present)(piece)
        last = chunks + half + 2 * chunks * (1 - x)
        pl.when(present & (item < last))(lambda: crossing(depth + x, chunk, depth).start())

    for actions in loose.values():
        for action in actions:
            action()

    def pass_on(section, depth, chunk):
        return pl.when(on[section])(
            lambda: crossing(depth + section, chunk, depth).wait_send()
        )

    @pl.when(on[0])
    def _():
        for chunk in range(half):
            crossing(2, chunk, 0).wait_recv()
        result[...] = before[2, pl.ds(0, half * rows)]

    @pl.when(on[1])
    def _():
        result[...] = after[1, pl.ds(half * rows, half * rows)]

    for section in (0, 1):
        for number in range(2 * chunks if section == 0 else chunks + half):
            pass_on(section, number // chunks, number % chunks)
    for part in seen.values():
        part.finishing = True
    for action in everything:
        action()


def own_micros(sections, fsdp, hidden_in, norm_gain, qkv_weight, qkv_bias, out_weight):
    depths, _, shard, qkv = qkv_weight.shape
    micros, seqs, length, width = hidden_in.shape
    rows = micros * seqs * length
    owned = rows // sections
    count_z = fsdp // 4
    half_dim = HEAD_DIM // 2
    frequency = np.exp(np.arange(half_dim) * (-2.0 * math.log(THETA) / HEAD_DIM))
    turn = np.arange(length)[:, None] * frequency[None, :]
    cosine, sine_part = np.cos(turn), np.sin(turn)
    angles = np.stack(
        [
            np.concatenate([cosine, cosine], axis=-1),
            np.concatenate([-sine_part, sine_part], axis=-1),
        ]
    ).astype(np.float32)
    count = len(make_streams(qkv, qkv + width))
    sems = (count, len(KINDS), count_z)
    anywhere = pl.BlockSpec(memory_space=pl.ANY)
    in_vmem = pl.BlockSpec(memory_space=pltpu.VMEM)
    result = pl.pallas_call(
        partial(section_kernel, count_z, length, CHUNKS),
        out_shape=jax.ShapeDtypeStruct((owned, width), hidden_in.dtype),
        in_specs=[anywhere] * 5 + [in_vmem],
        out_specs=in_vmem,
        scratch_shapes=[
            pltpu.VMEM((3, count_z, 2, 2, shard, qkv + width), qkv_weight.dtype),
            pltpu.VMEM((depths, 1, 1, width), jnp.float32),
            pltpu.VMEM((depths, 1, 1, qkv), jnp.float32),
            pltpu.VMEM((3, rows, width), jnp.bfloat16),
            pltpu.VMEM((2, rows, width), jnp.bfloat16),
            pltpu.VMEM((rows // CHUNKS, width), jnp.bfloat16),
            pltpu.VMEM((rows // CHUNKS, qkv), jnp.float32),
            pltpu.VMEM((rows // CHUNKS, width), jnp.bfloat16),
            pltpu.SemaphoreType.DMA(sems),
            pltpu.SemaphoreType.DMA(sems),
            pltpu.SemaphoreType.DMA((2, 3, CHUNKS)),
            pltpu.SemaphoreType.DMA((7,)),
        ],
        compiler_params=pltpu.CompilerParams(
            collective_id=0, has_side_effects=True, vmem_limit_bytes=62 * 1024 * 1024
        ),
    )(
        hidden_in.reshape(rows, width),
        norm_gain.reshape(depths, 1, 1, width),
        qkv_weight,
        qkv_bias.reshape(depths, 1, 1, qkv),
        out_weight,
        jnp.asarray(angles),
    )
    return result.reshape(micros // sections, seqs, length, width)


def solution(mesh):
    in_specs = (
        P(None, "fsdp", None, None),
        P(None, "section", None),
        P(None, "section", "fsdp", None),
        P(None, "section", None),
        P(None, "section", "fsdp", None),
    )
    out_specs = P("section", "fsdp", None, None)
    whole_fits = mesh.shape["section"] == 2 and mesh.shape["fsdp"] % 4 == 0
    body = partial(own_micros, mesh.shape["section"], mesh.shape["fsdp"]) if whole_fits else per_device
    return jax.shard_map(
        body, mesh=mesh, in_specs=in_specs, out_specs=out_specs, check_vma=False
    )
```

```python
import heapq
from functools import partial
import math

import jax
import jax.numpy as jnp
import numpy as np
from jax import lax
from jax.experimental import pallas as pl
from jax.experimental.pallas import tpu as pltpu
from jax.sharding import PartitionSpec as P

HEADS = 12
KV_HEADS = 2
HEAD_DIM = 128


THETA = 1000000.0
EPS = 1.0


def as_sent(array):

    def short(part):
        return part.astype(jnp.bfloat16) if part.dtype == jnp.float32 else part

    return jax.tree.map(short, array)


def passed_along(block, axis, distance):
    devices = range(lax.axis_size(axis))
    route = [((i - distance) % len(devices), i) for i in devices]
    return lax.ppermute(block, axis, route)


def from_root(value, axis, source):
    kept = jnp.where(lax.axis_index(axis) == source, value, 0).astype(value.dtype)
    return lax.psum(kept, axis)


def rotate(tensor, cosine, sine_part):
    half_dim = tensor.shape[-1] // 2
    leading = tensor[..., :half_dim]
    second = tensor[..., half_dim:]
    return jnp.concatenate(
        [leading * cosine - second * sine_part, second * cosine + leading * sine_part], axis=-1
    )


def attend_layer(hidden, gain, w_qkv, bias, w_out):
    rows, length, width = hidden.shape
    group_size = HEADS // KV_HEADS
    kv_width = KV_HEADS * HEAD_DIM
    wide = hidden.astype(jnp.float32)
    inv_rms = lax.rsqrt(jnp.mean(wide * wide, axis=-1, keepdims=True) + EPS)
    normed = (wide * inv_rms * gain).astype(jnp.bfloat16)
    projected = (
        jnp.dot(normed.reshape(rows * length, width), w_qkv, preferred_element_type=jnp.float32)
        + bias
    )
    projected = projected.reshape(rows, length, width + 2 * kv_width)
    queries = projected[..., :width].reshape(rows, length, KV_HEADS, group_size, HEAD_DIM)
    key_rows = projected[..., width : width + kv_width].reshape(rows, length, KV_HEADS, HEAD_DIM)
    value_rows = (
        projected[..., width + kv_width :]
        .astype(jnp.bfloat16)
        .reshape(rows, length, KV_HEADS, HEAD_DIM)
    )
    half_dim = HEAD_DIM // 2
    frequency = jnp.exp(
        jnp.arange(half_dim, dtype=jnp.float32) * (-2.0 * math.log(THETA) / HEAD_DIM)
    )
    angles = jnp.arange(length, dtype=jnp.float32)[:, None] * frequency[None, :]
    cosine = jnp.cos(angles)
    sine_part = jnp.sin(angles)
    queries = rotate(queries, cosine[None, :, None, None, :], sine_part[None, :, None, None, :])
    key_rows = rotate(key_rows, cosine[None, :, None, :], sine_part[None, :, None, :])
    scores = jnp.einsum(
        "rqkgd,rpkd->rkgqp", queries, key_rows, precision=lax.Precision.HIGHEST
    ) / math.sqrt(HEAD_DIM)
    causal = jnp.arange(length)[:, None] >= jnp.arange(length)[None, :]
    scores = jnp.where(causal, scores, -1e30)
    row_max = jnp.max(scores, axis=-1, keepdims=True)
    weights = jnp.exp(scores - row_max)
    probability = (weights / jnp.sum(weights, axis=-1, keepdims=True)).astype(jnp.bfloat16)
    context = jnp.einsum(
        "rkgqp,rpkd->rqkgd", probability, value_rows, preferred_element_type=jnp.float32
    )
    context = context.reshape(rows, length, width).astype(jnp.bfloat16)
    update = jnp.dot(
        context.reshape(rows * length, width), w_out, preferred_element_type=jnp.float32
    )
    return (wide + update.reshape(rows, length, width)).astype(jnp.bfloat16)


def run_span(weight_pair, gain, bias, block_rows):
    return attend_layer(block_rows, gain, weight_pair[0], bias, weight_pair[1])


def vanish(block_rows):
    return jnp.zeros_like(block_rows)


def per_device(hidden_in, norm_gain, qkv_weight, qkv_bias, out_weight):
    sections = lax.axis_size("section")
    my_section = lax.axis_index("section")
    micro_count = hidden_in.shape[0]
    owned_count = micro_count // sections
    tick_count = 2 * micro_count + sections - 1
    span_gains = norm_gain[:, 0]
    biases = qkv_bias[:, 0]
    waiting = jnp.zeros_like(hidden_in)
    result = jnp.zeros_like(hidden_in)

    def make_tick(layers):
        branches = [vanish]
        for span_no in range(2):
            branches.append(
                partial(run_span, layers[span_no], span_gains[span_no], biases[span_no])
            )

        def advance(moment, state_pair):
            waiting, result = state_pair
            work_item = moment - my_section
            active = (work_item >= 0) & (work_item < 2 * micro_count)
            span_id = jnp.clip(work_item // micro_count, 0, 1)
            slot_id = jnp.mod(work_item, micro_count)
            entering = lax.dynamic_index_in_dim(hidden_in, slot_id, 0, keepdims=False)
            stored = lax.dynamic_index_in_dim(waiting, slot_id, 0, keepdims=False)
            block_in = jnp.where((span_id == 0) & (my_section == 0), entering, stored)
            selector = jnp.where(active, span_id + 1, 0)
            block_out = lax.switch(selector, branches, block_in)
            arrived = jax.tree.map(
                lambda part, own: part.astype(own.dtype),
                passed_along(as_sent(block_out), "section", 1),
                block_out,
            )
            sender = jnp.mod(my_section - 1, sections)
            sent_item = moment - sender
            accept = (
                (sent_item >= 0)
                & (sent_item < 2 * micro_count)
                & jnp.logical_not((sender == sections - 1) & (sent_item >= micro_count))
            )
            got_slot = jnp.mod(sent_item, micro_count)
            before = lax.dynamic_index_in_dim(waiting, got_slot, 0, keepdims=False)
            waiting = lax.dynamic_update_index_in_dim(
                waiting, jnp.where(accept, arrived, before), got_slot, 0
            )
            finish = moment - (sections - 1) - micro_count
            completed = (finish >= 0) & (finish < micro_count)
            final_slot = jnp.clip(finish, 0, micro_count - 1)
            previous = lax.dynamic_index_in_dim(result, final_slot, 0, keepdims=False)
            owned = completed & (my_section == sections - 1)
            result = lax.dynamic_update_index_in_dim(
                result, jnp.where(owned, block_out, previous), final_slot, 0
            )
            return (waiting, result)

        return advance

    first_pair = (
        lax.all_gather(qkv_weight[0, 0], "fsdp", axis=0, tiled=True),
        lax.all_gather(out_weight[0, 0], "fsdp", axis=0, tiled=True),
    )
    state_pair = lax.fori_loop(
        0, micro_count, make_tick((first_pair, first_pair)), (waiting, result)
    )
    second_pair = (
        lax.all_gather(qkv_weight[1, 0], "fsdp", axis=0, tiled=True),
        lax.all_gather(out_weight[1, 0], "fsdp", axis=0, tiled=True),
    )
    state_pair = lax.fori_loop(
        micro_count, tick_count, make_tick((first_pair, second_pair)), state_pair
    )
    waiting, result = state_pair
    result = from_root(result, "section", sections - 1)
    return lax.dynamic_slice_in_dim(result, my_section * owned_count, owned_count, 0)


MESH = pl.DeviceIdType.MESH
LANES = 128
KINDS = ("y", "up", "down", "own", "core_y", "core_z", "x_y", "x_z", "x_own")
LINK = 46650.0
SLOWER = 1.03
LAG = 1.9
CHUNKS = 4
COSTS = {"project": 1.9, "attend": 3.1, "update": 1.1}
PIECES = tuple(COSTS)
BEHIND = 0
FIRST = (
    (0.0, "zy", 13, "q"),
    (0.0, "yz", 3, "q"),
    (0.0, "zy", 10, "o"),
    (0.0, "yz", 2, "o"),
)
OTHER = (
    (0.0, "zy", 12, "q"),
    (0.0, "yz", 4, "q"),
    (0.0, "zy", 11, "o"),
    (0.0, "yz", 1, "o"),
)
SECOND = ((47.0, 'zy', 13, 'q'), (47.0, 'yz', 3, 'q'), (55.0, 'zy', 6, 'o'), (0.0, 'zy', 6, 'o', 'relay'))
LAST = (
    (60.0, "zy", 15, "q"),
    (55.0, "yz", 1, "q"),
    (65.0, "zy", 4, "o"),
    (65.0, "zy", 4, "o"),
    (65.0, "yz", 4, "o"),
)
SHIFTS = {(0, 1): 0, (0, 0): 2, (1, 1): -4, (1, 0): 4}
BLEND = 1.0
EARLY = 0.0
ROUNDS = 4


class Stream:
    def __init__(self, number, slot, section, order, low, high, group, release, mode=None):
        self.number, self.slot, self.section, self.order = number, slot, section, order
        self.low, self.tiles, self.group = low, high - low, group
        self.release, self.mode = release, mode


def make_streams(projected, columns):
    split, total = projected // LANES, columns // LANES
    streams = []

    def add(table, slot, section):
        single = len({row[3] for row in table}) == 1
        for group, low, high in (("q", 0, split), ("o", split, total)):
            rows = [row for row in table if row[3] == group]
            if single:
                low, high = 0, total
            whole, done = sum(row[2] for row in rows), 0
            for row in rows:
                start = low + done * (high - low) // whole
                done += row[2]
                end = low + done * (high - low) // whole
                place = (2, 1) if len(row) > 4 else (slot, section)
                mode = row[4] if len(row) > 4 else None
                streams.append(
                    Stream(len(streams), *place, row[1], start, end, group, row[0], mode)
                )

    add(FIRST, 0, 0)
    add(OTHER, 0, 1)
    add(SECOND, 1, 0)
    add(LAST, 1, 1)
    return streams


def arrivals(count_z, shard, streams):
    free, heard, events, pushed = {}, {}, [], []
    unit = shard * LANES * 2 / LINK * SLOWER

    def push(now, *rest):
        heapq.heappush(events, (now, len(pushed), rest))
        pushed.append(now)

    def issue(now, x, z, kind, size, rest):
        done = max(now, free.get((x, z, kind), 0.0)) + size
        free[x, z, kind] = done
        push(done + LAG, *rest)

    def size_of(stream, stage):
        return stream.tiles * unit * (2 if "y" in stream.order[: max(stage, 0)] else 1)

    def have(now, x, stream, stage, source, z):
        if stage == len(stream.order):
            return
        size = size_of(stream, stage)
        if stream.order[stage] == "y":
            issue(now, x, z, "y", size, ("arrive", x, stream, stage, source, z))
            return
        if z < count_z - 1:
            issue(now, x, z, "up", size, ("arrive", x, stream, stage, source, z + 1))
        if z > 0:
            issue(now, x, z, "down", size, ("arrive", x, stream, stage, source, z - 1))
        have(now, x, stream, stage + 1, source, z)

    def note(now, x, kind, stream, stage, shift):
        heard.setdefault((x, kind, stream.number, stage, shift), []).append(now)

    for stream in streams:
        for z in range(count_z):
            push(stream.release, "start", stream.section, stream, -1, z, z)
    while events:
        now, _, (kind, x, stream, stage, source, z) = heapq.heappop(events)
        if kind == "start" and stream.mode == "relay":
            note(now, 1 - x, "give", stream, -1, 0)
            issue(now, 1 - x, z, "x", size_of(stream, -1), ("given", x, stream, -1, z, z))
            continue
        note(now, x, kind, stream, stage, source - z)
        if kind in ("start", "given"):
            have(now, x, stream, 0, source, z)
        if kind == "arrive":
            size = size_of(stream, stage)
            if stream.order[stage] == "z" and 0 < z < count_z - 1:
                way, to = ("up", z + 1) if source < z else ("down", z - 1)
                issue(now, x, z, way, size, ("arrive", x, stream, stage, source, to))
            have(now, x, stream, stage + 1, source, z)
            if stream.mode == "relay":
                issue(now, x, z, "x", size, ("mirror", 1 - x, stream, stage, source, z))
    return heard


def slot_of(kind, stream):
    return 1 if kind == "mirror" else stream.slot


def needs(streams, program):
    last = {}
    for time, x, what in program:
        if what[0] in ("arrive", "mirror"):
            stream = streams[what[1]]
            for group in (stream.group, "all"):
                key = (x, slot_of(what[0], stream), group)
                last[key] = max(last.get(key, 0.0), time)
    return last


def time_line(chunks, last, pace):
    spots, link = [], [0.0, 0.0]
    ready = {key: time + 1.0 for key, time in last.items()}

    def cross(now, x):
        link[x] = max(link[x], now) + pace
        return link[x] + LAG

    ends, got = [0.0, 0.0], {}
    for x, depth in ((0, 0), (1, 0), (0, 1), (1, 1)):
        now, sent = ends[x], {}
        whole = ready[x, depth, "all"]
        first = ready.get((x, depth, "q"), whole)
        for chunk in range(chunks):
            now = max(now, first, got.get(chunk, 0.0))
            for kind in PIECES:
                now = max(now, whole) if kind == "update" else now
                spots.append((now, x, (kind, depth, chunk)))
                now += COSTS[kind]
            sent[chunk] = cross(now, x)
        ends[x], got = now, sent
    return spots


def run(count_z, shard, streams, program, chunks, pace):
    unit = shard * LANES * 2 / LINK * SLOWER
    devices = [(x, z) for x in (0, 1) for z in range(count_z)]
    lists = [[what for _, x, what in program if x == section] for section in (0, 1)]
    now = {d: 0.0 for d in devices}
    at = {d: 0 for d in devices}
    free, arrived, record = {}, {}, {}

    def size_of(stream, stage):
        return stream.tiles * unit * (2 if "y" in stream.order[: max(stage, 0)] else 1)

    def send(d, kind, size, to, *key):
        done = max(now[d], free.get((d, kind), 0.0)) + size
        free[d, kind] = done
        arrived[(to, *key)] = done + LAG

    def have(d, stream, stage, source):
        x, z = d
        if stage == len(stream.order):
            return
        size = size_of(stream, stage)
        if stream.order[stage] == "y":
            send(d, "y", size, d, "arrive", stream.number, stage, source)
            return
        if z < count_z - 1:
            send(d, "up", size, (x, z + 1), "arrive", stream.number, stage, source)
        if z > 0:
            send(d, "down", size, (x, z - 1), "arrive", stream.number, stage, source)
        have(d, stream, stage + 1, source)

    def wait(d, what, *key):
        if (d, *key) not in arrived:
            return False
        now[d] = max(now[d], arrived[(d, *key)])
        record.setdefault((d[0], what), []).append(arrived[(d, *key)])
        return True

    def piece(d, what):
        x, z = d
        kind, depth, chunk = what
        if kind == "project" and (x or depth):
            if not wait(d, what, "act", depth, chunk):
                return False
        else:
            record.setdefault((x, what), []).append(now[d])
        now[d] += COSTS[kind]
        if kind == "update":
            to = (0, depth + 1) if x else (1, depth)
            if depth + x < 2 or chunk < chunks // 2:
                send(d, "x", pace * SLOWER, (to[0], z), "act", to[1], chunk)
        return True

    def step(d, what):
        if what[0] in COSTS:
            return piece(d, what)
        x, z = d
        kind, number, stage, shift = what
        stream, source = streams[number], z + shift
        if not 0 <= source < count_z:
            return True
        if kind == "start":
            have(d, stream, 0, z)
            return True
        if kind == "give":
            send(d, "x", size_of(stream, -1), (1 - x, z), "given", number, -1, z)
            return True
        if not wait(d, what, kind, number, stage, source):
            return False
        size = size_of(stream, stage)
        if kind == "given":
            have(d, stream, 0, z)
        if kind == "arrive":
            if stream.order[stage] == "z":
                if source < z < count_z - 1:
                    send(d, "up", size, (x, z + 1), "arrive", number, stage, source)
                if 0 < z < source:
                    send(d, "down", size, (x, z - 1), "arrive", number, stage, source)
            have(d, stream, stage + 1, source)
            if stream.mode == "relay":
                send(d, "x", size, (1 - x, z), "mirror", number, stage, source)
        return True

    moved = True
    while moved:
        moved = False
        for d in devices:
            while at[d] < len(lists[d[0]]) and step(d, lists[d[0]][at[d]]):
                at[d] += 1
                moved = True
    if any(at[d] < len(lists[d[0]]) for d in devices):
        return 1e9, record
    tail = [t for key, t in arrived.items() if key[1:3] == ("act", 2)]
    return max(list(now.values()) + tail), record


def in_order(streams, moves, spots):
    last, ends, pieces = needs(streams, moves), {}, []
    for time, x, what in sorted(spots, key=lambda e: (e[2][1], e[2][2], PIECES.index(e[2][0]))):
        kind, depth, _ = what
        group = "all" if kind == "update" else "q"
        time = max(time, last.get((x, depth, group), last[x, depth, "all"]) + 0.01)
        time = ends[x] = max(time, ends.get(x, 0.0) + 0.001)
        pieces.append((time, x, what))
    entries = [(time, 0, x, what) for time, x, what in moves]
    entries += [(time, 1, x, what) for time, x, what in pieces]
    return [(time, x, what) for time, _, x, what in sorted(entries, key=lambda e: e[:2])]


def make_plan(count_z, shard, streams, chunks, pace):
    heard = arrivals(count_z, shard, streams)
    moves = [(sum(t) / len(t), key[0], key[1:]) for key, t in heard.items()]
    spots = time_line(chunks, needs(streams, moves), pace)
    spots = [(t + SHIFTS.get((x, what[1]), 0.0), x, what) for t, x, what in spots]
    best, kept = 1e10, None
    for _ in range(ROUNDS):
        program = in_order(streams, moves, spots)
        end, record = run(count_z, shard, streams, program, chunks, pace)
        if end < best:
            best, kept = end, program

        def again(entry):
            time, x, what = entry
            seen = record.get((x, what))
            if not seen:
                return entry
            if what[0] in COSTS:
                return (min(seen) + EARLY, x, what)
            return ((1 - BLEND) * sum(seen) / len(seen) + BLEND * max(seen), x, what)

        moves = sorted(map(again, moves), key=lambda entry: entry[0])
        spots = list(map(again, spots))
    return best, kept


def both(first, second):
    if first is None or second is None:
        return second if first is None else first
    return first & second


def under(when, action):
    if when is None:
        action()
    else:
        pl.when(when)(action)


class Place:
    def __init__(self, count_z):
        self.x = lax.axis_index("section")
        self.f = lax.axis_index("fsdp")
        self.p, self.y, self.z = self.f % 2, (self.f // 2) % 2, self.f // 4
        self.count_z = count_z

    def target(self, kind):
        if kind.startswith("x"):
            return {"section": 1 - self.x, "fsdp": self.f}
        step = {"y": 2 - 4 * self.y, "up": 4, "down": -4}.get(kind, 1 - 2 * self.p)
        return {"section": self.x, "fsdp": self.f + step}


class Gather:
    def __init__(self, stream, section, slot, held, place, send_sems, recv_sems):
        self.stream, self.slot, self.held, self.place = stream, slot, held, place
        self.send_sems, self.recv_sems, self.finishing = send_sems, recv_sems, False
        self.here = place.x == section

    def valid(self, d):
        z = self.place.z + d
        return (z >= 0) & (z < self.place.count_z)

    def region(self, shift, rows, p, slot=None):
        columns = pl.ds(self.stream.low * LANES, self.stream.tiles * LANES)
        slot = self.slot if slot is None else slot
        return self.held.at[slot, self.place.z + shift, rows, p, :, columns]

    def copy(self, kind, ref, shift, to=None):
        slot = self.place.z + shift
        kind_no = KINDS.index(kind)
        recv_no = KINDS.index("up") if kind == "down" else kind_no
        number = self.stream.number
        return pltpu.make_async_remote_copy(
            src_ref=ref,
            dst_ref=ref if to is None else to,
            send_sem=self.send_sems.at[number, kind_no, slot],
            recv_sem=self.recv_sems.at[number, recv_no, slot],
            device_id=self.place.target(kind),
            device_id_type=MESH,
        )

    def rows(self, got, other=False):
        if got:
            return pl.ds(0, 2)
        return 1 - self.place.y if other else self.place.y

    def send(self, kind, ref, shift, when=None, to=None):
        copy = self.copy(kind, ref, shift, to)
        under(both(self.here, when), copy.wait_send if self.finishing else copy.start)

    def wait(self, kind, ref, shift, when=None):
        if not self.finishing:
            copy = self.copy(kind, ref, shift)
            under(both(self.here, when), copy.wait_recv)

    def have(self, stage, shift, when=None):
        order, place = self.stream.order, self.place
        if stage == len(order):
            return
        ref = self.region(shift, self.rows("y" in order[:stage]), place.p)
        if order[stage] == "y":
            self.send("y", ref, shift, when)
            return
        self.send("up", ref, shift, place.z < place.count_z - 1)
        self.send("down", ref, shift, place.z > 0)
        self.have(stage + 1, shift)

    def shifts(self):
        pairs = [(-r, r) for r in range(1, self.place.count_z)]
        return [d for pair in pairs for d in pair]

    def rows_at(self, stage):
        order = self.stream.order
        if stage < 0:
            return self.rows(False)
        return self.rows("y" in order[:stage], other=order[stage] == "y")

    def start(self):
        self.have(0, 0)
        self.send("own", self.region(0, self.rows(False), self.place.p), 0)

    def give(self):
        ref = self.region(0, self.rows(False), self.place.p)
        self.send("x_own", ref, 0, None, self.region(0, self.rows(False), self.place.p, 2))
        self.send("own", ref, 0)

    def given(self):
        self.wait("x_own", self.region(0, self.rows(False), self.place.p), 0)
        self.have(0, 0)

    def arrive(self, stage, shift):
        place = self.place
        dim = self.stream.order[stage]
        when = self.valid(shift) if shift else None
        kind = ("up" if shift < 0 else "down") if dim == "z" else dim
        ref = self.region(shift, self.rows_at(stage), place.p)
        self.wait(kind, ref, shift, when)
        if dim == "z":
            onward = place.z < place.count_z - 1 if shift < 0 else place.z > 0
            self.send(kind, ref, shift, both(when, onward))
        self.have(stage + 1, shift, when)
        if self.stream.mode == "relay":
            to = self.region(shift, self.rows_at(stage), place.p, 1)
            self.send("x_" + dim, ref, shift, when, to)
        else:
            self.send("core_" + dim, ref, shift, when)

    def mirror(self, stage, shift):
        dim = self.stream.order[stage]
        when = self.valid(shift) if shift else None
        ref = self.region(shift, self.rows_at(stage), self.place.p)
        self.wait("x_" + dim, ref, shift, when)
        self.send("core_" + dim, ref, shift, when)

    def from_partner(self):
        order, place = self.stream.order, self.place
        self.wait("own", self.region(0, self.rows(False), 1 - place.p), 0)
        for stage, dim in enumerate(order):
            spread = "z" in order[:stage]
            shifts = self.shifts() if dim == "z" else [0] + (self.shifts() if spread else [])
            for shift in shifts:
                ref = self.region(shift, self.rows_at(stage), 1 - place.p)
                self.wait("core_" + dim, ref, shift, self.valid(shift) if shift else None)


def greet(place):
    barrier = pltpu.get_barrier_semaphore()
    z, count_z = place.z, place.count_z

    def signal(kind):
        pl.semaphore_signal(barrier, inc=1, device_id=place.target(kind), device_id_type=MESH)

    signal("x")
    signal("y")
    signal("own")
    pl.when(z < count_z - 1)(lambda: signal("up"))
    pl.when(z > 0)(lambda: signal("down"))
    ends = jnp.where(z < count_z - 1, 1, 0) + jnp.where(z > 0, 1, 0)
    pl.semaphore_wait(barrier, 3 + ends)


def turned(tensor, cosine, sine_part):
    return tensor * cosine + pltpu.roll(tensor, tensor.shape[-1] // 2, 1) * sine_part


def thirds(tensor):
    parts = []
    for _ in range(3):
        part = tensor.astype(jnp.bfloat16)
        parts.append(part)
        tensor = tensor - part.astype(jnp.float32)
    return parts


def exact_scores(queries, keys):
    q1, q2, q3 = thirds(queries)
    k1, k2, k3 = thirds(keys)
    left = jnp.concatenate([q1, q2, q1, q2, q1, q3], axis=1)
    right = jnp.concatenate([k1, k1, k2, k2, k3, k1], axis=1)
    return lax.dot_general(
        left, right, (((1,), (1,)), ((), ())), preferred_element_type=jnp.float32
    )


def layer_pieces(depth, source, length, held, gains, biases, angles, scratch, store):
    normed, projected, context = scratch
    rows, width = normed.shape
    depth_rows = held.shape[1] * held.shape[2] * held.shape[3] * held.shape[4]
    group_size = HEADS // KV_HEADS
    kv_width = KV_HEADS * HEAD_DIM

    def halved(columns):
        return columns // 2 if columns % (2 * LANES) == 0 else LANES

    def weight(column, tile):
        return held[depth, :, :, :, :, pl.ds(column, tile)].reshape(depth_rows, tile)

    def project():
        wide = source[...].astype(jnp.float32)
        inv_rms = lax.rsqrt(jnp.mean(wide * wide, axis=-1, keepdims=True) + EPS)
        normed[...] = (wide * inv_rms * gains[depth, 0]).astype(jnp.bfloat16)

        tile = halved(projected.shape[1])

        @pl.loop(0, projected.shape[1] // tile)
        def _(j):
            column = pl.multiple_of(j * tile, tile)
            block = jnp.dot(normed[...], weight(column, tile), preferred_element_type=jnp.float32)
            projected[:, pl.ds(column, tile)] = block + biases[depth, 0, :, pl.ds(column, tile)]

    def attend():
        cosine, sine_part = angles[0], angles[1]
        shape = (group_size * length, length)
        query_at = lax.rem(lax.broadcasted_iota(jnp.int32, shape, 0), length)
        causal = query_at >= lax.broadcasted_iota(jnp.int32, shape, 1)

        @pl.loop(0, rows // length)
        def _(unit):
            there = pl.ds(pl.multiple_of(unit * length, length), length)
            for head in range(KV_HEADS):
                first = head * group_size * HEAD_DIM

                def columns(start):
                    return projected[there, start : start + HEAD_DIM]

                queries = jnp.concatenate(
                    [
                        turned(columns(first + h * HEAD_DIM), cosine, sine_part)
                        for h in range(group_size)
                    ],
                    axis=0,
                )
                keys = turned(columns(width + head * HEAD_DIM), cosine, sine_part)
                values = columns(width + kv_width + head * HEAD_DIM).astype(jnp.bfloat16)
                scores = exact_scores(queries, keys) * (1.0 / math.sqrt(HEAD_DIM))
                scores = jnp.where(causal, scores, -1e30)
                weights = jnp.exp(scores - jnp.max(scores, axis=-1, keepdims=True))
                total = jnp.sum(weights, axis=-1, keepdims=True)
                probability = (weights / total).astype(jnp.bfloat16)
                block = jnp.dot(probability, values, preferred_element_type=jnp.float32)
                block = block.astype(jnp.bfloat16)
                for h in range(group_size):
                    to = slice(first + h * HEAD_DIM, first + (h + 1) * HEAD_DIM)
                    context[there, to] = block[h * length : (h + 1) * length]

    def update():
        tile = halved(width)

        @pl.loop(0, width // tile)
        def _(j):
            column = pl.multiple_of(j * tile, tile)
            to = pl.ds(column, tile)
            block = jnp.dot(
                context[...], weight(projected.shape[1] + column, tile), preferred_element_type=jnp.float32
            )
            wide = source[:, to].astype(jnp.float32)
            store[:, to] = (wide + block).astype(jnp.bfloat16)

    return project, attend, update


def section_kernel(
    count_z,
    length,
    chunks,
    hidden_ref,
    gain_ref,
    qkv_ref,
    bias_ref,
    out_ref,
    angles,
    result,
    held,
    gains,
    biases,
    before,
    after,
    normed,
    projected,
    context,
    send_sems,
    recv_sems,
    act_sems,
    local_sems,
):
    place = Place(count_z)
    x, y, z, p = place.x, place.y, place.z, place.p
    qkv = qkv_ref.shape[-1]
    width = out_ref.shape[-1]
    rows = before.shape[1] // chunks
    half = chunks // 2
    on = [x == 0, x == 1]

    loads = [
        (None, pltpu.make_async_copy(gain_ref, gains, local_sems.at[0])),
        (None, pltpu.make_async_copy(bias_ref, biases, local_sems.at[1])),
        (on[0], pltpu.make_async_copy(hidden_ref, before.at[0], local_sems.at[2])),
    ]
    for depth in range(2):
        home = held.at[depth, z, y, p]
        parts = ((qkv_ref, pl.ds(0, qkv)), (out_ref, pl.ds(qkv, width)))
        for number, (ref, columns) in enumerate(parts):
            sem = local_sems.at[3 + 2 * depth + number]
            load = pltpu.make_async_copy(ref.at[depth, 0], home.at[:, columns], sem)
            loads.append((None, load))
    for when, load in loads:
        under(when, load.start)
    greet(place)
    for when, load in loads:
        under(when, load.wait)

    streams = make_streams(qkv, qkv + width)
    pace = 2 * rows * width / LINK
    _, program = make_plan(count_z, held.shape[4], streams, chunks, pace)

    seen, met, moves = {}, set(), {}
    for _, section, what in program:
        if what[0] not in COSTS and (section, what[1]) not in seen:
            stream = streams[what[1]]
            slot = 1 if section == 0 and stream.mode else stream.slot
            seen[section, what[1]] = Gather(
                stream, section, slot, held, place, send_sems, recv_sems
            )

    def partners(section, slot, groups):
        found = []
        for (owner, number), part in seen.items():
            known = part.slot != slot or owner != section or (owner, number) in met
            if not known and part.stream.group in groups:
                met.add((owner, number))
                found.append(part.from_partner)
        return found

    def move(section, what):
        part = seen[section, what[1]]
        rest = what[2:] if what[0] in ("arrive", "mirror") else ()
        return partial(getattr(part, what[0]), *rest)

    everything, segments, loose = [], {}, {0: [], 1: []}
    for _, section, what in program:
        kind, number = what[:2]
        if kind not in COSTS:
            everything.append(move(section, what))
            loose[section].append(everything[-1])
            continue
        spot = number * chunks + what[2] + BEHIND * section, PIECES.index(kind)
        loose[section] += partners(section, number, "qo" if kind == "update" else "q")
        segments.setdefault(spot, []).extend(loose[section])
        loose[section] = []

    def crossing(slot, chunk, depth):
        here = pl.ds(pl.multiple_of(chunk * rows, rows), rows)
        return pltpu.make_async_remote_copy(
            src_ref=after.at[depth, here],
            dst_ref=before.at[slot, here],
            send_sem=act_sems.at[0, depth, chunk],
            recv_sem=act_sems.at[1, slot, chunk],
            device_id=place.target("x"),
            device_id_type=MESH,
        )

    @pl.loop(0, 2 * chunks + BEHIND)
    def _(step):
        item = step - BEHIND * x
        present = (item >= 0) & (item < 2 * chunks)
        depth, chunk = item // chunks, item % chunks
        here = pl.ds(pl.multiple_of(chunk * rows, rows), rows)
        pieces = layer_pieces(
            depth,
            before.at[depth, here],
            length,
            held,
            gains,
            biases,
            angles,
            (normed, projected, context),
            after.at[depth, here],
        )
        for number, piece in enumerate(pieces):
            for (spot, place_in), actions in segments.items():
                if place_in == number and actions:
                    pl.when(step == spot)(lambda actions=actions: [f() for f in actions] and None)
            if number == 0:
                pl.when(present & (item + x > 0) & (item + chunks * x >= chunks))(
                    lambda: crossing(depth, chunk, 0).wait_recv()
                )
            pl.when(present)(piece)
        last = chunks + half + 2 * chunks * (1 - x)
        pl.when(present & (item < last))(lambda: crossing(depth + x, chunk, depth).start())

    for actions in loose.values():
        for action in actions:
            action()

    def pass_on(section, depth, chunk):
        return pl.when(on[section])(
            lambda: crossing(depth + section, chunk, depth).wait_send()
        )

    @pl.when(on[0])
    def _():
        for chunk in range(half):
            crossing(2, chunk, 0).wait_recv()
        result[...] = before[2, pl.ds(0, half * rows)]

    @pl.when(on[1])
    def _():
        result[...] = after[1, pl.ds(half * rows, half * rows)]

    for section in (0, 1):
        for number in range(2 * chunks if section == 0 else chunks + half):
            pass_on(section, number // chunks, number % chunks)
    for part in seen.values():
        part.finishing = True
    for action in everything:
        action()


def own_micros(sections, fsdp, hidden_in, norm_gain, qkv_weight, qkv_bias, out_weight):
    depths, _, shard, qkv = qkv_weight.shape
    micros, seqs, length, width = hidden_in.shape
    rows = micros * seqs * length
    owned = rows // sections
    count_z = fsdp // 4
    half_dim = HEAD_DIM // 2
    frequency = np.exp(np.arange(half_dim) * (-2.0 * math.log(THETA) / HEAD_DIM))
    turn = np.arange(length)[:, None] * frequency[None, :]
    cosine, sine_part = np.cos(turn), np.sin(turn)
    angles = np.stack(
        [
            np.concatenate([cosine, cosine], axis=-1),
            np.concatenate([-sine_part, sine_part], axis=-1),
        ]
    ).astype(np.float32)
    count = len(make_streams(qkv, qkv + width))
    sems = (count, len(KINDS), count_z)
    anywhere = pl.BlockSpec(memory_space=pl.ANY)
    in_vmem = pl.BlockSpec(memory_space=pltpu.VMEM)
    result = pl.pallas_call(
        partial(section_kernel, count_z, length, CHUNKS),
        out_shape=jax.ShapeDtypeStruct((owned, width), hidden_in.dtype),
        in_specs=[anywhere] * 5 + [in_vmem],
        out_specs=in_vmem,
        scratch_shapes=[
            pltpu.VMEM((3, count_z, 2, 2, shard, qkv + width), qkv_weight.dtype),
            pltpu.VMEM((depths, 1, 1, width), jnp.float32),
            pltpu.VMEM((depths, 1, 1, qkv), jnp.float32),
            pltpu.VMEM((3, rows, width), jnp.bfloat16),
            pltpu.VMEM((2, rows, width), jnp.bfloat16),
            pltpu.VMEM((rows // CHUNKS, width), jnp.bfloat16),
            pltpu.VMEM((rows // CHUNKS, qkv), jnp.float32),
            pltpu.VMEM((rows // CHUNKS, width), jnp.bfloat16),
            pltpu.SemaphoreType.DMA(sems),
            pltpu.SemaphoreType.DMA(sems),
            pltpu.SemaphoreType.DMA((2, 3, CHUNKS)),
            pltpu.SemaphoreType.DMA((7,)),
        ],
        compiler_params=pltpu.CompilerParams(
            collective_id=0, has_side_effects=True, vmem_limit_bytes=62 * 1024 * 1024
        ),
    )(
        hidden_in.reshape(rows, width),
        norm_gain.reshape(depths, 1, 1, width),
        qkv_weight,
        qkv_bias.reshape(depths, 1, 1, qkv),
        out_weight,
        jnp.asarray(angles),
    )
    return result.reshape(micros // sections, seqs, length, width)


def solution(mesh):
    in_specs = (
        P(None, "fsdp", None, None),
        P(None, "section", None),
        P(None, "section", "fsdp", None),
        P(None, "section", None),
        P(None, "section", "fsdp", None),
    )
    out_specs = P("section", "fsdp", None, None)
    whole_fits = mesh.shape["section"] == 2 and mesh.shape["fsdp"] % 4 == 0
    body = partial(own_micros, mesh.shape["section"], mesh.shape["fsdp"]) if whole_fits else per_device
    return jax.shard_map(
        body, mesh=mesh, in_specs=in_specs, out_specs=out_specs, check_vma=False
    )
```
